32 devices in a mesh: seq: 4 (over y, core), wide: 8 (over z, x).
Axes of the slice: x: 2, y: 2, z: 4, core: 2. Of those that a mesh axis runs over, the one named last changes fastest.
Arguments:
- block_input: bfloat16 [16, 1024, 1024], P('wide', 'seq'), may hold values from -6 to 6
- segment_ids: int32 [16, 1024], P('wide'), may hold values from 0 to 3, never falling along the last dimension, each value on 1 to 512 neighbouring positions
- assignment: int32 [16, 1024], P('wide', 'seq'), may hold values from 0 to 7, as said below
- norm_attn: bfloat16 [1024], P(('seq', 'wide')), may hold values from 0.5 to 1.5
- weight_qkv: bfloat16 [1024, 3072], P(('seq', 'wide')), may hold values from -0.1875 to 0.1875
- weight_proj: bfloat16 [1024, 1024], P(('seq', 'wide')), may hold values from -1.5 to 1.5
- norm_ffn: bfloat16 [1024], P(('seq', 'wide')), may hold values from 0.5 to 1.5
- weight_up: bfloat16 [1024, 4096], P(('seq', 'wide')), may hold values from -0.1875 to 0.1875
- weight_down: bfloat16 [4096, 1024], P(('seq', 'wide')), may hold values from -0.09375 to 0.09375
- centroids: bfloat16 [8, 1024], P('wide'), may hold values from -0.09375 to 0.09375
- expert_norms: bfloat16 [8, 2, 1024], P('wide'), may hold values from 0.5 to 1.5
- expert_in: bfloat16 [8, 2, 1024, 4096], P('wide', None, None, 'seq'), may hold values from -0.1875 to 0.1875
- expert_out: bfloat16 [8, 2, 4096, 1024], P('wide', None, 'seq'), may hold values from -0.09375 to 0.09375
- grad_out: bfloat16 [16, 1024, 1024], P('wide', 'seq'), may hold values from -6 to 6
Outputs:
- output: bfloat16 [16, 1024, 1024], P('wide', 'seq')
- grad_input: float32 [16, 1024, 1024], P('wide', 'seq')
- grad_norm_attn: float32 [1024], P(('seq', 'wide'))
- grad_weight_qkv: float32 [1024, 3072], P(('seq', 'wide'))
- grad_weight_proj: float32 [1024, 1024], P(('seq', 'wide'))
- grad_norm_ffn: float32 [1024], P(('seq', 'wide'))
- grad_weight_up: float32 [1024, 4096], P(('seq', 'wide'))
- grad_weight_down: float32 [4096, 1024], P(('seq', 'wide'))
- grad_centroids: float32 [8, 1024], P('wide')
- grad_expert_norms: float32 [8, 2, 1024], P('wide')
- grad_expert_in: float32 [8, 2, 1024, 4096], P('wide', None, None, 'seq')
- grad_expert_out: float32 [8, 2, 4096, 1024], P('wide', None, 'seq')
- log_gate: float32 [8], P('wide')
- log_score: float32 [8], P('wide')
The draws below stay inside these ranges and needn't reach their ends.
Inputs may be any that keep to these rules, and one draw needn't show every extreme that they name: `assignment`: in the block of one device (the 2 rows of one index of wide at the 256 positions of one index of seq) every expert is named by exactly 64 tokens.
All inputs are finite; a program needn't handle non-finite values.
Results may differ from the reference program's by a relative error of at most 0.017.
Values may be sent and summed in bfloat16 or wider, within the bound.
A program may use at most 320 MiB of HBM per device.

```python
import math
import jax
import jax.numpy as jnp
import numpy as np
from jax import lax

D = 1024
HEADS = 16
FF = 4096
HEAD_DIM = 64
LEN = 1024
ROWS_DEV = 2
DOCS = 4
DOC_MOST = 512
SEQ_DEV = 256
TOK_DEV = 512
ROWS = 16
TOKENS = 16384
EXPERTS = 8


def draw_assignment(key, part):
    blocks_wide = ROWS // ROWS_DEV
    blocks_seq = LEN // SEQ_DEV
    block_keys = jax.random.split(key, blocks_wide * blocks_seq)
    shuffled = jax.vmap(lambda block_key: jax.random.permutation(block_key, TOK_DEV))(block_keys)
    chosen = (shuffled % EXPERTS).astype(jnp.int32)
    chosen = chosen.reshape(blocks_wide, blocks_seq, ROWS_DEV, SEQ_DEV).transpose(0, 2, 1, 3)
    return chosen.reshape(ROWS, LEN)


def block_levels(own_key, shape, cuts, least, largest):
    def one(dim, parts):
        steps = jax.random.uniform(jax.random.fold_in(jax.random.fold_in(own_key, 6), dim), (parts,), jnp.float32, least / len(cuts), largest / len(cuts))
        return jnp.repeat(jnp.exp(steps), shape[dim] // parts).reshape((-1,) + (1,) * (len(shape) - dim - 1))

    gain = one(*cuts[0])
    for cut in cuts[1:]:
        gain = gain * one(*cut)
    return gain


def split_up(amount, total, most, slope):
    portions = [(1 << 20) // math.isqrt(rank ** slope) + 1 for rank in range(2, amount + 1)]
    surplus, given = total - most - (amount - 1), [1] * (amount - 1)
    while surplus > 0:
        candidates = [i for i in range(amount - 1) if given[i] < most]
        whole, left = sum([portions[i] for i in candidates]), surplus
        for i in candidates:
            more = min(most - given[i], max(1, left * portions[i] // whole), surplus)
            given[i] = given[i] + more
            surplus = surplus - more
    return np.array([most] + given)


def ragged(own_key, number_of, total, most, skew):
    if number_of == 2:
        one = jax.random.randint(own_key, (), max(1, total - most), min(most, total - 1) + 1)
        return jnp.stack([one, total - one])
    sizes = jnp.asarray(split_up(number_of, total, most, skew), jnp.int32)
    twos = (number_of - 1) // 2
    source_of, receiver = sizes[1:1 + 2 * twos:2], sizes[2:2 + 2 * twos:2]
    margin = jnp.minimum(source_of - 1, most - receiver)
    moved = jax.random.randint(jax.random.fold_in(own_key, 1), (twos,), 0, 1 << 20) % (margin + 1)
    sizes = sizes.at[1:1 + 2 * twos:2].set(source_of - moved).at[2:2 + 2 * twos:2].set(receiver + moved)
    return sizes[jax.random.permutation(jax.random.fold_in(own_key, 2), number_of)]


def gaussian(stream_key, shape, spread, most, pieces=(), dtype=jnp.bfloat16):
    gain = block_levels(stream_key, shape, pieces, -0.22, 0.18) if pieces else 1.0
    result = jax.random.normal(stream_key, shape, jnp.float32) * spread * gain
    return jnp.minimum(jnp.maximum(result, -most), most).astype(dtype)


def setup_inputs(seed: int = 0) -> dict:
    key_of = jax.random.split(jax.random.key(seed), 15)
    return {
        "block_input": gaussian(key_of[0], (ROWS, LEN, D), 1.0, 6.0, ((0, 8), (1, 4))),
        "segment_ids": jax.vmap(lambda own: jnp.searchsorted(jnp.cumsum(ragged(own, DOCS, LEN, DOC_MOST, 2)), jnp.arange(LEN), side="right"))(jax.random.split(key_of[1], ROWS)).reshape((ROWS, LEN)).astype(jnp.int32),
        "assignment": draw_assignment(jax.random.fold_in(key_of[14], 71), 0),
        "norm_attn": jnp.clip(1.0 + 0.1 * jax.random.normal(key_of[3], (D,), jnp.float32), 0.5, 1.5).astype(jnp.bfloat16),
        "weight_qkv": gaussian(key_of[4], (D, 3 * D), D ** -0.5, 0.1875, ((0, 32),)),
        "weight_proj": gaussian(key_of[5], (D, D), (D // 64) ** -0.5, 1.5, ((0, 32),)),
        "norm_ffn": jnp.clip(1.0 + 0.1 * jax.random.normal(key_of[6], (D,), jnp.float32), 0.5, 1.5).astype(jnp.bfloat16),
        "weight_up": gaussian(key_of[7], (D, FF), D ** -0.5, 0.1875, ((0, 32),)),
        "weight_down": gaussian(key_of[8], (FF, D), FF ** -0.5, 0.09375, ((0, 32),)),
        "centroids": gaussian(key_of[9], (EXPERTS, D), (4 * D) ** -0.5, 0.09375, ((0, 8),)),
        "expert_norms": jnp.clip(1.0 + 0.1 * jax.random.normal(key_of[10], (EXPERTS, 2, D), jnp.float32), 0.5, 1.5).astype(jnp.bfloat16),
        "expert_in": gaussian(key_of[11], (EXPERTS, 2, D, FF), D ** -0.5, 0.1875, ((0, 8), (3, 4))),
        "expert_out": gaussian(key_of[12], (EXPERTS, 2, FF, D), FF ** -0.5, 0.09375, ((0, 8), (2, 4))),
        "grad_out": gaussian(key_of[13], (ROWS, LEN, D), 1.0, 6.0, ((0, 8), (1, 4))),
    }


epsilon = 1e-05
highest = lax.Precision.HIGHEST

@jax.custom_vjp
def low(v):
    return lax.optimization_barrier(v.astype(jnp.bfloat16)).astype(jnp.float32)

@jax.custom_vjp
def low_back(v):
    return v

def low_keep(v):
    return (low(v), None)

def low_pass(kept, grad):
    return (grad,)

def back_keep(v):
    return (v, None)

def back_low(kept, grad):
    return (low(grad),)
low.defvjp(low_keep, low_pass)
low_back.defvjp(back_keep, back_low)

def layer_norm(values, norm_gain):
    centered = values - lax.optimization_barrier(jnp.mean(values, axis=-1, keepdims=True))
    variance = lax.optimization_barrier(jnp.mean(centered * centered, axis=-1, keepdims=True))
    return centered * lax.rsqrt(variance + epsilon) * norm_gain

def matmul(left_side, right_side):
    return jnp.dot(left_side, right_side, precision=highest)

def attend_row(packed):
    qkv_row, segment_row = packed
    query_rows = qkv_row[:, :D].reshape(LEN, HEADS, HEAD_DIM)
    key_rows = qkv_row[:, D:2 * D].reshape(LEN, HEADS, HEAD_DIM)
    value_rows = qkv_row[:, 2 * D:].reshape(LEN, HEADS, HEAD_DIM)
    score_scale = 1.0 / math.sqrt(HEAD_DIM)
    scores = jnp.einsum('qhd,khd->hqk', query_rows, key_rows, precision=highest) * score_scale
    scores = low_back(scores)
    position = jnp.arange(LEN)
    allowed = (segment_row[:, None] == segment_row[None, :]) & (position[None, :] <= position[:, None])
    scores = jnp.where(allowed[None], scores, -1e+30)
    probs_low = low(jax.nn.softmax(scores, axis=-1))
    return jnp.einsum('hqk,khd->qhd', probs_low, value_rows, precision=highest).reshape(LEN, D)

def expert_apply(packed):
    routed_rows, centroid, norm_pair, inner_pair, outer_pair = packed
    logit_row = matmul(routed_rows, centroid)
    gate_value = jax.nn.sigmoid(logit_row)
    state_now = routed_rows
    for sublayer in range(2):
        normed = low(layer_norm(state_now, norm_pair[sublayer]))
        pre_expert = low_back(matmul(normed, inner_pair[sublayer]))
        expert_active = low(jax.nn.gelu(pre_expert, approximate=False))
        state_now = state_now + low_back(matmul(expert_active, outer_pair[sublayer]))
    returned = low(low_back(gate_value[:, None] * state_now))
    return (returned, jnp.stack([jnp.mean(gate_value), jnp.mean(logit_row * logit_row)]))

def reference(block_input, segment_ids, assignment, norm_attn, weight_qkv, weight_proj, norm_ffn, weight_up, weight_down, centroids, expert_norms, expert_in, expert_out, grad_out):
    by_expert = jnp.argsort(assignment.reshape(TOKENS), stable=True).astype(jnp.int32)
    restore = jnp.argsort(by_expert, stable=True).astype(jnp.int32)

    def forward(input_rows, gain_attn, qkv_weight, proj_weight, gain_ffn, up_weight, down_weight, centroid_all, norm_all, inner_all, outer_all):
        tokens_flat = input_rows.reshape(TOKENS, D)
        normed_attn = low(layer_norm(tokens_flat, gain_attn))
        qkv = low(low_back(matmul(normed_attn, qkv_weight)))
        attended = lax.map(jax.checkpoint(attend_row), (qkv.reshape(ROWS, LEN, 3 * D), segment_ids))
        attended = low(low_back(attended.reshape(TOKENS, D)))
        hidden = tokens_flat + low_back(matmul(attended, proj_weight))
        normed_ffn = low(layer_norm(hidden, gain_ffn))
        pre_act = low_back(matmul(normed_ffn, up_weight))
        active = low(jax.nn.gelu(pre_act, approximate=False))
        dense_out = hidden + low_back(matmul(active, down_weight))
        routed = low(low_back(dense_out))
        grouped = routed[by_expert].reshape(EXPERTS, TOKENS // EXPERTS, D)
        returned, expert_stats = lax.map(jax.checkpoint(expert_apply), (grouped, centroid_all, norm_all, inner_all, outer_all))
        returned = returned.reshape(TOKENS, D)[restore]
        return ((dense_out + returned).reshape(ROWS, LEN, D), expert_stats)
    floats = (block_input.astype(jnp.float32), norm_attn.astype(jnp.float32), weight_qkv.astype(jnp.float32), weight_proj.astype(jnp.float32), norm_ffn.astype(jnp.float32), weight_up.astype(jnp.float32), weight_down.astype(jnp.float32), centroids.astype(jnp.float32), expert_norms.astype(jnp.float32), expert_in.astype(jnp.float32), expert_out.astype(jnp.float32))
    output, pull_back, expert_stats = jax.vjp(forward, *floats, has_aux=True)
    gradients = pull_back(grad_out.astype(jnp.float32))
    return (output.astype(jnp.bfloat16), gradients[0], gradients[1], gradients[2], gradients[3], gradients[4], gradients[5], gradients[6], gradients[7], gradients[8], gradients[9], gradients[10], expert_stats[:, 0], expert_stats[:, 1])
```

```python
import functools
import math

import jax
import jax.numpy as jnp
from jax import lax
from jax.experimental import pallas as pl
from jax.experimental.pallas import tpu as pltpu
from jax.sharding import PartitionSpec as P

HEADS = 16
HEAD_DIM = 64
BLOCKS = 4

epsilon = 1e-05
highest = lax.Precision.HIGHEST
bf16 = jnp.bfloat16
f32 = jnp.float32


def layer_norm(values, norm_gain):
    centered = values - jnp.mean(values, axis=-1, keepdims=True)
    variance = jnp.mean(centered * centered, axis=-1, keepdims=True)
    return centered * lax.rsqrt(variance + epsilon) * norm_gain


def norm_back(values, norm_gain, grad_normed):
    _, pull_back = jax.vjp(layer_norm, values, norm_gain)
    return pull_back(grad_normed)


def gelu_pair(values):
    cdf = 0.5 * (1.0 + lax.erf(values * math.sqrt(0.5)))
    density = jnp.exp(values * values * -0.5) * (1.0 / math.sqrt(2.0 * math.pi))
    return values * cdf, cdf + values * density


def product(left_side, right_side):
    return jnp.dot(left_side, right_side, preferred_element_type=f32)


def product_bt(left_side, right_side):
    return lax.dot_general(
        left_side, right_side, (((1,), (1,)), ((), ())), preferred_element_type=f32
    )


def product_at(left_side, right_side):
    return lax.dot_general(
        left_side, right_side, (((0,), (0,)), ((), ())), preferred_element_type=f32
    )


def seq_send(values, pairs):
    return lax.ppermute(values, "seq", pairs)


def swap_core(values):
    return seq_send(values, [(0, 1), (1, 0), (2, 3), (3, 2)])


def swap_chip(values):
    return seq_send(values, [(0, 2), (2, 0), (1, 3), (3, 1)])


def pair_probs(query, keys, bias, score_scale):
    scores = product_bt(keys, query) * score_scale + bias
    exp_scores = jnp.exp(scores - jnp.max(scores, axis=0, keepdims=True))
    return exp_scores * (1.0 / jnp.sum(exp_scores, axis=0, keepdims=True))


def attend_kernel(score_scale, q_ref, k0, v0, k1, v1, k2, v2, bias_ref, out_ref):
    bias = bias_ref[0]
    parts = []
    for head in range(2):
        cols = slice(head * HEAD_DIM, (head + 1) * HEAD_DIM)
        keys = jnp.concatenate([k2[0][:, cols], k1[0][:, cols], k0[0][:, cols]], axis=0)
        vals = jnp.concatenate([v2[0][:, cols], v1[0][:, cols], v0[0][:, cols]], axis=0)
        probs_low = pair_probs(q_ref[0][:, cols], keys, bias, score_scale).astype(bf16)
        parts.append(product_at(vals, probs_low))
    out_ref[0] = jnp.concatenate(parts, axis=0).T.astype(bf16)


def attend_back_kernel(
    score_scale, q_ref, k0, v0, k1, v1, k2, v2, bias_ref, grad_ref, dq_ref, d0, d1, d2
):
    bias = bias_ref[0]
    dq_parts, dk_parts, dv_parts = [], [], []
    for head in range(2):
        cols = slice(head * HEAD_DIM, (head + 1) * HEAD_DIM)
        query = q_ref[0][:, cols]
        grad_att = grad_ref[0][:, cols]
        keys = jnp.concatenate([k2[0][:, cols], k1[0][:, cols], k0[0][:, cols]], axis=0)
        vals = jnp.concatenate([v2[0][:, cols], v1[0][:, cols], v0[0][:, cols]], axis=0)
        probs = pair_probs(query, keys, bias, score_scale)
        grad_probs = product_bt(vals, grad_att)
        dv_parts.append(product(probs.astype(bf16), grad_att))
        inner_sum = jnp.sum(probs * grad_probs, axis=0, keepdims=True)
        grad_scores = (probs * (grad_probs - inner_sum)).astype(bf16)
        dk_parts.append(product(grad_scores, query) * score_scale)
        dq_parts.append(product_at(keys, grad_scores) * score_scale)
    dq_ref[0] = jnp.concatenate(dq_parts, axis=0).T.astype(bf16)
    d_keys = jnp.concatenate(dk_parts, axis=1).astype(bf16)
    d_vals = jnp.concatenate(dv_parts, axis=1).astype(bf16)
    size = d_keys.shape[0] // 3
    for place, ref in enumerate((d2, d1, d0)):
        ref[0, 0] = d_keys[place * size : (place + 1) * size]
        ref[1, 0] = d_vals[place * size : (place + 1) * size]


def attention_specs(local_len, model_width, key_len):
    width = 2 * HEAD_DIM
    groups = model_width // width
    query = pl.BlockSpec((1, local_len, width), lambda row, head: (row, 0, head))
    values = pl.BlockSpec((1, local_len, width), lambda row, head: (row, 0, head + groups))
    bias = pl.BlockSpec((1, key_len, local_len), lambda row, head: (row, 0, 0))
    return groups, query, [query, query, values, query, values, query, values, bias]


def attend(query, kv_blocks, bias):
    rows, local_len, model_width = query.shape
    groups, spec, in_specs = attention_specs(local_len, model_width, bias.shape[1])
    operands = [block for block in kv_blocks for _ in range(2)]
    flops = 4 * rows * model_width * local_len * bias.shape[1]
    return pl.pallas_call(
        functools.partial(attend_kernel, 1.0 / math.sqrt(HEAD_DIM)),
        grid=(rows, groups),
        in_specs=in_specs,
        out_specs=spec,
        out_shape=jax.ShapeDtypeStruct(query.shape, bf16),
        cost_estimate=pl.CostEstimate(
            flops=flops * 6, bytes_accessed=8 * query.size * 2, transcendentals=0
        ),
        name="attend",
    )(query, *operands, bias)


def attend_back(query, kv_blocks, bias, grad_attended):
    rows, local_len, model_width = query.shape
    groups, spec, in_specs = attention_specs(local_len, model_width, bias.shape[1])
    operands = [block for block in kv_blocks for _ in range(2)]
    pair_spec = pl.BlockSpec((2, 1, local_len, 2 * HEAD_DIM), lambda row, head: (0, row, 0, head))
    pair_shape = jax.ShapeDtypeStruct((2, rows, local_len, model_width), bf16)
    flops = 10 * rows * model_width * local_len * bias.shape[1]
    return pl.pallas_call(
        functools.partial(attend_back_kernel, 1.0 / math.sqrt(HEAD_DIM)),
        grid=(rows, groups),
        in_specs=in_specs + [spec],
        out_specs=[spec, pair_spec, pair_spec, pair_spec],
        out_shape=[jax.ShapeDtypeStruct(query.shape, bf16)] + [pair_shape] * 3,
        cost_estimate=pl.CostEstimate(
            flops=flops * 6, bytes_accessed=16 * query.size * 2, transcendentals=0
        ),
        name="attend_back",
    )(query, *operands, bias, grad_attended)


def ffn_forward(normed, inner_parts, outer_parts, residual):
    kept = []
    total = residual
    for inner, outer in zip(inner_parts, outer_parts):
        act, slope = gelu_pair(product(normed, inner))
        act = act.astype(bf16)
        kept.append((act, slope.astype(bf16)))
        total = total + product(act, outer)
    return total, kept


def ffn_backward(kept, inner_parts, outer_parts, grad_branch):
    grad_pres = []
    grad_normed = None
    for (act, slope), inner, outer in zip(kept, inner_parts, outer_parts):
        grad_pre = (product_bt(grad_branch, outer) * slope.astype(f32)).astype(bf16)
        grad_pres.append(grad_pre)
        piece = product_bt(grad_pre, inner)
        grad_normed = piece if grad_normed is None else grad_normed + piece
    return grad_pres, grad_normed


def reduce_slices(own, core, chip, both):
    got_both = swap_core(both().astype(bf16))
    got_core = swap_core(core().astype(bf16))
    got_chip = swap_chip((chip() + got_both.astype(f32)).astype(bf16))
    return own() + got_core.astype(f32) + got_chip.astype(f32)


def per_device(
    block_input,
    segment_ids,
    assignment,
    norm_attn,
    weight_qkv,
    weight_proj,
    norm_ffn,
    weight_up,
    weight_down,
    centroids,
    expert_norms,
    expert_in,
    expert_out,
    grad_out,
):
    row_count, local_len, model_width = block_input.shape
    token_count = row_count * local_len
    seq_devices = lax.axis_size("seq")
    seq_index = lax.axis_index("seq")
    experts = lax.axis_size("wide")
    devices = seq_devices * experts
    every = ("seq", "wide")
    shard = weight_up.shape[0]
    hidden_width = weight_up.shape[1]

    gains_own = jnp.stack([norm_attn, norm_ffn]).astype(f32)
    gains_all = lax.all_to_all(
        jnp.broadcast_to(gains_own[None], (devices, 2, shard)), every, 0, 0, tiled=True
    )
    gains_all = gains_all.transpose(1, 0, 2).reshape(2, model_width)
    gain_attn = gains_all[0]
    gain_ffn = gains_all[1]

    qkv_full = lax.all_gather(weight_qkv, every, axis=0, tiled=True)
    up_own = (
        weight_up.reshape(shard, devices, BLOCKS, shard)
        .transpose(0, 2, 1, 3)
        .reshape(shard, hidden_width)
    )
    down_own = weight_down.reshape(BLOCKS, shard, model_width).transpose(1, 0, 2)
    rest_own = jnp.concatenate(
        [weight_proj, up_own, down_own.reshape(shard, BLOCKS * model_width)], axis=1
    )
    rest_full = lax.all_gather(rest_own, every, axis=0, tiled=True)

    def rest_block(index):
        return rest_full[:, index * model_width : (index + 1) * model_width]

    proj_full = rest_block(0)
    up_parts = [rest_block(1 + index) for index in range(BLOCKS)]
    down_parts = [rest_block(1 + BLOCKS + index) for index in range(BLOCKS)]

    inner_own = expert_in[0]
    outer_own = expert_out[0]
    inner_core = swap_core(inner_own)
    outer_core = swap_core(outer_own)
    inner_chip = swap_chip(inner_own)
    inner_both = swap_core(inner_chip)

    capacity = token_count // experts
    chosen = assignment.reshape(token_count)
    one_hot = (chosen[:, None] == jnp.arange(experts, dtype=jnp.int32)[None, :]).astype(jnp.int32)
    rank_within = jnp.sum((jnp.cumsum(one_hot, axis=0) - 1) * one_hot, axis=1)
    slot_index = chosen * capacity + rank_within
    source_of = (
        jnp.zeros((token_count,), jnp.int32)
        .at[slot_index]
        .set(jnp.arange(token_count, dtype=jnp.int32))
    )

    tokens_flat = block_input.reshape(token_count, model_width).astype(f32)
    normed_attn = layer_norm(tokens_flat, gain_attn).astype(bf16)
    kv_own = product(normed_attn, qkv_full[:, model_width:]).astype(bf16)
    kv_own = kv_own.reshape(row_count, local_len, 2 * model_width)
    query = product(normed_attn, qkv_full[:, :model_width]).astype(bf16)
    query = query.reshape(row_count, local_len, model_width)

    kv_far = seq_send(kv_own, [(0, 2), (1, 3)])
    kv_near = seq_send(
        jnp.where(seq_index == 3, kv_far, kv_own), [(0, 1), (2, 3), (3, 2)]
    )
    kv_blocks = (kv_own, kv_near, kv_far)
    outer_late, _ = lax.optimization_barrier((outer_own, kv_far))
    outer_chip = swap_chip(outer_late)
    outer_both = swap_core(outer_chip)

    before = 2 * local_len
    offset = seq_index * local_len
    padded_seg = jnp.pad(segment_ids, ((0, 0), (before, 0)), constant_values=-1)
    key_seg = lax.dynamic_slice_in_dim(padded_seg, offset, before + local_len, 1)
    query_seg = key_seg[:, before:]
    key_pos = jnp.arange(before + local_len)
    query_pos = before + jnp.arange(local_len)
    allowed = (key_seg[:, :, None] == query_seg[:, None, :]) & (
        key_pos[None, :, None] <= query_pos[None, None, :]
    )
    bias = jnp.where(allowed, 0.0, -1e30).astype(f32)

    attended_rows = attend(query, kv_blocks, bias)
    attended = attended_rows.reshape(token_count, model_width)
    hidden = tokens_flat + product(attended, proj_full)
    normed_ffn = layer_norm(hidden, gain_ffn).astype(bf16)
    dense_out, dense_kept = ffn_forward(normed_ffn, up_parts, down_parts, hidden)
    routed = dense_out.astype(bf16)

    received = lax.all_to_all(routed[source_of], "wide", split_axis=0, concat_axis=0, tiled=True)
    received_f = received.astype(f32)
    centroid_row = centroids[0]
    centroid_f = centroid_row.astype(f32)
    logit_row = jnp.dot(received, centroid_row, preferred_element_type=f32)
    gate_value = jax.nn.sigmoid(logit_row)
    gains_f = expert_norms[0].astype(f32)
    state_now = received_f
    kept_layers = []
    slices = []
    for sublayer in range(2):
        inner_parts = [part[sublayer] for part in (inner_own, inner_core, inner_chip, inner_both)]
        outer_parts = [part[sublayer] for part in (outer_own, outer_core, outer_chip, outer_both)]
        normed = layer_norm(state_now, gains_f[sublayer]).astype(bf16)
        state_next, kept = ffn_forward(normed, inner_parts, outer_parts, state_now)
        kept_layers.append((state_now, normed, kept))
        slices.append((inner_parts, outer_parts))
        state_now = state_next
    returned = (gate_value[:, None] * state_now).astype(bf16)
    back_rows = lax.all_to_all(returned, "wide", split_axis=0, concat_axis=0, tiled=True)
    output = (
        (dense_out + back_rows[slot_index].astype(f32)).astype(bf16).reshape(block_input.shape)
    )
    gate_sum = jnp.sum(gate_value)
    score_sum = jnp.sum(logit_row * logit_row)
    grad_flat = grad_out.reshape(token_count, model_width)
    grad_back = lax.all_to_all(
        grad_flat[source_of], "wide", split_axis=0, concat_axis=0, tiled=True
    )
    grad_ret = grad_back.astype(f32)
    grad_gate = jnp.sum(grad_ret * state_now, axis=-1)
    grad_state = grad_ret * gate_value[:, None]
    inner_grads = [None, None]
    outer_grads = [None, None]
    gain_grads = [None, None]
    for sublayer in (1, 0):
        state_in, normed_in, kept = kept_layers[sublayer]
        inner_parts, outer_parts = slices[sublayer]
        grad_branch = grad_state.astype(bf16)
        grad_pres, grad_normed = ffn_backward(kept, inner_parts, outer_parts, grad_branch)
        outer_grads[sublayer] = reduce_slices(
            *[functools.partial(product_at, act, grad_branch) for act, _ in kept]
        )
        inner_grads[sublayer] = reduce_slices(
            *[functools.partial(product_at, normed_in, grad_pre) for grad_pre in grad_pres]
        )
        grad_resid, gain_grad = norm_back(state_in, gains_f[sublayer], grad_normed)
        grad_state = grad_state + grad_resid
        gain_grads[sublayer] = gain_grad
    grad_logit = grad_gate * gate_value * (1.0 - gate_value)
    grad_routed = (grad_state + grad_logit[:, None] * centroid_f[None, :]).astype(bf16)
    centroid_grad = jnp.dot(grad_logit, received_f, precision=highest)
    returned_grad = lax.all_to_all(grad_routed, "wide", split_axis=0, concat_axis=0, tiled=True)
    grad_dense = grad_flat.astype(f32) + returned_grad[slot_index].astype(f32)

    grad_down_in = grad_dense.astype(bf16)
    grad_pres, grad_normed_ffn = ffn_backward(dense_kept, up_parts, down_parts, grad_down_in)
    grad_hidden_norm, grad_gain_ffn = norm_back(hidden, gain_ffn, grad_normed_ffn)
    grad_hidden = grad_dense + grad_hidden_norm
    grad_proj = grad_hidden.astype(bf16)
    rest_grad = jnp.concatenate(
        [product_at(attended, grad_proj).astype(bf16)]
        + [product_at(normed_ffn, grad_pre).astype(bf16) for grad_pre in grad_pres]
        + [product_at(act, grad_down_in).astype(bf16) for act, _ in dense_kept],
        axis=1,
    )
    rest_sum = lax.psum_scatter(rest_grad, every, scatter_dimension=0, tiled=True).astype(f32)
    grad_attended = product_bt(grad_proj, proj_full).astype(bf16)
    grad_query, grad_kv0, grad_kv1, grad_kv2 = attend_back(
        query, kv_blocks, bias, grad_attended.reshape(query.shape)
    )
    got_near = seq_send(grad_kv1, [(1, 0), (3, 2), (2, 3)])
    far_sum = jnp.where(
        seq_index == 3, (grad_kv2.astype(f32) + got_near.astype(f32)).astype(bf16), grad_kv2
    )
    got_far = seq_send(far_sum, [(2, 0), (3, 1)])
    kv_sum = grad_kv0.astype(f32) + got_far.astype(f32)
    kv_sum = kv_sum + jnp.where(seq_index % 2 == 0, got_near.astype(f32), 0.0)
    kv_sum = kv_sum.astype(bf16).reshape(2, token_count, model_width)
    grad_qkv = [grad_query.reshape(token_count, model_width), kv_sum[0], kv_sum[1]]
    qkv_grad = jnp.concatenate(
        [product_at(normed_attn, part).astype(bf16) for part in grad_qkv], axis=1
    )
    qkv_sum = lax.psum_scatter(qkv_grad, every, scatter_dimension=0, tiled=True).astype(f32)
    grad_normed_attn = sum(
        product_bt(part, qkv_full[:, index * model_width : (index + 1) * model_width])
        for index, part in enumerate(grad_qkv)
    )
    grad_input_norm, grad_gain_attn = norm_back(tokens_flat, gain_attn, grad_normed_attn)
    grad_input = (grad_hidden + grad_input_norm).reshape(block_input.shape)

    gain_terms = jnp.stack([grad_gain_attn, grad_gain_ffn]).reshape(2, devices, shard)
    gain_terms = lax.all_to_all(gain_terms.transpose(1, 0, 2), every, 0, 0, tiled=True)
    gain_sums = jnp.sum(gain_terms, axis=0)
    expert_totals = lax.psum(
        (jnp.stack(gain_grads), centroid_grad, jnp.stack([gate_sum, score_sum])), "seq"
    )
    up_grad = (
        rest_sum[:, model_width : model_width + hidden_width]
        .reshape(shard, BLOCKS, devices, shard)
        .transpose(0, 2, 1, 3)
        .reshape(shard, hidden_width)
    )
    down_grad = (
        rest_sum[:, model_width + hidden_width :]
        .reshape(shard, BLOCKS, model_width)
        .transpose(1, 0, 2)
        .reshape(BLOCKS * shard, model_width)
    )
    token_total = token_count * seq_devices
    return (
        output,
        grad_input,
        gain_sums[0],
        qkv_sum,
        rest_sum[:, :model_width],
        gain_sums[1],
        up_grad,
        down_grad,
        expert_totals[1][None],
        expert_totals[0][None],
        jnp.stack(inner_grads)[None],
        jnp.stack(outer_grads)[None],
        (expert_totals[2][0] / token_total)[None],
        (expert_totals[2][1] / token_total)[None],
    )


def solution(mesh):
    in_specs = (
        P("wide", "seq", None),
        P("wide", None),
        P("wide", "seq"),
        P(("seq", "wide")),
        P(("seq", "wide"), None),
        P(("seq", "wide"), None),
        P(("seq", "wide")),
        P(("seq", "wide"), None),
        P(("seq", "wide"), None),
        P("wide", None),
        P("wide", None, None),
        P("wide", None, None, "seq"),
        P("wide", None, "seq", None),
        P("wide", "seq", None),
    )
    out_specs = (
        P("wide", "seq", None),
        P("wide", "seq", None),
        P(("seq", "wide")),
        P(("seq", "wide"), None),
        P(("seq", "wide"), None),
        P(("seq", "wide")),
        P(("seq", "wide"), None),
        P(("seq", "wide"), None),
        P("wide", None),
        P("wide", None, None),
        P("wide", None, None, "seq"),
        P("wide", None, "seq", None),
        P("wide"),
        P("wide"),
    )
    return jax.shard_map(
        per_device, mesh=mesh, in_specs=in_specs, out_specs=out_specs, check_vma=False
    )
```

```python
import functools
import math

import jax
import jax.numpy as jnp
from jax import lax
from jax.experimental import pallas as pl
from jax.experimental.layout import Layout, with_layout_constraint
from jax.experimental.pallas import tpu as pltpu
from jax.sharding import PartitionSpec as P

HEADS = 16
HEAD_DIM = 64
BLOCKS = 4

epsilon = 1e-05
highest = lax.Precision.HIGHEST
bf16 = jnp.bfloat16
f32 = jnp.float32


def layer_norm(values, norm_gain):
    centered = values - jnp.mean(values, axis=-1, keepdims=True)
    variance = jnp.mean(centered * centered, axis=-1, keepdims=True)
    return centered * lax.rsqrt(variance + epsilon) * norm_gain


def norm_back(values, norm_gain, grad_normed):
    _, pull_back = jax.vjp(layer_norm, values, norm_gain)
    return pull_back(grad_normed)


def gelu_pair(values):
    cdf = 0.5 * (1.0 + lax.erf(values * math.sqrt(0.5)))
    density = jnp.exp(values * values * -0.5) * (1.0 / math.sqrt(2.0 * math.pi))
    return values * cdf, cdf + values * density


def product(left_side, right_side):
    return jnp.dot(left_side, right_side, preferred_element_type=f32)


def product_bt(left_side, right_side):
    return lax.dot_general(
        left_side, right_side, (((1,), (1,)), ((), ())), preferred_element_type=f32
    )


def product_at(left_side, right_side):
    return lax.dot_general(
        left_side, right_side, (((0,), (0,)), ((), ())), preferred_element_type=f32
    )


def row_major(values):
    return with_layout_constraint(values, Layout(major_to_minor=(0, 1)))


def weight_grad(left_side, right_side):
    return row_major(product_at(left_side, right_side).astype(bf16))


def seq_send(values, pairs):
    return lax.ppermute(values, "seq", pairs)


def swap_core(values):
    return seq_send(values, [(0, 1), (1, 0), (2, 3), (3, 2)])


def swap_chip(values):
    return seq_send(values, [(0, 2), (2, 0), (1, 3), (3, 1)])


def pair_probs(query, keys, bias, score_scale):
    scores = product_bt(keys, query) * score_scale + bias
    exp_scores = jnp.exp(scores - jnp.max(scores, axis=0, keepdims=True))
    return exp_scores * (1.0 / jnp.sum(exp_scores, axis=0, keepdims=True))


def attend_kernel(score_scale, q_ref, k0, v0, k1, v1, k2, v2, bias_ref, out_ref):
    bias = bias_ref[0]
    parts = []
    for head in range(2):
        cols = slice(head * HEAD_DIM, (head + 1) * HEAD_DIM)
        keys = jnp.concatenate([k2[0][:, cols], k1[0][:, cols], k0[0][:, cols]], axis=0)
        vals = jnp.concatenate([v2[0][:, cols], v1[0][:, cols], v0[0][:, cols]], axis=0)
        probs_low = pair_probs(q_ref[0][:, cols], keys, bias, score_scale).astype(bf16)
        parts.append(product_at(vals, probs_low))
    out_ref[0] = jnp.concatenate(parts, axis=0).T.astype(bf16)


def attend_back_kernel(
    score_scale, q_ref, k0, v0, k1, v1, k2, v2, bias_ref, grad_ref, dq_ref, d0, d1, d2
):
    bias = bias_ref[0]
    dq_parts, dk_parts, dv_parts = [], [], []
    for head in range(2):
        cols = slice(head * HEAD_DIM, (head + 1) * HEAD_DIM)
        query = q_ref[0][:, cols]
        grad_att = grad_ref[0][:, cols]
        keys = jnp.concatenate([k2[0][:, cols], k1[0][:, cols], k0[0][:, cols]], axis=0)
        vals = jnp.concatenate([v2[0][:, cols], v1[0][:, cols], v0[0][:, cols]], axis=0)
        probs = pair_probs(query, keys, bias, score_scale)
        grad_probs = product_bt(vals, grad_att)
        dv_parts.append(product(probs.astype(bf16), grad_att))
        inner_sum = jnp.sum(probs * grad_probs, axis=0, keepdims=True)
        grad_scores = (probs * (grad_probs - inner_sum)).astype(bf16)
        dk_parts.append(product(grad_scores, query) * score_scale)
        dq_parts.append(product_at(keys, grad_scores) * score_scale)
    dq_ref[0] = jnp.concatenate(dq_parts, axis=0).T.astype(bf16)
    d_keys = jnp.concatenate(dk_parts, axis=1).astype(bf16)
    d_vals = jnp.concatenate(dv_parts, axis=1).astype(bf16)
    size = d_keys.shape[0] // 3
    for place, ref in enumerate((d2, d1, d0)):
        ref[0, 0] = d_keys[place * size : (place + 1) * size]
        ref[1, 0] = d_vals[place * size : (place + 1) * size]


def attention_specs(local_len, model_width, key_len):
    width = 2 * HEAD_DIM
    groups = model_width // width
    query = pl.BlockSpec((1, local_len, width), lambda row, head: (row, 0, head))
    values = pl.BlockSpec((1, local_len, width), lambda row, head: (row, 0, head + groups))
    bias = pl.BlockSpec((1, key_len, local_len), lambda row, head: (row, 0, 0))
    return groups, query, [query, query, values, query, values, query, values, bias]


def attend(query, kv_blocks, bias):
    rows, local_len, model_width = query.shape
    groups, spec, in_specs = attention_specs(local_len, model_width, bias.shape[1])
    operands = [block for block in kv_blocks for _ in range(2)]
    flops = 4 * rows * model_width * local_len * bias.shape[1]
    return pl.pallas_call(
        functools.partial(attend_kernel, 1.0 / math.sqrt(HEAD_DIM)),
        grid=(rows, groups),
        in_specs=in_specs,
        out_specs=spec,
        out_shape=jax.ShapeDtypeStruct(query.shape, bf16),
        cost_estimate=pl.CostEstimate(
            flops=flops * 6, bytes_accessed=8 * query.size * 2, transcendentals=0
        ),
        name="attend",
    )(query, *operands, bias)


def attend_back(query, kv_blocks, bias, grad_attended):
    rows, local_len, model_width = query.shape
    groups, spec, in_specs = attention_specs(local_len, model_width, bias.shape[1])
    operands = [block for block in kv_blocks for _ in range(2)]
    pair_spec = pl.BlockSpec((2, 1, local_len, 2 * HEAD_DIM), lambda row, head: (0, row, 0, head))
    pair_shape = jax.ShapeDtypeStruct((2, rows, local_len, model_width), bf16)
    flops = 10 * rows * model_width * local_len * bias.shape[1]
    return pl.pallas_call(
        functools.partial(attend_back_kernel, 1.0 / math.sqrt(HEAD_DIM)),
        grid=(rows, groups),
        in_specs=in_specs + [spec],
        out_specs=[spec, pair_spec, pair_spec, pair_spec],
        out_shape=[jax.ShapeDtypeStruct(query.shape, bf16)] + [pair_shape] * 3,
        cost_estimate=pl.CostEstimate(
            flops=flops * 6, bytes_accessed=16 * query.size * 2, transcendentals=0
        ),
        name="attend_back",
    )(query, *operands, bias, grad_attended)


def ffn_forward(normed, inner_parts, outer_parts, residual):
    kept = []
    total = residual
    for inner, outer in zip(inner_parts, outer_parts):
        act, slope = gelu_pair(product(normed, inner))
        act = act.astype(bf16)
        kept.append((act, slope.astype(bf16)))
        total = total + product(act, outer)
    return total, kept


def ffn_backward(kept, inner_parts, outer_parts, grad_branch):
    grad_pres = []
    grad_normed = None
    for (act, slope), inner, outer in zip(kept, inner_parts, outer_parts):
        grad_pre = (product_bt(grad_branch, outer) * slope.astype(f32)).astype(bf16)
        grad_pres.append(grad_pre)
        piece = product_bt(grad_pre, inner)
        grad_normed = piece if grad_normed is None else grad_normed + piece
    return grad_pres, grad_normed


class SliceSum:
    def __init__(self, operands):
        self.operands = operands

    def terms(self):
        return [weight_grad(left, right) for left, right in self.operands]

    def send_core(self, terms):
        self.own, core, self.chip, both = terms
        self.got_core = swap_core(core)
        self.got_both = swap_core(both)

    def chip_sum(self):
        return (self.chip.astype(f32) + self.got_both.astype(f32)).astype(bf16)

    def send_chip(self, values):
        self.got_chip = swap_chip(values)

    def total(self):
        return self.own.astype(f32) + self.got_core.astype(f32) + self.got_chip.astype(f32)


def cube_bits():
    bits = []
    for axis in ("seq", "wide"):
        count = lax.axis_size(axis).bit_length() - 1
        bits += [(axis, bit) for bit in reversed(range(count))]
    return bits


def cube_orders(bits):
    core = bits.index(("seq", 0))
    chip = bits.index(("seq", 1))
    wide = [place for place, (axis, _) in enumerate(bits) if axis == "wide"]
    if len(wide) == 3:
        far, near, across = wide
        return (
            (far, chip, near, across, core),
            (near, across, far, chip, core),
            (chip, far, across, near, core),
        )
    return (
        (chip, *wide, core),
        (*wide, chip, core),
        (*wide[1:], chip, wide[0], core),
    )


def cube_place(bits):
    index = {axis: lax.axis_index(axis) for axis in ("seq", "wide")}
    mine = [lax.rem(index[axis] // (1 << bit), 2) for axis, bit in bits]

    def partner(place):
        axis, bit = bits[place]
        other = dict(index)
        other[axis] = index[axis] + (1 - 2 * mine[place]) * (1 << bit)
        return (other["seq"], other["wide"])

    return mine, partner


def cube_barrier(bits, partner):
    barrier = pltpu.get_barrier_semaphore()
    for place in range(len(bits)):
        pl.semaphore_signal(
            barrier, inc=1, device_id=partner(place), device_id_type=pl.DeviceIdType.MESH
        )
    pl.semaphore_wait(barrier, len(bits))


def gather_kernel(bits, orders, own_ref, out_ref, send_sem, recv_sem, copy_sem):
    mine, partner = cube_place(bits)
    own_copy = pltpu.make_async_copy(own_ref, out_ref.at[tuple(mine)], copy_sem)
    own_copy.start()
    cube_barrier(bits, partner)
    own_copy.wait()
    width = own_ref.shape[1] // len(orders)
    copies = []
    held = [[False] * len(bits) for _ in orders]
    for stage in range(len(bits)):
        for color, order in enumerate(orders):
            if stage:
                copies[(stage - 1) * len(orders) + color].wait_recv()
                held[color][order[stage - 1]] = True
            place = tuple(
                slice(None) if whole else mine[axis] for axis, whole in enumerate(held[color])
            )
            ref = out_ref.at[place + (slice(None), pl.ds(color * width, width))]
            copy = pltpu.make_async_remote_copy(
                src_ref=ref,
                dst_ref=ref,
                send_sem=send_sem.at[color, stage],
                recv_sem=recv_sem.at[color, stage],
                device_id=partner(order[stage]),
                device_id_type=pl.DeviceIdType.MESH,
            )
            copy.start()
            copies.append(copy)
    for copy in copies:
        copy.wait_send()
    for copy in copies[-len(orders) :]:
        copy.wait_recv()


def gather_rows(own):
    bits = cube_bits()
    orders = cube_orders(bits)
    rows, width = own.shape
    out = pl.pallas_call(
        functools.partial(gather_kernel, bits, orders),
        in_specs=[pl.BlockSpec(memory_space=pltpu.VMEM)],
        out_specs=pl.BlockSpec(memory_space=pl.ANY),
        out_shape=jax.ShapeDtypeStruct((2,) * len(bits) + (rows, width), own.dtype),
        scratch_shapes=[
            pltpu.SemaphoreType.DMA((len(orders), len(bits))),
            pltpu.SemaphoreType.DMA((len(orders), len(bits))),
            pltpu.SemaphoreType.DMA,
        ],
        compiler_params=pltpu.CompilerParams(collective_id=0, has_side_effects=True),
        name="gather_rows",
    )(own)
    return out.reshape(rows << len(bits), width)


def scatter_kernel(bits, orders, terms_ref, out_ref, *scratch):
    stages = len(bits)
    colors = len(orders)
    got = scratch[: colors * stages]
    sums = scratch[colors * stages : colors * (2 * stages - 1)]
    send_sem, recv_sem = scratch[colors * (2 * stages - 1) :]
    mine, partner = cube_place(bits)
    cube_barrier(bits, partner)
    width = terms_ref.shape[-1] // colors
    copies = []

    def half(color, stage, keep):
        done = orders[color][:stage]
        place = []
        for axis in range(stages):
            if axis in done:
                continue
            if axis == orders[color][stage]:
                place.append(mine[axis] if keep else 1 - mine[axis])
            else:
                place.append(slice(None))
        if stage == 0:
            return terms_ref.at[tuple(place) + (slice(None), pl.ds(color * width, width))]
        return sums[color * (stages - 1) + stage - 1].at[tuple(place)]

    for stage in range(stages + 1):
        for color in range(colors):
            if stage:
                copies[(stage - 1) * colors + color].wait_recv()
                kept = half(color, stage - 1, True)[...].astype(f32)
                total = kept + got[color * stages + stage - 1][...].astype(f32)
                if stage == stages:
                    out_ref[:, pl.ds(color * width, width)] = total
                    continue
                sums[color * (stages - 1) + stage - 1][...] = total.astype(bf16)
            copy = pltpu.make_async_remote_copy(
                src_ref=half(color, stage, False),
                dst_ref=got[color * stages + stage],
                send_sem=send_sem.at[color, stage],
                recv_sem=recv_sem.at[color, stage],
                device_id=partner(orders[color][stage]),
                device_id_type=pl.DeviceIdType.MESH,
            )
            copy.start()
            copies.append(copy)
    for copy in copies:
        copy.wait_send()


def scatter_rows(terms):
    bits = cube_bits()
    orders = [order[::-1] for order in cube_orders(bits)]
    colors = len(orders)
    stages = len(bits)
    rows = terms.shape[0] >> stages
    width = terms.shape[1]
    got = [
        pltpu.VMEM((2,) * (stages - 1 - stage) + (rows, width // colors), bf16)
        for _ in range(colors)
        for stage in range(stages)
    ]
    sums = [
        pltpu.VMEM((2,) * (stages - 1 - stage) + (rows, width // colors), bf16)
        for _ in range(colors)
        for stage in range(stages - 1)
    ]
    return pl.pallas_call(
        functools.partial(scatter_kernel, bits, orders),
        in_specs=[pl.BlockSpec(memory_space=pltpu.VMEM)],
        out_specs=pl.BlockSpec(memory_space=pltpu.VMEM),
        out_shape=jax.ShapeDtypeStruct((rows, width), f32),
        scratch_shapes=got
        + sums
        + [
            pltpu.SemaphoreType.DMA((colors, stages)),
            pltpu.SemaphoreType.DMA((colors, stages)),
        ],
        compiler_params=pltpu.CompilerParams(collective_id=1, has_side_effects=True),
        name="scatter_rows",
    )(terms.reshape((2,) * stages + (rows, width)))


def together(*values):
    return lax.optimization_barrier(values)


def per_device(
    block_input,
    segment_ids,
    assignment,
    norm_attn,
    weight_qkv,
    weight_proj,
    norm_ffn,
    weight_up,
    weight_down,
    centroids,
    expert_norms,
    expert_in,
    expert_out,
    grad_out,
):
    row_count, local_len, model_width = block_input.shape
    token_count = row_count * local_len
    seq_devices = lax.axis_size("seq")
    seq_index = lax.axis_index("seq")
    experts = lax.axis_size("wide")
    devices = seq_devices * experts
    every = ("seq", "wide")
    shard = weight_up.shape[0]
    hidden_width = weight_up.shape[1]

    gains_own = jnp.stack([norm_attn, norm_ffn]).astype(f32)
    gains_all = lax.all_to_all(
        jnp.broadcast_to(gains_own[None], (devices, 2, shard)), every, 0, 0, tiled=True
    )
    gains_all = gains_all.transpose(1, 0, 2).reshape(2, model_width)
    gain_attn = gains_all[0]
    gain_ffn = gains_all[1]

    qkv_full = gather_rows(weight_qkv)
    up_own = (
        weight_up.reshape(shard, devices, BLOCKS, shard)
        .transpose(0, 2, 1, 3)
        .reshape(shard, hidden_width)
    )
    down_own = weight_down.reshape(BLOCKS, shard, model_width).transpose(1, 0, 2)
    rest_own = jnp.concatenate(
        [weight_proj, up_own, down_own.reshape(shard, BLOCKS * model_width)], axis=1
    )
    rest_full = lax.all_gather(rest_own, every, axis=0, tiled=True)

    def rest_block(index):
        return rest_full[:, index * model_width : (index + 1) * model_width]

    proj_full = rest_block(0)
    up_parts = [rest_block(1 + index) for index in range(BLOCKS)]
    down_parts = [rest_block(1 + BLOCKS + index) for index in range(BLOCKS)]

    inner_own = expert_in[0]
    outer_own = expert_out[0]
    inner_core = swap_core(inner_own)
    outer_core = swap_core(outer_own)
    inner_chip = [swap_chip(inner_own[0]), None]
    outer_chip = [None, None]

    capacity = token_count // experts
    chosen = assignment.reshape(token_count)
    one_hot = (chosen[:, None] == jnp.arange(experts, dtype=jnp.int32)[None, :]).astype(jnp.int32)
    rank_within = jnp.sum((jnp.cumsum(one_hot, axis=0) - 1) * one_hot, axis=1)
    slot_index = chosen * capacity + rank_within
    source_of = (
        jnp.zeros((token_count,), jnp.int32)
        .at[slot_index]
        .set(jnp.arange(token_count, dtype=jnp.int32))
    )

    tokens_flat = block_input.reshape(token_count, model_width).astype(f32)
    normed_attn = layer_norm(tokens_flat, gain_attn).astype(bf16)
    kv_own = product(normed_attn, qkv_full[:, model_width:]).astype(bf16)
    kv_own = kv_own.reshape(row_count, local_len, 2 * model_width)
    query = product(normed_attn, qkv_full[:, :model_width]).astype(bf16)
    query = query.reshape(row_count, local_len, model_width)

    kv_far = seq_send(kv_own, [(0, 2), (1, 3)])
    kv_near = seq_send(
        jnp.where(seq_index == 3, kv_far, kv_own), [(0, 1), (2, 3), (3, 2)]
    )
    kv_blocks = (kv_own, kv_near, kv_far)
    late = together(outer_own[0], inner_own[1], outer_own[1], kv_far)
    outer_chip[0], inner_chip[1], outer_chip[1] = [swap_chip(part) for part in late[:3]]

    before = 2 * local_len
    offset = seq_index * local_len
    padded_seg = jnp.pad(segment_ids, ((0, 0), (before, 0)), constant_values=-1)
    key_seg = lax.dynamic_slice_in_dim(padded_seg, offset, before + local_len, 1)
    query_seg = key_seg[:, before:]
    key_pos = jnp.arange(before + local_len)
    query_pos = before + jnp.arange(local_len)
    allowed = (key_seg[:, :, None] == query_seg[:, None, :]) & (
        key_pos[None, :, None] <= query_pos[None, None, :]
    )
    bias = jnp.where(allowed, 0.0, -1e30).astype(f32)

    attended_rows = attend(query, kv_blocks, bias)
    attended = attended_rows.reshape(token_count, model_width)
    hidden = tokens_flat + product(attended, proj_full)
    normed_ffn = layer_norm(hidden, gain_ffn).astype(bf16)
    dense_out, dense_kept = ffn_forward(normed_ffn, up_parts, down_parts, hidden)
    routed = dense_out.astype(bf16)

    received = lax.all_to_all(routed[source_of], "wide", split_axis=0, concat_axis=0, tiled=True)
    received_f = received.astype(f32)
    inner_both = [swap_core(together(inner_chip[0], attended)[0]), None]
    outer_both = [swap_core(together(outer_chip[0], received)[0]), None]
    inner_both[1] = swap_core(together(inner_chip[1], received)[0])
    outer_both[1] = swap_core(together(outer_chip[1], received)[0])
    centroid_row = centroids[0]
    centroid_f = centroid_row.astype(f32)
    logit_row = jnp.dot(received, centroid_row, preferred_element_type=f32)
    gate_value = jax.nn.sigmoid(logit_row)
    gains_f = expert_norms[0].astype(f32)
    state_now = received_f
    kept_layers = []
    slices = []
    for sublayer in range(2):
        inner_parts = [part[sublayer] for part in (inner_own, inner_core, inner_chip, inner_both)]
        outer_parts = [part[sublayer] for part in (outer_own, outer_core, outer_chip, outer_both)]
        normed = layer_norm(state_now, gains_f[sublayer]).astype(bf16)
        state_next, kept = ffn_forward(normed, inner_parts, outer_parts, state_now)
        kept_layers.append((state_now, normed, kept))
        slices.append((inner_parts, outer_parts))
        state_now = state_next
    returned = (gate_value[:, None] * state_now).astype(bf16)
    back_rows = lax.all_to_all(returned, "wide", split_axis=0, concat_axis=0, tiled=True)
    output = (
        (dense_out + back_rows[slot_index].astype(f32)).astype(bf16).reshape(block_input.shape)
    )
    gate_sum = jnp.sum(gate_value)
    score_sum = jnp.sum(logit_row * logit_row)
    grad_flat = grad_out.reshape(token_count, model_width)
    grad_back = lax.all_to_all(
        grad_flat[source_of], "wide", split_axis=0, concat_axis=0, tiled=True
    )
    grad_ret = grad_back.astype(f32)
    grad_gate = jnp.sum(grad_ret * state_now, axis=-1)
    grad_state = grad_ret * gate_value[:, None]
    gain_grads = [None, None]
    weight_terms = [None, None]
    for sublayer in (1, 0):
        state_in, normed_in, kept = kept_layers[sublayer]
        inner_parts, outer_parts = slices[sublayer]
        grad_branch = grad_state.astype(bf16)
        grad_pres, grad_normed = ffn_backward(kept, inner_parts, outer_parts, grad_branch)
        weight_terms[sublayer] = (
            [(act, grad_branch) for act, _ in kept],
            [(normed_in, grad_pre) for grad_pre in grad_pres],
        )
        grad_resid, gain_grad = norm_back(state_in, gains_f[sublayer], grad_normed)
        grad_state = grad_state + grad_resid
        gain_grads[sublayer] = gain_grad
    grad_logit = grad_gate * gate_value * (1.0 - gate_value)
    grad_routed = (grad_state + grad_logit[:, None] * centroid_f[None, :]).astype(bf16)
    centroid_grad = jnp.dot(grad_logit, received_f, precision=highest)
    returned_grad = lax.all_to_all(grad_routed, "wide", split_axis=0, concat_axis=0, tiled=True)
    outer_sum1 = SliceSum(weight_terms[1][0])
    inner_sum1 = SliceSum(weight_terms[1][1])
    returned_grad, *held = together(returned_grad, *outer_sum1.terms(), *inner_sum1.terms())
    outer_sum1.send_core(held[:4])
    inner_sum1.send_core(held[4:])
    grad_dense = grad_flat.astype(f32) + returned_grad[slot_index].astype(f32)

    grad_down_in = grad_dense.astype(bf16)
    grad_pres, grad_normed_ffn = ffn_backward(dense_kept, up_parts, down_parts, grad_down_in)
    grad_hidden_norm, grad_gain_ffn = norm_back(hidden, gain_ffn, grad_normed_ffn)
    grad_hidden = grad_dense + grad_hidden_norm
    grad_proj = grad_hidden.astype(bf16)
    rest_grad = jnp.concatenate(
        [weight_grad(attended, grad_proj)]
        + [weight_grad(normed_ffn, grad_pre) for grad_pre in grad_pres]
        + [weight_grad(act, grad_down_in) for act, _ in dense_kept],
        axis=1,
    )
    rest_grad = row_major(rest_grad)
    grad_attended = product_bt(grad_proj, proj_full).astype(bf16)
    grad_attended, rest_grad, *held = together(
        grad_attended, rest_grad, outer_sum1.chip_sum(), inner_sum1.chip_sum()
    )
    outer_sum1.send_chip(held[0])
    inner_sum1.send_chip(held[1])
    rest_sum = lax.psum_scatter(rest_grad, every, scatter_dimension=0, tiled=True).astype(f32)
    grad_query, grad_kv0, grad_kv1, grad_kv2 = attend_back(
        query, kv_blocks, bias, grad_attended.reshape(query.shape)
    )
    got_near = seq_send(grad_kv1, [(1, 0), (3, 2), (2, 3)])
    far_sum = jnp.where(
        seq_index == 3, (grad_kv2.astype(f32) + got_near.astype(f32)).astype(bf16), grad_kv2
    )
    far_sum, outer_sum1.got_chip, inner_sum1.got_chip = together(
        far_sum, outer_sum1.got_chip, inner_sum1.got_chip
    )
    got_far = seq_send(far_sum, [(2, 0), (3, 1)])
    outer_sum0 = SliceSum(weight_terms[0][0])
    inner_sum0 = SliceSum(weight_terms[0][1])
    got_far, *held = together(got_far, *outer_sum0.terms(), *inner_sum0.terms())
    outer_sum0.send_core(held[:4])
    inner_sum0.send_core(held[4:])
    outer_sum0.send_chip(outer_sum0.chip_sum())
    inner_sum0.send_chip(inner_sum0.chip_sum())
    kv_sum = grad_kv0.astype(f32) + got_far.astype(f32)
    kv_sum = kv_sum + jnp.where(seq_index % 2 == 0, got_near.astype(f32), 0.0)
    kv_sum = kv_sum.astype(bf16).reshape(2, token_count, model_width)
    grad_qkv = [grad_query.reshape(token_count, model_width), kv_sum[0], kv_sum[1]]
    qkv_grad = row_major(
        jnp.concatenate([weight_grad(normed_attn, part) for part in grad_qkv], axis=1)
    )
    grad_normed_attn = sum(
        product_bt(part, qkv_full[:, index * model_width : (index + 1) * model_width])
        for index, part in enumerate(grad_qkv)
    )
    grad_input_norm, grad_gain_attn = norm_back(tokens_flat, gain_attn, grad_normed_attn)
    grad_input = (grad_hidden + grad_input_norm).reshape(block_input.shape)

    gain_terms = jnp.stack([grad_gain_attn, grad_gain_ffn]).reshape(2, devices, shard)
    gain_terms, qkv_grad = together(gain_terms.transpose(1, 0, 2), qkv_grad)
    gain_terms = lax.all_to_all(gain_terms, every, 0, 0, tiled=True)
    qkv_sum = scatter_rows(qkv_grad)
    gain_sums = jnp.sum(gain_terms, axis=0)
    expert_totals = lax.psum(
        (jnp.stack(gain_grads), centroid_grad, jnp.stack([gate_sum, score_sum])), "seq"
    )
    up_grad = (
        rest_sum[:, model_width : model_width + hidden_width]
        .reshape(shard, BLOCKS, devices, shard)
        .transpose(0, 2, 1, 3)
        .reshape(shard, hidden_width)
    )
    down_grad = (
        rest_sum[:, model_width + hidden_width :]
        .reshape(shard, BLOCKS, model_width)
        .transpose(1, 0, 2)
        .reshape(BLOCKS * shard, model_width)
    )
    token_total = token_count * seq_devices
    return (
        output,
        grad_input,
        gain_sums[0],
        qkv_sum,
        rest_sum[:, :model_width],
        gain_sums[1],
        up_grad,
        down_grad,
        expert_totals[1][None],
        expert_totals[0][None],
        jnp.stack([inner_sum0.total(), inner_sum1.total()])[None],
        jnp.stack([outer_sum0.total(), outer_sum1.total()])[None],
        (expert_totals[2][0] / token_total)[None],
        (expert_totals[2][1] / token_total)[None],
    )


def solution(mesh):
    in_specs = (
        P("wide", "seq", None),
        P("wide", None),
        P("wide", "seq"),
        P(("seq", "wide")),
        P(("seq", "wide"), None),
        P(("seq", "wide"), None),
        P(("seq", "wide")),
        P(("seq", "wide"), None),
        P(("seq", "wide"), None),
        P("wide", None),
        P("wide", None, None),
        P("wide", None, None, "seq"),
        P("wide", None, "seq", None),
        P("wide", "seq", None),
    )
    out_specs = (
        P("wide", "seq", None),
        P("wide", "seq", None),
        P(("seq", "wide")),
        P(("seq", "wide"), None),
        P(("seq", "wide"), None),
        P(("seq", "wide")),
        P(("seq", "wide"), None),
        P(("seq", "wide"), None),
        P("wide", None),
        P("wide", None, None),
        P("wide", None, None, "seq"),
        P("wide", None, "seq", None),
        P("wide"),
        P("wide"),
    )
    return jax.shard_map(
        per_device, mesh=mesh, in_specs=in_specs, out_specs=out_specs, check_vma=False
    )
```

```python
import functools
import math

import jax
import jax.numpy as jnp
from jax import lax
from jax.experimental import pallas as pl
from jax.experimental.layout import Layout, with_layout_constraint
from jax.experimental.pallas import tpu as pltpu
from jax.sharding import PartitionSpec as P

HEADS = 16
HEAD_DIM = 64
BLOCKS = 4

epsilon = 1e-05
highest = lax.Precision.HIGHEST
bf16 = jnp.bfloat16
f32 = jnp.float32


def layer_norm(values, norm_gain):
    centered = values - jnp.mean(values, axis=-1, keepdims=True)
    variance = jnp.mean(centered * centered, axis=-1, keepdims=True)
    return centered * lax.rsqrt(variance + epsilon) * norm_gain


def norm_back(values, norm_gain, grad_normed):
    _, pull_back = jax.vjp(layer_norm, values, norm_gain)
    return pull_back(grad_normed)


def gelu_pair(values):
    cdf = 0.5 * (1.0 + lax.erf(values * math.sqrt(0.5)))
    density = jnp.exp(values * values * -0.5) * (1.0 / math.sqrt(2.0 * math.pi))
    return values * cdf, cdf + values * density


def product(left_side, right_side):
    return jnp.dot(left_side, right_side, preferred_element_type=f32)


def product_bt(left_side, right_side):
    return lax.dot_general(
        left_side, right_side, (((1,), (1,)), ((), ())), preferred_element_type=f32
    )


def product_at(left_side, right_side):
    return lax.dot_general(
        left_side, right_side, (((0,), (0,)), ((), ())), preferred_element_type=f32
    )


def row_major(values):
    return with_layout_constraint(values, Layout(major_to_minor=(0, 1)))


def weight_grad(left_side, right_side):
    return row_major(product_at(left_side, right_side).astype(bf16))


def seq_send(values, pairs):
    return lax.ppermute(values, "seq", pairs)


def swap_core(values):
    return seq_send(values, [(0, 1), (1, 0), (2, 3), (3, 2)])


def swap_chip(values):
    return seq_send(values, [(0, 2), (2, 0), (1, 3), (3, 1)])


def pair_probs(query, keys, bias, score_scale):
    scores = product_bt(keys, query) * score_scale + bias
    exp_scores = jnp.exp(scores - jnp.max(scores, axis=0, keepdims=True))
    return exp_scores * (1.0 / jnp.sum(exp_scores, axis=0, keepdims=True))


def ride_chip(source, target, send_sem, recv_sem):
    seq = lax.axis_index("seq")
    other = (lax.rem(seq + 2, 4), lax.axis_index("wide"))
    step = pl.program_id(0) * pl.num_programs(1) + pl.program_id(1)
    copy = pltpu.make_async_remote_copy(
        src_ref=source,
        dst_ref=target,
        send_sem=send_sem,
        recv_sem=recv_sem,
        device_id=other,
        device_id_type=pl.DeviceIdType.MESH,
    )

    @pl.when(step == 0)
    def _():
        barrier = pltpu.get_barrier_semaphore()
        pl.semaphore_signal(
            barrier, inc=1, device_id=other, device_id_type=pl.DeviceIdType.MESH
        )
        pl.semaphore_wait(barrier, 1)
        copy.start()

    @pl.when(step == pl.num_programs(0) * pl.num_programs(1) - 1)
    def _():
        copy.wait()


def attend_kernel(
    score_scale,
    q_ref,
    k0,
    v0,
    k1,
    v1,
    k2,
    v2,
    bias_ref,
    ride_ref,
    out_ref,
    rode_ref,
    send_sem,
    recv_sem,
):
    ride_chip(ride_ref.at[0], rode_ref, send_sem, recv_sem)
    bias = bias_ref[0]
    parts = []
    for head in range(2):
        cols = slice(head * HEAD_DIM, (head + 1) * HEAD_DIM)
        keys = jnp.concatenate([k2[0][:, cols], k1[0][:, cols], k0[0][:, cols]], axis=0)
        vals = jnp.concatenate([v2[0][:, cols], v1[0][:, cols], v0[0][:, cols]], axis=0)
        probs_low = pair_probs(q_ref[0][:, cols], keys, bias, score_scale).astype(bf16)
        parts.append(product_at(vals, probs_low))
    out_ref[0] = jnp.concatenate(parts, axis=0).T.astype(bf16)


def attend_back_kernel(
    score_scale,
    q_ref,
    k0,
    v0,
    k1,
    v1,
    k2,
    v2,
    bias_ref,
    grad_ref,
    ride_ref,
    dq_ref,
    d0,
    d1,
    d2,
    rode_ref,
    send_sem,
    recv_sem,
):
    ride_chip(ride_ref, rode_ref, send_sem, recv_sem)
    bias = bias_ref[0]
    dq_parts, dk_parts, dv_parts = [], [], []
    for head in range(2):
        cols = slice(head * HEAD_DIM, (head + 1) * HEAD_DIM)
        query = q_ref[0][:, cols]
        grad_att = grad_ref[0][:, cols]
        keys = jnp.concatenate([k2[0][:, cols], k1[0][:, cols], k0[0][:, cols]], axis=0)
        vals = jnp.concatenate([v2[0][:, cols], v1[0][:, cols], v0[0][:, cols]], axis=0)
        probs = pair_probs(query, keys, bias, score_scale)
        grad_probs = product_bt(vals, grad_att)
        dv_parts.append(product(probs.astype(bf16), grad_att))
        inner_sum = jnp.sum(probs * grad_probs, axis=0, keepdims=True)
        grad_scores = (probs * (grad_probs - inner_sum)).astype(bf16)
        dk_parts.append(product(grad_scores, query) * score_scale)
        dq_parts.append(product_at(keys, grad_scores) * score_scale)
    dq_ref[0] = jnp.concatenate(dq_parts, axis=0).T.astype(bf16)
    d_keys = jnp.concatenate(dk_parts, axis=1).astype(bf16)
    d_vals = jnp.concatenate(dv_parts, axis=1).astype(bf16)
    size = d_keys.shape[0] // 3
    for place, ref in enumerate((d2, d1, d0)):
        ref[0, 0] = d_keys[place * size : (place + 1) * size]
        ref[1, 0] = d_vals[place * size : (place + 1) * size]


def attention_specs(local_len, model_width, key_len):
    width = 2 * HEAD_DIM
    groups = model_width // width
    query = pl.BlockSpec((1, local_len, width), lambda row, head: (row, 0, head))
    values = pl.BlockSpec((1, local_len, width), lambda row, head: (row, 0, head + groups))
    bias = pl.BlockSpec((1, key_len, local_len), lambda row, head: (row, 0, 0))
    return groups, query, [query, query, values, query, values, query, values, bias]


def attend(query, kv_blocks, bias, ride):
    rows, local_len, model_width = query.shape
    groups, spec, in_specs = attention_specs(local_len, model_width, bias.shape[1])
    operands = [block for block in kv_blocks for _ in range(2)]
    flops = 4 * rows * model_width * local_len * bias.shape[1]
    return pl.pallas_call(
        functools.partial(attend_kernel, 1.0 / math.sqrt(HEAD_DIM)),
        grid=(rows, groups),
        in_specs=in_specs + [pl.BlockSpec(memory_space=pl.ANY)],
        out_specs=[spec, pl.BlockSpec(memory_space=pl.ANY)],
        out_shape=[
            jax.ShapeDtypeStruct(query.shape, bf16),
            jax.ShapeDtypeStruct(ride.shape[1:], ride.dtype),
        ],
        scratch_shapes=[pltpu.SemaphoreType.DMA, pltpu.SemaphoreType.DMA],
        compiler_params=pltpu.CompilerParams(collective_id=2, has_side_effects=True),
        cost_estimate=pl.CostEstimate(
            flops=flops * 6, bytes_accessed=8 * query.size * 2, transcendentals=0
        ),
        name="attend",
    )(query, *operands, bias, ride)


def attend_back(query, kv_blocks, bias, grad_attended, ride):
    rows, local_len, model_width = query.shape
    groups, spec, in_specs = attention_specs(local_len, model_width, bias.shape[1])
    operands = [block for block in kv_blocks for _ in range(2)]
    pair_spec = pl.BlockSpec((2, 1, local_len, 2 * HEAD_DIM), lambda row, head: (0, row, 0, head))
    pair_shape = jax.ShapeDtypeStruct((2, rows, local_len, model_width), bf16)
    flops = 10 * rows * model_width * local_len * bias.shape[1]
    return pl.pallas_call(
        functools.partial(attend_back_kernel, 1.0 / math.sqrt(HEAD_DIM)),
        grid=(rows, groups),
        in_specs=in_specs + [spec, pl.BlockSpec(memory_space=pl.ANY)],
        out_specs=[spec, pair_spec, pair_spec, pair_spec, pl.BlockSpec(memory_space=pl.ANY)],
        out_shape=[jax.ShapeDtypeStruct(query.shape, bf16)]
        + [pair_shape] * 3
        + [jax.ShapeDtypeStruct(ride.shape, ride.dtype)],
        scratch_shapes=[pltpu.SemaphoreType.DMA, pltpu.SemaphoreType.DMA],
        compiler_params=pltpu.CompilerParams(collective_id=3, has_side_effects=True),
        cost_estimate=pl.CostEstimate(
            flops=flops * 6, bytes_accessed=16 * query.size * 2, transcendentals=0
        ),
        name="attend_back",
    )(query, *operands, bias, grad_attended, ride)


def ffn_forward(normed, inner_parts, outer_parts, residual):
    kept = []
    total = residual
    for inner, outer in zip(inner_parts, outer_parts):
        act, slope = gelu_pair(product(normed, inner))
        act = act.astype(bf16)
        kept.append((act, slope.astype(bf16)))
        total = total + product(act, outer)
    return total, kept


def ffn_backward(kept, inner_parts, outer_parts, grad_branch):
    grad_pres = []
    grad_normed = None
    for (act, slope), inner, outer in zip(kept, inner_parts, outer_parts):
        grad_pre = (product_bt(grad_branch, outer) * slope.astype(f32)).astype(bf16)
        grad_pres.append(grad_pre)
        piece = product_bt(grad_pre, inner)
        grad_normed = piece if grad_normed is None else grad_normed + piece
    return grad_pres, grad_normed


class SliceSum:
    def __init__(self, operands):
        self.operands = operands

    def term(self, place):
        return weight_grad(*self.operands[place])

    def send_both(self, values):
        self.got_both = swap_core(values)

    def send_core(self, values):
        self.got_core = swap_core(values)

    def chip_sum(self):
        values = product_at(*self.operands[2]) + self.got_both.astype(f32)
        return row_major(values.astype(bf16))

    def send_chip(self, values):
        self.got_chip = swap_chip(values)

    def total(self):
        return self.own.astype(f32) + self.got_core.astype(f32) + self.got_chip.astype(f32)


def cube_bits():
    bits = []
    for axis in ("seq", "wide"):
        count = lax.axis_size(axis).bit_length() - 1
        bits += [(axis, bit) for bit in reversed(range(count))]
    return bits


def cube_orders(bits):
    core = bits.index(("seq", 0))
    chip = bits.index(("seq", 1))
    wide = [place for place, (axis, _) in enumerate(bits) if axis == "wide"]
    if len(wide) == 3:
        far, near, across = wide
        return ((chip, far, near, across, core), (chip, across, far, near, core))
    return ((chip, *wide, core), (chip, *wide[2:], *wide[:2], core))


def cube_place(bits):
    index = {axis: lax.axis_index(axis) for axis in ("seq", "wide")}
    mine = [lax.rem(index[axis] // (1 << bit), 2) for axis, bit in bits]

    def partner(place):
        axis, bit = bits[place]
        other = dict(index)
        other[axis] = index[axis] + (1 - 2 * mine[place]) * (1 << bit)
        return (other["seq"], other["wide"])

    return mine, partner


def cube_barrier(bits, partner):
    barrier = pltpu.get_barrier_semaphore()
    for place in range(len(bits)):
        pl.semaphore_signal(
            barrier, inc=1, device_id=partner(place), device_id_type=pl.DeviceIdType.MESH
        )
    pl.semaphore_wait(barrier, len(bits))


def gather_kernel(
    bits,
    orders,
    own_ref,
    inner_ref,
    outer_ref,
    out_ref,
    inner_core_ref,
    outer_core_ref,
    inner_chip_ref,
    send_sem,
    recv_sem,
    copy_sem,
    ride_send,
    ride_recv,
):
    mine, partner = cube_place(bits)
    own_copy = pltpu.make_async_copy(own_ref, out_ref.at[tuple(mine)], copy_sem)
    own_copy.start()
    cube_barrier(bits, partner)
    own_copy.wait()
    width = own_ref.shape[1] // len(orders)
    core = partner(bits.index(("seq", 0)))
    chip = partner(bits.index(("seq", 1)))
    rides = [
        (inner_ref.at[0, 0], inner_chip_ref, chip),
        (inner_ref.at[0], inner_core_ref, core),
        (outer_ref.at[0], outer_core_ref, core),
    ]
    rides = [
        pltpu.make_async_remote_copy(
            src_ref=source,
            dst_ref=target,
            send_sem=ride_send.at[place],
            recv_sem=ride_recv.at[place],
            device_id=device,
            device_id_type=pl.DeviceIdType.MESH,
        )
        for place, (source, target, device) in enumerate(rides)
    ]
    copies = []
    held = [[False] * len(bits) for _ in orders]
    for stage in range(len(bits)):
        for color, order in enumerate(orders):
            if stage:
                copies[(stage - 1) * len(orders) + color].wait_recv()
                held[color][order[stage - 1]] = True
            place = tuple(
                slice(None) if whole else mine[axis] for axis, whole in enumerate(held[color])
            )
            ref = out_ref.at[place + (slice(None), pl.ds(color * width, width))]
            copy = pltpu.make_async_remote_copy(
                src_ref=ref,
                dst_ref=ref,
                send_sem=send_sem.at[color, stage],
                recv_sem=recv_sem.at[color, stage],
                device_id=partner(order[stage]),
                device_id_type=pl.DeviceIdType.MESH,
            )
            copy.start()
            copies.append(copy)
        if stage == 0:
            for ride in rides:
                ride.start()
    for copy in copies:
        copy.wait_send()
    for copy in copies[-len(orders) :]:
        copy.wait_recv()
    for ride in rides:
        ride.wait()


def gather_rows(own, expert_in, expert_out):
    bits = cube_bits()
    orders = cube_orders(bits)
    rows, width = own.shape
    anywhere = pl.BlockSpec(memory_space=pl.ANY)
    out, inner_core, outer_core, inner_chip = pl.pallas_call(
        functools.partial(gather_kernel, bits, orders),
        in_specs=[pl.BlockSpec(memory_space=pltpu.VMEM), anywhere, anywhere],
        out_specs=[anywhere] * 4,
        out_shape=[
            jax.ShapeDtypeStruct((2,) * len(bits) + (rows, width), own.dtype),
            jax.ShapeDtypeStruct(expert_in.shape[1:], expert_in.dtype),
            jax.ShapeDtypeStruct(expert_out.shape[1:], expert_out.dtype),
            jax.ShapeDtypeStruct(expert_in.shape[2:], expert_in.dtype),
        ],
        scratch_shapes=[
            pltpu.SemaphoreType.DMA((len(orders), len(bits))),
            pltpu.SemaphoreType.DMA((len(orders), len(bits))),
            pltpu.SemaphoreType.DMA,
            pltpu.SemaphoreType.DMA((3,)),
            pltpu.SemaphoreType.DMA((3,)),
        ],
        compiler_params=pltpu.CompilerParams(collective_id=0, has_side_effects=True),
        cost_estimate=pl.CostEstimate(flops=0, bytes_accessed=25 * own.size << 5, transcendentals=0),
        name="gather_rows",
    )(own, expert_in, expert_out)
    return out.reshape(rows << len(bits), width), inner_core, outer_core, inner_chip


def scatter_kernel(bits, orders, terms_ref, out_ref, *scratch):
    stages = len(bits)
    colors = len(orders)
    got = scratch[: colors * stages]
    sums = scratch[colors * stages : colors * (2 * stages - 1)]
    send_sem, recv_sem = scratch[colors * (2 * stages - 1) :]
    mine, partner = cube_place(bits)
    cube_barrier(bits, partner)
    width = terms_ref.shape[-1] // colors
    copies = []

    def half(color, stage, keep):
        done = orders[color][:stage]
        place = []
        for axis in range(stages):
            if axis in done:
                continue
            if axis == orders[color][stage]:
                place.append(mine[axis] if keep else 1 - mine[axis])
            else:
                place.append(slice(None))
        if stage == 0:
            return terms_ref.at[tuple(place) + (slice(None), pl.ds(color * width, width))]
        return sums[color * (stages - 1) + stage - 1].at[tuple(place)]

    for stage in range(stages + 1):
        for color in range(colors):
            if stage:
                copies[(stage - 1) * colors + color].wait_recv()
                kept = half(color, stage - 1, True)[...].astype(f32)
                total = kept + got[color * stages + stage - 1][...].astype(f32)
                if stage == stages:
                    out_ref[:, pl.ds(color * width, width)] = total
                    continue
                sums[color * (stages - 1) + stage - 1][...] = total.astype(bf16)
            copy = pltpu.make_async_remote_copy(
                src_ref=half(color, stage, False),
                dst_ref=got[color * stages + stage],
                send_sem=send_sem.at[color, stage],
                recv_sem=recv_sem.at[color, stage],
                device_id=partner(orders[color][stage]),
                device_id_type=pl.DeviceIdType.MESH,
            )
            copy.start()
            copies.append(copy)
    for copy in copies:
        copy.wait_send()


def scatter_rows(terms):
    bits = cube_bits()
    orders = [order[::-1] for order in cube_orders(bits)]
    colors = len(orders)
    stages = len(bits)
    rows = terms.shape[0] >> stages
    width = terms.shape[1]
    got = [
        pltpu.VMEM((2,) * (stages - 1 - stage) + (rows, width // colors), bf16)
        for _ in range(colors)
        for stage in range(stages)
    ]
    sums = [
        pltpu.VMEM((2,) * (stages - 1 - stage) + (rows, width // colors), bf16)
        for _ in range(colors)
        for stage in range(stages - 1)
    ]
    return pl.pallas_call(
        functools.partial(scatter_kernel, bits, orders),
        in_specs=[pl.BlockSpec(memory_space=pltpu.VMEM)],
        out_specs=pl.BlockSpec(memory_space=pltpu.VMEM),
        out_shape=jax.ShapeDtypeStruct((rows, width), f32),
        scratch_shapes=got
        + sums
        + [
            pltpu.SemaphoreType.DMA((colors, stages)),
            pltpu.SemaphoreType.DMA((colors, stages)),
        ],
        compiler_params=pltpu.CompilerParams(collective_id=1, has_side_effects=True),
        cost_estimate=pl.CostEstimate(flops=0, bytes_accessed=50 * terms.size, transcendentals=0),
        name="scatter_rows",
    )(terms.reshape((2,) * stages + (rows, width)))


def together(*values):
    return lax.optimization_barrier(values)


def per_device(
    block_input,
    segment_ids,
    assignment,
    norm_attn,
    weight_qkv,
    weight_proj,
    norm_ffn,
    weight_up,
    weight_down,
    centroids,
    expert_norms,
    expert_in,
    expert_out,
    grad_out,
):
    row_count, local_len, model_width = block_input.shape
    token_count = row_count * local_len
    seq_devices = lax.axis_size("seq")
    seq_index = lax.axis_index("seq")
    experts = lax.axis_size("wide")
    devices = seq_devices * experts
    every = ("seq", "wide")
    shard = weight_up.shape[0]
    hidden_width = weight_up.shape[1]

    gains_own = jnp.stack([norm_attn, norm_ffn]).astype(f32)
    gains_all = lax.all_to_all(
        jnp.broadcast_to(gains_own[None], (devices, 2, shard)), every, 0, 0, tiled=True
    )
    gains_all = gains_all.transpose(1, 0, 2).reshape(2, model_width)
    gain_attn = gains_all[0]
    gain_ffn = gains_all[1]

    qkv_full, inner_core, outer_core, inner_first = gather_rows(weight_qkv, expert_in, expert_out)
    up_own = (
        weight_up.reshape(shard, devices, BLOCKS, shard)
        .transpose(0, 2, 1, 3)
        .reshape(shard, hidden_width)
    )
    down_own = weight_down.reshape(BLOCKS, shard, model_width).transpose(1, 0, 2)
    rest_own = jnp.concatenate(
        [weight_proj, up_own, down_own.reshape(shard, BLOCKS * model_width)], axis=1
    )
    rest_full = lax.all_gather(rest_own, every, axis=0, tiled=True)

    def rest_block(index):
        return rest_full[:, index * model_width : (index + 1) * model_width]

    proj_full = rest_block(0)
    up_parts = [rest_block(1 + index) for index in range(BLOCKS)]
    down_parts = [rest_block(1 + BLOCKS + index) for index in range(BLOCKS)]

    inner_own = expert_in[0]
    outer_own = expert_out[0]
    inner_chip = [inner_first, None]
    outer_chip = [None, None]

    capacity = token_count // experts
    chosen = assignment.reshape(token_count)
    one_hot = (chosen[:, None] == jnp.arange(experts, dtype=jnp.int32)[None, :]).astype(jnp.int32)
    rank_within = jnp.sum((jnp.cumsum(one_hot, axis=0) - 1) * one_hot, axis=1)
    slot_index = chosen * capacity + rank_within
    source_of = (
        jnp.zeros((token_count,), jnp.int32)
        .at[slot_index]
        .set(jnp.arange(token_count, dtype=jnp.int32))
    )

    tokens_flat = block_input.reshape(token_count, model_width).astype(f32)
    normed_attn = layer_norm(tokens_flat, gain_attn).astype(bf16)
    kv_own = product(normed_attn, qkv_full[:, model_width:]).astype(bf16)
    kv_own = kv_own.reshape(row_count, local_len, 2 * model_width)
    query = product(normed_attn, qkv_full[:, :model_width]).astype(bf16)
    query = query.reshape(row_count, local_len, model_width)

    kv_far = seq_send(kv_own, [(0, 2), (1, 3)])
    kv_near = seq_send(
        jnp.where(seq_index == 3, kv_far, kv_own), [(0, 1), (2, 3), (3, 2)]
    )
    kv_blocks = (kv_own, kv_near, kv_far)
    before = 2 * local_len
    offset = seq_index * local_len
    padded_seg = jnp.pad(segment_ids, ((0, 0), (before, 0)), constant_values=-1)
    key_seg = lax.dynamic_slice_in_dim(padded_seg, offset, before + local_len, 1)
    query_seg = key_seg[:, before:]
    key_pos = jnp.arange(before + local_len)
    query_pos = before + jnp.arange(local_len)
    allowed = (key_seg[:, :, None] == query_seg[:, None, :]) & (
        key_pos[None, :, None] <= query_pos[None, None, :]
    )
    bias = jnp.where(allowed, 0.0, -1e30).astype(f32)

    attended_rows, outer_chip[0] = attend(query, kv_blocks, bias, outer_own)
    late = together(inner_own[1], outer_own[1], attended_rows)
    inner_chip[1], outer_chip[1] = [swap_chip(part) for part in late[:2]]
    attended = attended_rows.reshape(token_count, model_width)
    hidden = tokens_flat + product(attended, proj_full)
    normed_ffn = layer_norm(hidden, gain_ffn).astype(bf16)
    dense_out, dense_kept = ffn_forward(normed_ffn, up_parts, down_parts, hidden)
    routed = dense_out.astype(bf16)

    received = lax.all_to_all(routed[source_of], "wide", split_axis=0, concat_axis=0, tiled=True)
    received_f = received.astype(f32)
    inner_both = [swap_core(together(inner_chip[0], attended)[0]), None]
    outer_both = [swap_core(together(outer_chip[0], attended)[0]), None]
    centroid_row = centroids[0]
    centroid_f = centroid_row.astype(f32)
    logit_row = jnp.dot(received, centroid_row, preferred_element_type=f32)
    gate_value = jax.nn.sigmoid(logit_row)
    gains_f = expert_norms[0].astype(f32)
    state_now = received_f
    kept_layers = []
    slices = []
    for sublayer in range(2):
        if sublayer:
            inner_both[1] = swap_core(together(inner_chip[1], state_now)[0])
            outer_both[1] = swap_core(together(outer_chip[1], state_now)[0])
        inner_parts = [part[sublayer] for part in (inner_own, inner_core, inner_chip, inner_both)]
        outer_parts = [part[sublayer] for part in (outer_own, outer_core, outer_chip, outer_both)]
        normed = layer_norm(state_now, gains_f[sublayer]).astype(bf16)
        state_next, kept = ffn_forward(normed, inner_parts, outer_parts, state_now)
        kept_layers.append((state_now, normed, kept))
        slices.append((inner_parts, outer_parts))
        state_now = state_next
    returned = (gate_value[:, None] * state_now).astype(bf16)
    back_rows = lax.all_to_all(returned, "wide", split_axis=0, concat_axis=0, tiled=True)
    output = (
        (dense_out + back_rows[slot_index].astype(f32)).astype(bf16).reshape(block_input.shape)
    )
    gate_sum = jnp.sum(gate_value)
    score_sum = jnp.sum(logit_row * logit_row)
    grad_flat = grad_out.reshape(token_count, model_width)
    grad_back = lax.all_to_all(
        grad_flat[source_of], "wide", split_axis=0, concat_axis=0, tiled=True
    )
    grad_ret = grad_back.astype(f32)
    grad_gate = jnp.sum(grad_ret * state_now, axis=-1)
    grad_state = grad_ret * gate_value[:, None]
    gain_grads = [None, None]
    weight_terms = [None, None]
    sums = [None, None]
    for sublayer in (1, 0):
        state_in, normed_in, kept = kept_layers[sublayer]
        inner_parts, outer_parts = slices[sublayer]
        grad_branch = grad_state.astype(bf16)
        grad_pres, grad_normed = ffn_backward(kept, inner_parts, outer_parts, grad_branch)
        weight_terms[sublayer] = (
            [(act, grad_branch) for act, _ in kept],
            [(normed_in, grad_pre) for grad_pre in grad_pres],
        )
        grad_resid, gain_grad = norm_back(state_in, gains_f[sublayer], grad_normed)
        grad_state = grad_state + grad_resid
        gain_grads[sublayer] = gain_grad
        sums[sublayer] = [SliceSum(operands) for operands in weight_terms[sublayer]]
        if sublayer:
            grad_state, *held = together(grad_state, *[part.term(3) for part in sums[1]])
            for part, values in zip(sums[1], held):
                part.send_both(values)
    grad_logit = grad_gate * gate_value * (1.0 - gate_value)
    grad_routed = (grad_state + grad_logit[:, None] * centroid_f[None, :]).astype(bf16)
    centroid_grad = jnp.dot(grad_logit, received_f, precision=highest)
    grad_routed, *held = together(grad_routed, *[part.chip_sum() for part in sums[1]])
    for part, values in zip(sums[1], held):
        part.send_chip(values)
    returned_grad = lax.all_to_all(grad_routed, "wide", split_axis=0, concat_axis=0, tiled=True)
    returned_grad, *held = together(
        returned_grad,
        *[part.term(3) for part in sums[0]],
        *[part.term(1) for part in sums[1]],
        *[part.term(0) for part in sums[1]],
    )
    for part, values in zip(sums[0], held[:2]):
        part.send_both(values)
    for part, values in zip(sums[1], held[2:4]):
        part.send_core(values)
    for part, values in zip(sums[1], held[4:]):
        part.own = values
    grad_dense = grad_flat.astype(f32) + returned_grad[slot_index].astype(f32)

    grad_down_in = grad_dense.astype(bf16)
    grad_pres, grad_normed_ffn = ffn_backward(dense_kept, up_parts, down_parts, grad_down_in)
    grad_hidden_norm, grad_gain_ffn = norm_back(hidden, gain_ffn, grad_normed_ffn)
    grad_hidden = grad_dense + grad_hidden_norm
    grad_proj = grad_hidden.astype(bf16)
    rest_grad = jnp.concatenate(
        [weight_grad(attended, grad_proj)]
        + [weight_grad(normed_ffn, grad_pre) for grad_pre in grad_pres]
        + [weight_grad(act, grad_down_in) for act, _ in dense_kept],
        axis=1,
    )
    rest_grad = row_major(rest_grad)
    grad_attended = product_bt(grad_proj, proj_full).astype(bf16)
    outer1, inner1 = sums[1]
    outer0, inner0 = sums[0]
    grad_attended, rest_grad, outer1.got_chip, inner1.got_chip, outer_send, inner_send = together(
        grad_attended,
        rest_grad,
        outer1.got_chip,
        inner1.got_chip,
        outer0.chip_sum(),
        inner0.chip_sum(),
    )
    rest_sum = lax.psum_scatter(rest_grad, every, scatter_dimension=0, tiled=True).astype(f32)
    grad_query, grad_kv0, grad_kv1, grad_kv2, outer0.got_chip = attend_back(
        query, kv_blocks, bias, grad_attended.reshape(query.shape), outer_send
    )
    got_near = seq_send(grad_kv1, [(1, 0), (3, 2), (2, 3)])
    far_sum = jnp.where(
        seq_index == 3, (grad_kv2.astype(f32) + got_near.astype(f32)).astype(bf16), grad_kv2
    )
    got_far = seq_send(far_sum, [(2, 0), (3, 1)])
    got_far, *held = together(
        got_far, *[part.term(1) for part in sums[0]], *[part.term(0) for part in sums[0]]
    )
    for part, values in zip(sums[0], held[:2]):
        part.send_core(values)
    for part, values in zip(sums[0], held[2:]):
        part.own = values
    inner0.send_chip(together(inner_send, got_far)[0])
    kv_sum = grad_kv0.astype(f32) + got_far.astype(f32)
    kv_sum = kv_sum + jnp.where(seq_index % 2 == 0, got_near.astype(f32), 0.0)
    kv_sum = kv_sum.astype(bf16).reshape(2, token_count, model_width)
    grad_qkv = [grad_query.reshape(token_count, model_width), kv_sum[0], kv_sum[1]]
    qkv_grad = row_major(
        jnp.concatenate([weight_grad(normed_attn, part) for part in grad_qkv], axis=1)
    )
    grad_normed_attn = sum(
        product_bt(part, qkv_full[:, index * model_width : (index + 1) * model_width])
        for index, part in enumerate(grad_qkv)
    )
    grad_input_norm, grad_gain_attn = norm_back(tokens_flat, gain_attn, grad_normed_attn)
    grad_input = (grad_hidden + grad_input_norm).reshape(block_input.shape)

    gain_terms = jnp.stack([grad_gain_attn, grad_gain_ffn]).reshape(2, devices, shard)
    gain_terms, qkv_grad = together(gain_terms.transpose(1, 0, 2), qkv_grad)
    gain_terms = lax.all_to_all(gain_terms, every, 0, 0, tiled=True)
    qkv_sum = scatter_rows(qkv_grad)
    gain_sums = jnp.sum(gain_terms, axis=0)
    totals = jnp.concatenate(
        [
            jnp.stack(gain_grads),
            centroid_grad.reshape(1, model_width),
            jnp.pad(jnp.stack([gate_sum, score_sum]), (0, model_width - 2))[None],
        ]
    )
    totals = totals + swap_core(totals)
    totals = totals + swap_chip(totals)
    up_grad = (
        rest_sum[:, model_width : model_width + hidden_width]
        .reshape(shard, BLOCKS, devices, shard)
        .transpose(0, 2, 1, 3)
        .reshape(shard, hidden_width)
    )
    down_grad = (
        rest_sum[:, model_width + hidden_width :]
        .reshape(shard, BLOCKS, model_width)
        .transpose(1, 0, 2)
        .reshape(BLOCKS * shard, model_width)
    )
    token_total = token_count * seq_devices
    return (
        output,
        grad_input,
        gain_sums[0],
        qkv_sum,
        rest_sum[:, :model_width],
        gain_sums[1],
        up_grad,
        down_grad,
        totals[2:3],
        totals[:2][None],
        jnp.stack([inner0.total(), inner1.total()])[None],
        jnp.stack([outer0.total(), outer1.total()])[None],
        totals[3, :1] / token_total,
        totals[3, 1:2] / token_total,
    )


def solution(mesh):
    in_specs = (
        P("wide", "seq", None),
        P("wide", None),
        P("wide", "seq"),
        P(("seq", "wide")),
        P(("seq", "wide"), None),
        P(("seq", "wide"), None),
        P(("seq", "wide")),
        P(("seq", "wide"), None),
        P(("seq", "wide"), None),
        P("wide", None),
        P("wide", None, None),
        P("wide", None, None, "seq"),
        P("wide", None, "seq", None),
        P("wide", "seq", None),
    )
    out_specs = (
        P("wide", "seq", None),
        P("wide", "seq", None),
        P(("seq", "wide")),
        P(("seq", "wide"), None),
        P(("seq", "wide"), None),
        P(("seq", "wide")),
        P(("seq", "wide"), None),
        P(("seq", "wide"), None),
        P("wide", None),
        P("wide", None, None),
        P("wide", None, None, "seq"),
        P("wide", None, "seq", None),
        P("wide"),
        P("wide"),
    )
    return jax.shard_map(
        per_device, mesh=mesh, in_specs=in_specs, out_specs=out_specs, check_vma=False
    )
```

```python
import functools
import math

import jax
import jax.numpy as jnp
from jax import lax
from jax.experimental import pallas as pl
from jax.experimental.layout import Layout, with_layout_constraint
from jax.experimental.pallas import tpu as pltpu
from jax.sharding import PartitionSpec as P

HEADS = 16
HEAD_DIM = 64
BLOCKS = 4
LANES = 128

epsilon = 1e-05
highest = lax.Precision.HIGHEST
bf16 = jnp.bfloat16
f32 = jnp.float32


def layer_norm(values, norm_gain):
    centered = values - jnp.mean(values, axis=-1, keepdims=True)
    variance = jnp.mean(centered * centered, axis=-1, keepdims=True)
    return centered * lax.rsqrt(variance + epsilon) * norm_gain


def norm_back(values, norm_gain, grad_normed):
    _, pull_back = jax.vjp(layer_norm, values, norm_gain)
    return pull_back(grad_normed)


def gelu_pair(values):
    cdf = 0.5 * (1.0 + lax.erf(values * math.sqrt(0.5)))
    density = jnp.exp(values * values * -0.5) * (1.0 / math.sqrt(2.0 * math.pi))
    return values * cdf, cdf + values * density


def product(left_side, right_side):
    return jnp.dot(left_side, right_side, preferred_element_type=f32)


def product_bt(left_side, right_side):
    return lax.dot_general(
        left_side, right_side, (((1,), (1,)), ((), ())), preferred_element_type=f32
    )


def product_at(left_side, right_side):
    return lax.dot_general(
        left_side, right_side, (((0,), (0,)), ((), ())), preferred_element_type=f32
    )


def row_major(values):
    return with_layout_constraint(values, Layout(major_to_minor=(0, 1)))


def weight_grad(left_side, right_side):
    return row_major(product_at(left_side, right_side).astype(bf16))


def seq_send(values, pairs):
    return lax.ppermute(values, "seq", pairs)


def swap_core(values):
    return seq_send(values, [(0, 1), (1, 0), (2, 3), (3, 2)])


def swap_chip(values):
    return seq_send(values, [(0, 2), (2, 0), (1, 3), (3, 1)])


def pair_probs(query, keys, bias, score_scale):
    scores = product_bt(keys, query) * score_scale + bias
    exp_scores = jnp.exp(scores - jnp.max(scores, axis=0, keepdims=True))
    return exp_scores * (1.0 / jnp.sum(exp_scores, axis=0, keepdims=True))


def ride_chip(source, target, send_sem, recv_sem):
    seq = lax.axis_index("seq")
    other = (lax.rem(seq + 2, 4), lax.axis_index("wide"))
    step = pl.program_id(0) * pl.num_programs(1) + pl.program_id(1)
    copy = pltpu.make_async_remote_copy(
        src_ref=source,
        dst_ref=target,
        send_sem=send_sem,
        recv_sem=recv_sem,
        device_id=other,
        device_id_type=pl.DeviceIdType.MESH,
    )

    @pl.when(step == 0)
    def _():
        barrier = pltpu.get_barrier_semaphore()
        pl.semaphore_signal(
            barrier, inc=1, device_id=other, device_id_type=pl.DeviceIdType.MESH
        )
        pl.semaphore_wait(barrier, 1)
        copy.start()

    @pl.when(step == pl.num_programs(0) * pl.num_programs(1) - 1)
    def _():
        copy.wait()


def attend_kernel(
    score_scale,
    q_ref,
    k0,
    v0,
    k1,
    v1,
    k2,
    v2,
    bias_ref,
    ride_ref,
    out_ref,
    rode_ref,
    send_sem,
    recv_sem,
):
    ride_chip(ride_ref.at[0], rode_ref, send_sem, recv_sem)
    bias = bias_ref[0]
    parts = []
    for head in range(2):
        cols = slice(head * HEAD_DIM, (head + 1) * HEAD_DIM)
        keys = jnp.concatenate([k2[0][:, cols], k1[0][:, cols], k0[0][:, cols]], axis=0)
        vals = jnp.concatenate([v2[0][:, cols], v1[0][:, cols], v0[0][:, cols]], axis=0)
        probs_low = pair_probs(q_ref[0][:, cols], keys, bias, score_scale).astype(bf16)
        parts.append(product_at(vals, probs_low))
    out_ref[0] = jnp.concatenate(parts, axis=0).T.astype(bf16)


def attend_back_kernel(
    score_scale,
    q_ref,
    k0,
    v0,
    k1,
    v1,
    k2,
    v2,
    bias_ref,
    grad_ref,
    ride_ref,
    dq_ref,
    d0,
    d1,
    d2,
    rode_ref,
    send_sem,
    recv_sem,
):
    ride_chip(ride_ref, rode_ref, send_sem, recv_sem)
    bias = bias_ref[0]
    dq_parts, dk_parts, dv_parts = [], [], []
    for head in range(2):
        cols = slice(head * HEAD_DIM, (head + 1) * HEAD_DIM)
        query = q_ref[0][:, cols]
        grad_att = grad_ref[0][:, cols]
        keys = jnp.concatenate([k2[0][:, cols], k1[0][:, cols], k0[0][:, cols]], axis=0)
        vals = jnp.concatenate([v2[0][:, cols], v1[0][:, cols], v0[0][:, cols]], axis=0)
        probs = pair_probs(query, keys, bias, score_scale)
        grad_probs = product_bt(vals, grad_att)
        dv_parts.append(product(probs.astype(bf16), grad_att))
        inner_sum = jnp.sum(probs * grad_probs, axis=0, keepdims=True)
        grad_scores = (probs * (grad_probs - inner_sum)).astype(bf16)
        dk_parts.append(product(grad_scores, query) * score_scale)
        dq_parts.append(product_at(keys, grad_scores) * score_scale)
    dq_ref[0] = jnp.concatenate(dq_parts, axis=0).T.astype(bf16)
    d_keys = jnp.concatenate(dk_parts, axis=1).astype(bf16)
    d_vals = jnp.concatenate(dv_parts, axis=1).astype(bf16)
    size = d_keys.shape[0] // 3
    for place, ref in enumerate((d2, d1, d0)):
        ref[0, 0] = d_keys[place * size : (place + 1) * size]
        ref[1, 0] = d_vals[place * size : (place + 1) * size]


def attention_specs(local_len, model_width, key_len):
    width = 2 * HEAD_DIM
    groups = model_width // width
    query = pl.BlockSpec((1, local_len, width), lambda row, head: (row, 0, head))
    values = pl.BlockSpec((1, local_len, width), lambda row, head: (row, 0, head + groups))
    bias = pl.BlockSpec((1, key_len, local_len), lambda row, head: (row, 0, 0))
    return groups, query, [query, query, values, query, values, query, values, bias]


def attend(query, kv_blocks, bias, ride):
    rows, local_len, model_width = query.shape
    groups, spec, in_specs = attention_specs(local_len, model_width, bias.shape[1])
    operands = [block for block in kv_blocks for _ in range(2)]
    flops = 4 * rows * model_width * local_len * bias.shape[1]
    return pl.pallas_call(
        functools.partial(attend_kernel, 1.0 / math.sqrt(HEAD_DIM)),
        grid=(rows, groups),
        in_specs=in_specs + [pl.BlockSpec(memory_space=pl.ANY)],
        out_specs=[spec, pl.BlockSpec(memory_space=pl.ANY)],
        out_shape=[
            jax.ShapeDtypeStruct(query.shape, bf16),
            jax.ShapeDtypeStruct(ride.shape[1:], ride.dtype),
        ],
        scratch_shapes=[pltpu.SemaphoreType.DMA, pltpu.SemaphoreType.DMA],
        compiler_params=pltpu.CompilerParams(collective_id=2, has_side_effects=True),
        cost_estimate=pl.CostEstimate(
            flops=flops * 6, bytes_accessed=8 * query.size * 2, transcendentals=0
        ),
        name="attend",
    )(query, *operands, bias, ride)


def attend_back(query, kv_blocks, bias, grad_attended, ride):
    rows, local_len, model_width = query.shape
    groups, spec, in_specs = attention_specs(local_len, model_width, bias.shape[1])
    operands = [block for block in kv_blocks for _ in range(2)]
    pair_spec = pl.BlockSpec((2, 1, local_len, 2 * HEAD_DIM), lambda row, head: (0, row, 0, head))
    pair_shape = jax.ShapeDtypeStruct((2, rows, local_len, model_width), bf16)
    flops = 10 * rows * model_width * local_len * bias.shape[1]
    return pl.pallas_call(
        functools.partial(attend_back_kernel, 1.0 / math.sqrt(HEAD_DIM)),
        grid=(rows, groups),
        in_specs=in_specs + [spec, pl.BlockSpec(memory_space=pl.ANY)],
        out_specs=[spec, pair_spec, pair_spec, pair_spec, pl.BlockSpec(memory_space=pl.ANY)],
        out_shape=[jax.ShapeDtypeStruct(query.shape, bf16)]
        + [pair_shape] * 3
        + [jax.ShapeDtypeStruct(ride.shape, ride.dtype)],
        scratch_shapes=[pltpu.SemaphoreType.DMA, pltpu.SemaphoreType.DMA],
        compiler_params=pltpu.CompilerParams(collective_id=3, has_side_effects=True),
        cost_estimate=pl.CostEstimate(
            flops=flops * 6, bytes_accessed=16 * query.size * 2, transcendentals=0
        ),
        name="attend_back",
    )(query, *operands, bias, grad_attended, ride)


def ffn_forward(normed, inner_parts, outer_parts, residual):
    kept = []
    total = residual
    for inner, outer in zip(inner_parts, outer_parts):
        act, slope = gelu_pair(product(normed, inner))
        act = act.astype(bf16)
        kept.append((act, slope.astype(bf16)))
        total = total + product(act, outer)
    return total, kept


def ffn_backward(kept, inner_parts, outer_parts, grad_branch):
    grad_pres = []
    grad_normed = None
    for (act, slope), inner, outer in zip(kept, inner_parts, outer_parts):
        grad_pre = (product_bt(grad_branch, outer) * slope.astype(f32)).astype(bf16)
        grad_pres.append(grad_pre)
        piece = product_bt(grad_pre, inner)
        grad_normed = piece if grad_normed is None else grad_normed + piece
    return grad_pres, grad_normed


class SliceSum:
    def __init__(self, operands):
        self.operands = operands

    def term(self, place):
        return weight_grad(*self.operands[place])

    def send_both(self, values):
        self.got_both = swap_core(values)

    def send_core(self, values):
        self.got_core = swap_core(values)

    def chip_sum(self):
        values = product_at(*self.operands[2]) + self.got_both.astype(f32)
        return row_major(values.astype(bf16))

    def send_chip(self, values):
        self.got_chip = swap_chip(values)

    def total(self):
        return self.own.astype(f32) + self.got_core.astype(f32) + self.got_chip.astype(f32)


def cube_bits():
    bits = []
    for axis in ("seq", "wide"):
        count = lax.axis_size(axis).bit_length() - 1
        bits += [(axis, bit) for bit in reversed(range(count))]
    return bits


def cube_orders(bits):
    core = bits.index(("seq", 0))
    chip = bits.index(("seq", 1))
    wide = [place for place, (axis, _) in enumerate(bits) if axis == "wide"]
    if len(wide) == 3:
        far, near, across = wide
        return ((chip, far, near, across, core), (chip, across, far, near, core))
    return ((chip, *wide, core), (chip, *wide[2:], *wide[:2], core))


def cube_place(bits):
    index = {axis: lax.axis_index(axis) for axis in ("seq", "wide")}
    mine = [lax.rem(index[axis] // (1 << bit), 2) for axis, bit in bits]

    def partner(place):
        axis, bit = bits[place]
        other = dict(index)
        other[axis] = index[axis] + (1 - 2 * mine[place]) * (1 << bit)
        return (other["seq"], other["wide"])

    return mine, partner


def cube_barrier(bits, partner):
    barrier = pltpu.get_barrier_semaphore()
    for place in range(len(bits)):
        pl.semaphore_signal(
            barrier, inc=1, device_id=partner(place), device_id_type=pl.DeviceIdType.MESH
        )
    pl.semaphore_wait(barrier, len(bits))


def gather_kernel(
    bits,
    orders,
    own_ref,
    inner_ref,
    outer_ref,
    out_ref,
    inner_core_ref,
    outer_core_ref,
    inner_chip_ref,
    send_sem,
    recv_sem,
    copy_sem,
    ride_send,
    ride_recv,
):
    mine, partner = cube_place(bits)
    own_copy = pltpu.make_async_copy(own_ref, out_ref.at[tuple(mine)], copy_sem)
    own_copy.start()
    cube_barrier(bits, partner)
    own_copy.wait()
    width = own_ref.shape[1] // len(orders)
    core = partner(bits.index(("seq", 0)))
    chip = partner(bits.index(("seq", 1)))
    rides = [
        (inner_ref.at[0, 0], inner_chip_ref, chip),
        (inner_ref.at[0], inner_core_ref, core),
        (outer_ref.at[0], outer_core_ref, core),
    ]
    rides = [
        pltpu.make_async_remote_copy(
            src_ref=source,
            dst_ref=target,
            send_sem=ride_send.at[place],
            recv_sem=ride_recv.at[place],
            device_id=device,
            device_id_type=pl.DeviceIdType.MESH,
        )
        for place, (source, target, device) in enumerate(rides)
    ]
    copies = []
    held = [[False] * len(bits) for _ in orders]
    for stage in range(len(bits)):
        for color, order in enumerate(orders):
            if stage:
                copies[(stage - 1) * len(orders) + color].wait_recv()
                held[color][order[stage - 1]] = True
            place = tuple(
                slice(None) if whole else mine[axis] for axis, whole in enumerate(held[color])
            )
            ref = out_ref.at[place + (slice(None), pl.ds(color * width, width))]
            copy = pltpu.make_async_remote_copy(
                src_ref=ref,
                dst_ref=ref,
                send_sem=send_sem.at[color, stage],
                recv_sem=recv_sem.at[color, stage],
                device_id=partner(order[stage]),
                device_id_type=pl.DeviceIdType.MESH,
            )
            copy.start()
            copies.append(copy)
        if stage == 0:
            for ride in rides:
                ride.start()
    for copy in copies:
        copy.wait_send()
    for copy in copies[-len(orders) :]:
        copy.wait_recv()
    for ride in rides:
        ride.wait()


def gather_rows(own, expert_in, expert_out):
    bits = cube_bits()
    orders = cube_orders(bits)
    rows, width = own.shape
    anywhere = pl.BlockSpec(memory_space=pl.ANY)
    out, inner_core, outer_core, inner_chip = pl.pallas_call(
        functools.partial(gather_kernel, bits, orders),
        in_specs=[pl.BlockSpec(memory_space=pltpu.VMEM), anywhere, anywhere],
        out_specs=[anywhere] * 4,
        out_shape=[
            jax.ShapeDtypeStruct((2,) * len(bits) + (rows, width), own.dtype),
            jax.ShapeDtypeStruct(expert_in.shape[1:], expert_in.dtype),
            jax.ShapeDtypeStruct(expert_out.shape[1:], expert_out.dtype),
            jax.ShapeDtypeStruct(expert_in.shape[2:], expert_in.dtype),
        ],
        scratch_shapes=[
            pltpu.SemaphoreType.DMA((len(orders), len(bits))),
            pltpu.SemaphoreType.DMA((len(orders), len(bits))),
            pltpu.SemaphoreType.DMA,
            pltpu.SemaphoreType.DMA((3,)),
            pltpu.SemaphoreType.DMA((3,)),
        ],
        compiler_params=pltpu.CompilerParams(collective_id=0, has_side_effects=True),
        cost_estimate=pl.CostEstimate(flops=0, bytes_accessed=25 * own.size << 5, transcendentals=0),
        name="gather_rows",
    )(own, expert_in, expert_out)
    return out.reshape(rows << len(bits), width), inner_core, outer_core, inner_chip


def scatter_kernel(bits, orders, terms_ref, out_ref, *scratch):
    stages = len(bits)
    colors = len(orders)
    got = scratch[: colors * stages]
    sums = scratch[colors * stages : colors * (2 * stages - 1)]
    send_sem, recv_sem = scratch[colors * (2 * stages - 1) :]
    mine, partner = cube_place(bits)
    cube_barrier(bits, partner)
    width = terms_ref.shape[-1] // colors
    copies = []

    def half(color, stage, keep):
        done = orders[color][:stage]
        place = []
        for axis in range(stages):
            if axis in done:
                continue
            if axis == orders[color][stage]:
                place.append(mine[axis] if keep else 1 - mine[axis])
            else:
                place.append(slice(None))
        if stage == 0:
            return terms_ref.at[tuple(place) + (slice(None), pl.ds(color * width, width))]
        return sums[color * (stages - 1) + stage - 1].at[tuple(place)]

    for stage in range(stages + 1):
        for color in range(colors):
            if stage:
                copies[(stage - 1) * colors + color].wait_recv()
                kept = half(color, stage - 1, True)[...].astype(f32)
                total = kept + got[color * stages + stage - 1][...].astype(f32)
                if stage == stages:
                    out_ref[:, pl.ds(color * width, width)] = total
                    continue
                sums[color * (stages - 1) + stage - 1][...] = total.astype(bf16)
            copy = pltpu.make_async_remote_copy(
                src_ref=half(color, stage, False),
                dst_ref=got[color * stages + stage],
                send_sem=send_sem.at[color, stage],
                recv_sem=recv_sem.at[color, stage],
                device_id=partner(orders[color][stage]),
                device_id_type=pl.DeviceIdType.MESH,
            )
            copy.start()
            copies.append(copy)
    for copy in copies:
        copy.wait_send()


def scatter_rows(terms):
    bits = cube_bits()
    orders = [order[::-1] for order in cube_orders(bits)]
    colors = len(orders)
    stages = len(bits)
    rows = terms.shape[0] >> stages
    width = terms.shape[1]
    got = [
        pltpu.VMEM((2,) * (stages - 1 - stage) + (rows, width // colors), bf16)
        for _ in range(colors)
        for stage in range(stages)
    ]
    sums = [
        pltpu.VMEM((2,) * (stages - 1 - stage) + (rows, width // colors), bf16)
        for _ in range(colors)
        for stage in range(stages - 1)
    ]
    return pl.pallas_call(
        functools.partial(scatter_kernel, bits, orders),
        in_specs=[pl.BlockSpec(memory_space=pltpu.VMEM)],
        out_specs=pl.BlockSpec(memory_space=pltpu.VMEM),
        out_shape=jax.ShapeDtypeStruct((rows, width), f32),
        scratch_shapes=got
        + sums
        + [
            pltpu.SemaphoreType.DMA((colors, stages)),
            pltpu.SemaphoreType.DMA((colors, stages)),
        ],
        compiler_params=pltpu.CompilerParams(collective_id=1, has_side_effects=True),
        cost_estimate=pl.CostEstimate(flops=0, bytes_accessed=50 * terms.size, transcendentals=0),
        name="scatter_rows",
    )(terms.reshape((2,) * stages + (rows, width)))


def together(*values):
    return lax.optimization_barrier(values)


def per_device(
    block_input,
    segment_ids,
    assignment,
    norm_attn,
    weight_qkv,
    weight_proj,
    norm_ffn,
    weight_up,
    weight_down,
    centroids,
    expert_norms,
    expert_in,
    expert_out,
    grad_out,
):
    row_count, local_len, model_width = block_input.shape
    token_count = row_count * local_len
    seq_devices = lax.axis_size("seq")
    seq_index = lax.axis_index("seq")
    experts = lax.axis_size("wide")
    devices = seq_devices * experts
    every = ("seq", "wide")
    shard = weight_up.shape[0]
    hidden_width = weight_up.shape[1]

    gains_own = jnp.stack([norm_attn, norm_ffn], axis=1)
    first_own = jnp.concatenate(
        [weight_qkv, jnp.pad(gains_own, ((0, 0), (0, 2 * LANES - gains_own.shape[1])))], axis=1
    )
    qkv_full, inner_core, outer_core, inner_first = gather_rows(first_own, expert_in, expert_out)
    gains_all = qkv_full[:, 3 * model_width : 3 * model_width + 2].astype(f32).T
    gain_attn = gains_all[0]
    gain_ffn = gains_all[1]
    up_own = (
        weight_up.reshape(shard, devices, BLOCKS, shard)
        .transpose(0, 2, 1, 3)
        .reshape(shard, hidden_width)
    )
    down_own = weight_down.reshape(BLOCKS, shard, model_width).transpose(1, 0, 2)
    rest_own = jnp.concatenate(
        [weight_proj, up_own, down_own.reshape(shard, BLOCKS * model_width)], axis=1
    )
    rest_own, _ = together(rest_own, qkv_full)
    rest_full = lax.all_gather(rest_own, every, axis=0, tiled=True)

    def rest_block(index):
        return rest_full[:, index * model_width : (index + 1) * model_width]

    proj_full = rest_block(0)
    up_parts = [rest_block(1 + index) for index in range(BLOCKS)]
    down_parts = [rest_block(1 + BLOCKS + index) for index in range(BLOCKS)]

    inner_own = expert_in[0]
    outer_own = expert_out[0]
    inner_chip = [inner_first, None]
    outer_chip = [None, None]

    capacity = token_count // experts
    chosen = assignment.reshape(token_count)
    one_hot = (chosen[:, None] == jnp.arange(experts, dtype=jnp.int32)[None, :]).astype(jnp.int32)
    rank_within = jnp.sum((jnp.cumsum(one_hot, axis=0) - 1) * one_hot, axis=1)
    slot_index = chosen * capacity + rank_within
    source_of = (
        jnp.zeros((token_count,), jnp.int32)
        .at[slot_index]
        .set(jnp.arange(token_count, dtype=jnp.int32))
    )

    tokens_flat = block_input.reshape(token_count, model_width).astype(f32)
    normed_attn = layer_norm(tokens_flat, gain_attn).astype(bf16)
    kv_own = product(normed_attn, qkv_full[:, model_width : 3 * model_width]).astype(bf16)
    kv_own = kv_own.reshape(row_count, local_len, 2 * model_width)
    query = product(normed_attn, qkv_full[:, :model_width]).astype(bf16)
    query = query.reshape(row_count, local_len, model_width)

    kv_far = seq_send(kv_own, [(0, 2), (1, 3)])
    kv_near = seq_send(
        jnp.where(seq_index == 3, kv_far, kv_own), [(0, 1), (2, 3), (3, 2)]
    )
    kv_blocks = (kv_own, kv_near, kv_far)
    before = 2 * local_len
    offset = seq_index * local_len
    padded_seg = jnp.pad(segment_ids, ((0, 0), (before, 0)), constant_values=-1)
    key_seg = lax.dynamic_slice_in_dim(padded_seg, offset, before + local_len, 1)
    query_seg = key_seg[:, before:]
    key_pos = jnp.arange(before + local_len)
    query_pos = before + jnp.arange(local_len)
    allowed = (key_seg[:, :, None] == query_seg[:, None, :]) & (
        key_pos[None, :, None] <= query_pos[None, None, :]
    )
    bias = jnp.where(allowed, 0.0, -1e30).astype(f32)

    attended_rows, outer_chip[0] = attend(query, kv_blocks, bias, outer_own)
    late = together(inner_own[1], outer_own[1], attended_rows)
    inner_chip[1], outer_chip[1] = [swap_chip(part) for part in late[:2]]
    attended = attended_rows.reshape(token_count, model_width)
    hidden = tokens_flat + product(attended, proj_full)
    normed_ffn = layer_norm(hidden, gain_ffn).astype(bf16)
    dense_out, dense_kept = ffn_forward(normed_ffn, up_parts, down_parts, hidden)
    routed = dense_out.astype(bf16)

    received = lax.all_to_all(routed[source_of], "wide", split_axis=0, concat_axis=0, tiled=True)
    received, inner_chip[1] = together(received, inner_chip[1])
    received_f = received.astype(f32)
    inner_both = [swap_core(together(inner_chip[0], attended)[0]), None]
    outer_both = [swap_core(together(outer_chip[0], attended)[0]), None]
    centroid_row = centroids[0]
    centroid_f = centroid_row.astype(f32)
    logit_row = jnp.dot(received, centroid_row, preferred_element_type=f32)
    gate_value = jax.nn.sigmoid(logit_row)
    gains_f = expert_norms[0].astype(f32)
    state_now = received_f
    kept_layers = []
    slices = []
    for sublayer in range(2):
        if sublayer:
            inner_both[1] = swap_core(together(inner_chip[1], state_now)[0])
            outer_both[1] = swap_core(together(outer_chip[1], state_now)[0])
        inner_parts = [part[sublayer] for part in (inner_own, inner_core, inner_chip, inner_both)]
        outer_parts = [part[sublayer] for part in (outer_own, outer_core, outer_chip, outer_both)]
        normed = layer_norm(state_now, gains_f[sublayer]).astype(bf16)
        state_next, kept = ffn_forward(normed, inner_parts, outer_parts, state_now)
        kept_layers.append((state_now, normed, kept))
        slices.append((inner_parts, outer_parts))
        state_now = state_next
    returned = (gate_value[:, None] * state_now).astype(bf16)
    back_rows = lax.all_to_all(returned, "wide", split_axis=0, concat_axis=0, tiled=True)
    output = (
        (dense_out + back_rows[slot_index].astype(f32)).astype(bf16).reshape(block_input.shape)
    )
    gate_sum = jnp.sum(gate_value)
    score_sum = jnp.sum(logit_row * logit_row)
    grad_flat = grad_out.reshape(token_count, model_width)
    grad_back = lax.all_to_all(
        grad_flat[source_of], "wide", split_axis=0, concat_axis=0, tiled=True
    )
    grad_ret = grad_back.astype(f32)
    grad_gate = jnp.sum(grad_ret * state_now, axis=-1)
    grad_state = grad_ret * gate_value[:, None]
    gain_grads = [None, None]
    weight_terms = [None, None]
    sums = [None, None]
    for sublayer in (1, 0):
        state_in, normed_in, kept = kept_layers[sublayer]
        inner_parts, outer_parts = slices[sublayer]
        grad_branch = grad_state.astype(bf16)
        grad_pres, grad_normed = ffn_backward(kept, inner_parts, outer_parts, grad_branch)
        weight_terms[sublayer] = (
            [(act, grad_branch) for act, _ in kept],
            [(normed_in, grad_pre) for grad_pre in grad_pres],
        )
        grad_resid, gain_grad = norm_back(state_in, gains_f[sublayer], grad_normed)
        grad_state = grad_state + grad_resid
        gain_grads[sublayer] = gain_grad
        sums[sublayer] = [SliceSum(operands) for operands in weight_terms[sublayer]]
        if sublayer:
            grad_state, *held = together(grad_state, *[part.term(3) for part in sums[1]])
            for part, values in zip(sums[1], held):
                part.send_both(values)
    grad_logit = grad_gate * gate_value * (1.0 - gate_value)
    grad_routed = (grad_state + grad_logit[:, None] * centroid_f[None, :]).astype(bf16)
    centroid_grad = jnp.dot(grad_logit, received_f, precision=highest)
    grad_routed, *held = together(grad_routed, *[part.chip_sum() for part in sums[1]])
    for part, values in zip(sums[1], held):
        part.send_chip(values)
    returned_grad = lax.all_to_all(grad_routed, "wide", split_axis=0, concat_axis=0, tiled=True)
    returned_grad, *held = together(
        returned_grad,
        *[part.term(3) for part in sums[0]],
        *[part.term(1) for part in sums[1]],
        *[part.term(0) for part in sums[1]],
    )
    for part, values in zip(sums[0], held[:2]):
        part.send_both(values)
    for part, values in zip(sums[1], held[2:4]):
        part.send_core(values)
    for part, values in zip(sums[1], held[4:]):
        part.own = values
    grad_dense = grad_flat.astype(f32) + returned_grad[slot_index].astype(f32)

    grad_down_in = grad_dense.astype(bf16)
    grad_pres, grad_normed_ffn = ffn_backward(dense_kept, up_parts, down_parts, grad_down_in)
    grad_hidden_norm, grad_gain_ffn = norm_back(hidden, gain_ffn, grad_normed_ffn)
    grad_hidden = grad_dense + grad_hidden_norm
    outer1, inner1 = sums[1]
    outer0, inner0 = sums[0]
    grad_hidden, outer1.got_chip = together(grad_hidden, outer1.got_chip)
    grad_proj = grad_hidden.astype(bf16)
    rest_grad = jnp.concatenate(
        [weight_grad(attended, grad_proj)]
        + [weight_grad(normed_ffn, grad_pre) for grad_pre in grad_pres]
        + [weight_grad(act, grad_down_in) for act, _ in dense_kept],
        axis=1,
    )
    rest_grad = row_major(rest_grad)
    grad_attended = product_bt(grad_proj, proj_full).astype(bf16)
    grad_attended, rest_grad = together(grad_attended, rest_grad)
    grad_attended, inner1.got_chip, outer_send, inner_send = together(
        grad_attended, inner1.got_chip, outer0.chip_sum(), inner0.chip_sum()
    )
    rest_sum = lax.psum_scatter(rest_grad, every, scatter_dimension=0, tiled=True).astype(f32)
    grad_query, grad_kv0, grad_kv1, grad_kv2, outer0.got_chip = attend_back(
        query, kv_blocks, bias, grad_attended.reshape(query.shape), outer_send
    )
    got_near = seq_send(grad_kv1, [(1, 0), (3, 2), (2, 3)])
    far_sum = jnp.where(
        seq_index == 3, (grad_kv2.astype(f32) + got_near.astype(f32)).astype(bf16), grad_kv2
    )
    got_far = seq_send(far_sum, [(2, 0), (3, 1)])
    got_far, *held = together(
        got_far, *[part.term(1) for part in sums[0]], *[part.term(0) for part in sums[0]]
    )
    for part, values in zip(sums[0], held[:2]):
        part.send_core(values)
    for part, values in zip(sums[0], held[2:]):
        part.own = values
    inner0.send_chip(together(inner_send, got_far)[0])
    kv_sum = grad_kv0.astype(f32) + got_far.astype(f32)
    kv_sum = kv_sum + jnp.where(seq_index % 2 == 0, got_near.astype(f32), 0.0)
    kv_sum = kv_sum.astype(bf16).reshape(2, token_count, model_width)
    grad_qkv = [grad_query.reshape(token_count, model_width), kv_sum[0], kv_sum[1]]
    qkv_grad = row_major(
        jnp.concatenate([weight_grad(normed_attn, part) for part in grad_qkv], axis=1)
    )
    grad_normed_attn = sum(
        product_bt(part, qkv_full[:, index * model_width : (index + 1) * model_width])
        for index, part in enumerate(grad_qkv)
    )
    grad_input_norm, grad_gain_attn = norm_back(tokens_flat, gain_attn, grad_normed_attn)
    grad_input = (grad_hidden + grad_input_norm).reshape(block_input.shape)

    gain_terms = jnp.stack([grad_gain_attn, grad_gain_ffn]).reshape(2, devices, shard)
    gain_terms, qkv_grad = together(gain_terms.transpose(1, 0, 2), qkv_grad)
    gain_terms = lax.all_to_all(gain_terms, every, 0, 0, tiled=True)
    qkv_sum = scatter_rows(qkv_grad)
    gain_sums = jnp.sum(gain_terms, axis=0)
    totals = jnp.concatenate(
        [
            jnp.stack(gain_grads),
            centroid_grad.reshape(1, model_width),
            jnp.pad(jnp.stack([gate_sum, score_sum]), (0, model_width - 2))[None],
        ]
    )
    totals = totals + swap_core(totals)
    totals = totals + swap_chip(totals)
    up_grad = (
        rest_sum[:, model_width : model_width + hidden_width]
        .reshape(shard, BLOCKS, devices, shard)
        .transpose(0, 2, 1, 3)
        .reshape(shard, hidden_width)
    )
    down_grad = (
        rest_sum[:, model_width + hidden_width :]
        .reshape(shard, BLOCKS, model_width)
        .transpose(1, 0, 2)
        .reshape(BLOCKS * shard, model_width)
    )
    token_total = token_count * seq_devices
    return (
        output,
        grad_input,
        gain_sums[0],
        qkv_sum,
        rest_sum[:, :model_width],
        gain_sums[1],
        up_grad,
        down_grad,
        totals[2:3],
        totals[:2][None],
        jnp.stack([inner0.total(), inner1.total()])[None],
        jnp.stack([outer0.total(), outer1.total()])[None],
        totals[3, :1] / token_total,
        totals[3, 1:2] / token_total,
    )


def solution(mesh):
    in_specs = (
        P("wide", "seq", None),
        P("wide", None),
        P("wide", "seq"),
        P(("seq", "wide")),
        P(("seq", "wide"), None),
        P(("seq", "wide"), None),
        P(("seq", "wide")),
        P(("seq", "wide"), None),
        P(("seq", "wide"), None),
        P("wide", None),
        P("wide", None, None),
        P("wide", None, None, "seq"),
        P("wide", None, "seq", None),
        P("wide", "seq", None),
    )
    out_specs = (
        P("wide", "seq", None),
        P("wide", "seq", None),
        P(("seq", "wide")),
        P(("seq", "wide"), None),
        P(("seq", "wide"), None),
        P(("seq", "wide")),
        P(("seq", "wide"), None),
        P(("seq", "wide"), None),
        P("wide", None),
        P("wide", None, None),
        P("wide", None, None, "seq"),
        P("wide", None, "seq", None),
        P("wide"),
        P("wide"),
    )
    return jax.shard_map(
        per_device, mesh=mesh, in_specs=in_specs, out_specs=out_specs, check_vma=False
    )
```

```python
import functools
import math

import jax
import jax.numpy as jnp
from jax import lax
from jax.experimental import pallas as pl
from jax.experimental.layout import Layout, with_layout_constraint
from jax.experimental.pallas import tpu as pltpu
from jax.sharding import PartitionSpec as P

HEADS = 16
HEAD_DIM = 64
BLOCKS = 4
LANES = 128

epsilon = 1e-05
highest = lax.Precision.HIGHEST
bf16 = jnp.bfloat16
f32 = jnp.float32


def layer_norm(values, norm_gain):
    centered = values - jnp.mean(values, axis=-1, keepdims=True)
    variance = jnp.mean(centered * centered, axis=-1, keepdims=True)
    return centered * lax.rsqrt(variance + epsilon) * norm_gain


def norm_back(values, norm_gain, grad_normed):
    _, pull_back = jax.vjp(layer_norm, values, norm_gain)
    return pull_back(grad_normed)


def gelu_pair(values):
    cdf = 0.5 * (1.0 + lax.erf(values * math.sqrt(0.5)))
    density = jnp.exp(values * values * -0.5) * (1.0 / math.sqrt(2.0 * math.pi))
    return values * cdf, cdf + values * density


def product(left_side, right_side):
    return jnp.dot(left_side, right_side, preferred_element_type=f32)


def product_bt(left_side, right_side):
    return lax.dot_general(
        left_side, right_side, (((1,), (1,)), ((), ())), preferred_element_type=f32
    )


def product_at(left_side, right_side):
    return lax.dot_general(
        left_side, right_side, (((0,), (0,)), ((), ())), preferred_element_type=f32
    )


def row_major(values):
    return with_layout_constraint(values, Layout(major_to_minor=(0, 1)))


def weight_grad(left_side, right_side):
    return row_major(product_at(left_side, right_side).astype(bf16))


def seq_send(values, pairs):
    return lax.ppermute(values, "seq", pairs)


def swap_core(values):
    return seq_send(values, [(0, 1), (1, 0), (2, 3), (3, 2)])


def swap_chip(values):
    return seq_send(values, [(0, 2), (2, 0), (1, 3), (3, 1)])


def pair_probs(query, keys, bias, score_scale):
    scores = product_bt(keys, query) * score_scale + bias
    exp_scores = jnp.exp(scores - jnp.max(scores, axis=0, keepdims=True))
    return exp_scores * (1.0 / jnp.sum(exp_scores, axis=0, keepdims=True))


def ride_chip(source, target, send_sem, recv_sem):
    seq = lax.axis_index("seq")
    other = (lax.rem(seq + 2, 4), lax.axis_index("wide"))
    step = pl.program_id(0) * pl.num_programs(1) + pl.program_id(1)
    copy = pltpu.make_async_remote_copy(
        src_ref=source,
        dst_ref=target,
        send_sem=send_sem,
        recv_sem=recv_sem,
        device_id=other,
        device_id_type=pl.DeviceIdType.MESH,
    )

    @pl.when(step == 0)
    def _():
        barrier = pltpu.get_barrier_semaphore()
        pl.semaphore_signal(
            barrier, inc=1, device_id=other, device_id_type=pl.DeviceIdType.MESH
        )
        pl.semaphore_wait(barrier, 1)
        copy.start()

    @pl.when(step == pl.num_programs(0) * pl.num_programs(1) - 1)
    def _():
        copy.wait()


def attend_kernel(
    score_scale,
    q_ref,
    k0,
    v0,
    k1,
    v1,
    k2,
    v2,
    bias_ref,
    ride_ref,
    out_ref,
    rode_ref,
    send_sem,
    recv_sem,
):
    ride_chip(ride_ref.at[0], rode_ref, send_sem, recv_sem)
    bias = bias_ref[0]
    parts = []
    for head in range(2):
        cols = slice(head * HEAD_DIM, (head + 1) * HEAD_DIM)
        keys = jnp.concatenate([k2[0][:, cols], k1[0][:, cols], k0[0][:, cols]], axis=0)
        vals = jnp.concatenate([v2[0][:, cols], v1[0][:, cols], v0[0][:, cols]], axis=0)
        probs_low = pair_probs(q_ref[0][:, cols], keys, bias, score_scale).astype(bf16)
        parts.append(product_at(vals, probs_low))
    out_ref[0] = jnp.concatenate(parts, axis=0).T.astype(bf16)


def attend_back_kernel(
    score_scale,
    q_ref,
    k0,
    v0,
    k1,
    v1,
    k2,
    v2,
    bias_ref,
    grad_ref,
    dq_ref,
    d0,
    d1,
    d2,
):
    bias = bias_ref[0]
    dq_parts, dk_parts, dv_parts = [], [], []
    for head in range(2):
        cols = slice(head * HEAD_DIM, (head + 1) * HEAD_DIM)
        query = q_ref[0][:, cols]
        grad_att = grad_ref[0][:, cols]
        keys = jnp.concatenate([k2[0][:, cols], k1[0][:, cols], k0[0][:, cols]], axis=0)
        vals = jnp.concatenate([v2[0][:, cols], v1[0][:, cols], v0[0][:, cols]], axis=0)
        probs = pair_probs(query, keys, bias, score_scale)
        grad_probs = product_bt(vals, grad_att)
        dv_parts.append(product(probs.astype(bf16), grad_att))
        inner_sum = jnp.sum(probs * grad_probs, axis=0, keepdims=True)
        grad_scores = (probs * (grad_probs - inner_sum)).astype(bf16)
        dk_parts.append(product(grad_scores, query) * score_scale)
        dq_parts.append(product_at(keys, grad_scores) * score_scale)
    dq_ref[0] = jnp.concatenate(dq_parts, axis=0).T.astype(bf16)
    d_keys = jnp.concatenate(dk_parts, axis=1).astype(bf16)
    d_vals = jnp.concatenate(dv_parts, axis=1).astype(bf16)
    size = d_keys.shape[0] // 3
    for place, ref in enumerate((d2, d1, d0)):
        ref[0, 0] = d_keys[place * size : (place + 1) * size]
        ref[1, 0] = d_vals[place * size : (place + 1) * size]


def attention_specs(local_len, model_width, key_len):
    width = 2 * HEAD_DIM
    groups = model_width // width
    query = pl.BlockSpec((1, local_len, width), lambda row, head: (row, 0, head))
    values = pl.BlockSpec((1, local_len, width), lambda row, head: (row, 0, head + groups))
    bias = pl.BlockSpec((1, key_len, local_len), lambda row, head: (row, 0, 0))
    return groups, query, [query, query, values, query, values, query, values, bias]


def attend(query, kv_blocks, bias, ride):
    rows, local_len, model_width = query.shape
    groups, spec, in_specs = attention_specs(local_len, model_width, bias.shape[1])
    operands = [block for block in kv_blocks for _ in range(2)]
    flops = 4 * rows * model_width * local_len * bias.shape[1]
    return pl.pallas_call(
        functools.partial(attend_kernel, 1.0 / math.sqrt(HEAD_DIM)),
        grid=(rows, groups),
        in_specs=in_specs + [pl.BlockSpec(memory_space=pl.ANY)],
        out_specs=[spec, pl.BlockSpec(memory_space=pl.ANY)],
        out_shape=[
            jax.ShapeDtypeStruct(query.shape, bf16),
            jax.ShapeDtypeStruct(ride.shape[1:], ride.dtype),
        ],
        scratch_shapes=[pltpu.SemaphoreType.DMA, pltpu.SemaphoreType.DMA],
        compiler_params=pltpu.CompilerParams(collective_id=2, has_side_effects=True),
        cost_estimate=pl.CostEstimate(
            flops=flops * 6, bytes_accessed=8 * query.size * 2, transcendentals=0
        ),
        name="attend",
    )(query, *operands, bias, ride)


def attend_back(query, kv_blocks, bias, grad_attended):
    rows, local_len, model_width = query.shape
    groups, spec, in_specs = attention_specs(local_len, model_width, bias.shape[1])
    operands = [block for block in kv_blocks for _ in range(2)]
    pair_spec = pl.BlockSpec((2, 1, local_len, 2 * HEAD_DIM), lambda row, head: (0, row, 0, head))
    pair_shape = jax.ShapeDtypeStruct((2, rows, local_len, model_width), bf16)
    flops = 10 * rows * model_width * local_len * bias.shape[1]
    return pl.pallas_call(
        functools.partial(attend_back_kernel, 1.0 / math.sqrt(HEAD_DIM)),
        grid=(rows, groups),
        in_specs=in_specs + [spec],
        out_specs=[spec, pair_spec, pair_spec, pair_spec],
        out_shape=[jax.ShapeDtypeStruct(query.shape, bf16)] + [pair_shape] * 3,
        cost_estimate=pl.CostEstimate(
            flops=flops * 6, bytes_accessed=16 * query.size * 2, transcendentals=0
        ),
        name="attend_back",
    )(query, *operands, bias, grad_attended)


def ffn_forward(normed, inner_parts, outer_parts, residual):
    kept = []
    total = residual
    for inner, outer in zip(inner_parts, outer_parts):
        act, slope = gelu_pair(product(normed, inner))
        act = act.astype(bf16)
        kept.append((act, slope.astype(bf16)))
        total = total + product(act, outer)
    return total, kept


def ffn_backward(kept, inner_parts, outer_parts, grad_branch):
    grad_pres = []
    grad_normed = None
    for (act, slope), inner, outer in zip(kept, inner_parts, outer_parts):
        grad_pre = (product_bt(grad_branch, outer) * slope.astype(f32)).astype(bf16)
        grad_pres.append(grad_pre)
        piece = product_bt(grad_pre, inner)
        grad_normed = piece if grad_normed is None else grad_normed + piece
    return grad_pres, grad_normed


class SliceSum:
    def __init__(self, operands):
        self.operands = operands

    def term(self, place):
        return weight_grad(*self.operands[place])

    def send_both(self, values):
        self.got_both = swap_core(values)

    def send_core(self, values):
        self.got_core = swap_core(values)

    def chip_sum(self):
        values = product_at(*self.operands[2]) + self.got_both.astype(f32)
        return row_major(values.astype(bf16))

    def send_chip(self, values):
        self.got_chip = swap_chip(values)

    def total(self):
        return self.own.astype(f32) + self.got_core.astype(f32) + self.got_chip.astype(f32)


def cube_bits():
    bits = []
    for axis in ("seq", "wide"):
        count = lax.axis_size(axis).bit_length() - 1
        bits += [(axis, bit) for bit in reversed(range(count))]
    return bits


def cube_orders(bits):
    core = bits.index(("seq", 0))
    chip = bits.index(("seq", 1))
    wide = [place for place, (axis, _) in enumerate(bits) if axis == "wide"]
    if len(wide) == 3:
        far, near, across = wide
        return ((chip, far, near, across, core), (chip, across, far, near, core))
    return ((chip, *wide, core), (chip, *wide[2:], *wide[:2], core))


def cube_place(bits):
    index = {axis: lax.axis_index(axis) for axis in ("seq", "wide")}
    mine = [lax.rem(index[axis] // (1 << bit), 2) for axis, bit in bits]

    def partner(place):
        axis, bit = bits[place]
        other = dict(index)
        other[axis] = index[axis] + (1 - 2 * mine[place]) * (1 << bit)
        return (other["seq"], other["wide"])

    return mine, partner


def cube_barrier(bits, partner):
    barrier = pltpu.get_barrier_semaphore()
    for place in range(len(bits)):
        pl.semaphore_signal(
            barrier, inc=1, device_id=partner(place), device_id_type=pl.DeviceIdType.MESH
        )
    pl.semaphore_wait(barrier, len(bits))


def gather_kernel(
    bits,
    orders,
    own_ref,
    inner_ref,
    outer_ref,
    out_ref,
    inner_core_ref,
    outer_core_ref,
    inner_chip_ref,
    send_sem,
    recv_sem,
    copy_sem,
    ride_send,
    ride_recv,
):
    mine, partner = cube_place(bits)
    own_copy = pltpu.make_async_copy(own_ref, out_ref.at[tuple(mine)], copy_sem)
    own_copy.start()
    cube_barrier(bits, partner)
    own_copy.wait()
    width = own_ref.shape[1] // len(orders)
    core = partner(bits.index(("seq", 0)))
    chip = partner(bits.index(("seq", 1)))
    rides = [
        (inner_ref.at[0, 0], inner_chip_ref, chip),
        (inner_ref.at[0], inner_core_ref, core),
        (outer_ref.at[0], outer_core_ref, core),
    ]
    rides = [
        pltpu.make_async_remote_copy(
            src_ref=source,
            dst_ref=target,
            send_sem=ride_send.at[place],
            recv_sem=ride_recv.at[place],
            device_id=device,
            device_id_type=pl.DeviceIdType.MESH,
        )
        for place, (source, target, device) in enumerate(rides)
    ]
    copies = []
    held = [[False] * len(bits) for _ in orders]
    for stage in range(len(bits)):
        for color, order in enumerate(orders):
            if stage:
                copies[(stage - 1) * len(orders) + color].wait_recv()
                held[color][order[stage - 1]] = True
            place = tuple(
                slice(None) if whole else mine[axis] for axis, whole in enumerate(held[color])
            )
            ref = out_ref.at[place + (slice(None), pl.ds(color * width, width))]
            copy = pltpu.make_async_remote_copy(
                src_ref=ref,
                dst_ref=ref,
                send_sem=send_sem.at[color, stage],
                recv_sem=recv_sem.at[color, stage],
                device_id=partner(order[stage]),
                device_id_type=pl.DeviceIdType.MESH,
            )
            copy.start()
            copies.append(copy)
        if stage == 0:
            for ride in rides:
                ride.start()
    for copy in copies:
        copy.wait_send()
    for copy in copies[-len(orders) :]:
        copy.wait_recv()
    for ride in rides:
        ride.wait()


def gather_rows(own, expert_in, expert_out):
    bits = cube_bits()
    orders = cube_orders(bits)
    rows, width = own.shape
    anywhere = pl.BlockSpec(memory_space=pl.ANY)
    out, inner_core, outer_core, inner_chip = pl.pallas_call(
        functools.partial(gather_kernel, bits, orders),
        in_specs=[pl.BlockSpec(memory_space=pltpu.VMEM), anywhere, anywhere],
        out_specs=[anywhere] * 4,
        out_shape=[
            jax.ShapeDtypeStruct((2,) * len(bits) + (rows, width), own.dtype),
            jax.ShapeDtypeStruct(expert_in.shape[1:], expert_in.dtype),
            jax.ShapeDtypeStruct(expert_out.shape[1:], expert_out.dtype),
            jax.ShapeDtypeStruct(expert_in.shape[2:], expert_in.dtype),
        ],
        scratch_shapes=[
            pltpu.SemaphoreType.DMA((len(orders), len(bits))),
            pltpu.SemaphoreType.DMA((len(orders), len(bits))),
            pltpu.SemaphoreType.DMA,
            pltpu.SemaphoreType.DMA((3,)),
            pltpu.SemaphoreType.DMA((3,)),
        ],
        compiler_params=pltpu.CompilerParams(collective_id=0, has_side_effects=True),
        cost_estimate=pl.CostEstimate(flops=0, bytes_accessed=25 * own.size << 5, transcendentals=0),
        name="gather_rows",
    )(own, expert_in, expert_out)
    return out.reshape(rows << len(bits), width), inner_core, outer_core, inner_chip


def scatter_kernel(bits, orders, terms_ref, out_ref, *scratch):
    stages = len(bits)
    colors = len(orders)
    got = scratch[: colors * stages]
    sums = scratch[colors * stages : colors * (2 * stages - 1)]
    send_sem, recv_sem = scratch[colors * (2 * stages - 1) :]
    mine, partner = cube_place(bits)
    cube_barrier(bits, partner)
    width = terms_ref.shape[-1] // colors
    copies = []

    def half(color, stage, keep):
        done = orders[color][:stage]
        place = []
        for axis in range(stages):
            if axis in done:
                continue
            if axis == orders[color][stage]:
                place.append(mine[axis] if keep else 1 - mine[axis])
            else:
                place.append(slice(None))
        if stage == 0:
            return terms_ref.at[tuple(place) + (slice(None), pl.ds(color * width, width))]
        return sums[color * (stages - 1) + stage - 1].at[tuple(place)]

    for stage in range(stages + 1):
        for color in range(colors):
            if stage:
                copies[(stage - 1) * colors + color].wait_recv()
                kept = half(color, stage - 1, True)[...].astype(f32)
                total = kept + got[color * stages + stage - 1][...].astype(f32)
                if stage == stages:
                    out_ref[:, pl.ds(color * width, width)] = total
                    continue
                sums[color * (stages - 1) + stage - 1][...] = total.astype(bf16)
            copy = pltpu.make_async_remote_copy(
                src_ref=half(color, stage, False),
                dst_ref=got[color * stages + stage],
                send_sem=send_sem.at[color, stage],
                recv_sem=recv_sem.at[color, stage],
                device_id=partner(orders[color][stage]),
                device_id_type=pl.DeviceIdType.MESH,
            )
            copy.start()
            copies.append(copy)
    for copy in copies:
        copy.wait_send()


def scatter_rows(terms):
    bits = cube_bits()
    orders = [order[::-1] for order in cube_orders(bits)]
    colors = len(orders)
    stages = len(bits)
    rows = terms.shape[0] >> stages
    width = terms.shape[1]
    got = [
        pltpu.VMEM((2,) * (stages - 1 - stage) + (rows, width // colors), bf16)
        for _ in range(colors)
        for stage in range(stages)
    ]
    sums = [
        pltpu.VMEM((2,) * (stages - 1 - stage) + (rows, width // colors), bf16)
        for _ in range(colors)
        for stage in range(stages - 1)
    ]
    return pl.pallas_call(
        functools.partial(scatter_kernel, bits, orders),
        in_specs=[pl.BlockSpec(memory_space=pltpu.VMEM)],
        out_specs=pl.BlockSpec(memory_space=pltpu.VMEM),
        out_shape=jax.ShapeDtypeStruct((rows, width), f32),
        scratch_shapes=got
        + sums
        + [
            pltpu.SemaphoreType.DMA((colors, stages)),
            pltpu.SemaphoreType.DMA((colors, stages)),
        ],
        compiler_params=pltpu.CompilerParams(collective_id=1, has_side_effects=True),
        cost_estimate=pl.CostEstimate(flops=0, bytes_accessed=50 * terms.size, transcendentals=0),
        name="scatter_rows",
    )(terms.reshape((2,) * stages + (rows, width)))


def together(*values):
    return lax.optimization_barrier(values)


def per_device(
    block_input,
    segment_ids,
    assignment,
    norm_attn,
    weight_qkv,
    weight_proj,
    norm_ffn,
    weight_up,
    weight_down,
    centroids,
    expert_norms,
    expert_in,
    expert_out,
    grad_out,
):
    row_count, local_len, model_width = block_input.shape
    token_count = row_count * local_len
    seq_devices = lax.axis_size("seq")
    seq_index = lax.axis_index("seq")
    experts = lax.axis_size("wide")
    devices = seq_devices * experts
    every = ("seq", "wide")
    shard = weight_up.shape[0]
    hidden_width = weight_up.shape[1]

    gains_own = jnp.stack([norm_attn, norm_ffn], axis=1)
    first_own = jnp.concatenate(
        [weight_qkv, jnp.pad(gains_own, ((0, 0), (0, 2 * LANES - gains_own.shape[1])))], axis=1
    )
    qkv_full, inner_core, outer_core, inner_first = gather_rows(first_own, expert_in, expert_out)
    gains_all = qkv_full[:, 3 * model_width : 3 * model_width + 2].astype(f32).T
    gain_attn = gains_all[0]
    gain_ffn = gains_all[1]
    up_own = (
        weight_up.reshape(shard, devices, BLOCKS, shard)
        .transpose(0, 2, 1, 3)
        .reshape(shard, hidden_width)
    )
    down_own = weight_down.reshape(BLOCKS, shard, model_width).transpose(1, 0, 2)
    rest_own = jnp.concatenate(
        [weight_proj, up_own, down_own.reshape(shard, BLOCKS * model_width)], axis=1
    )
    rest_own, _ = together(rest_own, qkv_full)
    rest_full = lax.all_gather(rest_own, every, axis=0, tiled=True)

    def rest_block(index):
        return rest_full[:, index * model_width : (index + 1) * model_width]

    proj_full = rest_block(0)
    up_parts = [rest_block(1 + index) for index in range(BLOCKS)]
    down_parts = [rest_block(1 + BLOCKS + index) for index in range(BLOCKS)]

    inner_own = expert_in[0]
    outer_own = expert_out[0]
    inner_chip = [inner_first, None]
    outer_chip = [None, None]

    capacity = token_count // experts
    chosen = assignment.reshape(token_count)
    one_hot = (chosen[:, None] == jnp.arange(experts, dtype=jnp.int32)[None, :]).astype(jnp.int32)
    rank_within = jnp.sum((jnp.cumsum(one_hot, axis=0) - 1) * one_hot, axis=1)
    slot_index = chosen * capacity + rank_within
    source_of = (
        jnp.zeros((token_count,), jnp.int32)
        .at[slot_index]
        .set(jnp.arange(token_count, dtype=jnp.int32))
    )

    tokens_flat = block_input.reshape(token_count, model_width).astype(f32)
    normed_attn = layer_norm(tokens_flat, gain_attn).astype(bf16)
    kv_own = product(normed_attn, qkv_full[:, model_width : 3 * model_width]).astype(bf16)
    kv_own = kv_own.reshape(row_count, local_len, 2 * model_width)
    query = product(normed_attn, qkv_full[:, :model_width]).astype(bf16)
    query = query.reshape(row_count, local_len, model_width)

    kv_far = seq_send(kv_own, [(0, 2), (1, 3)])
    kv_near = seq_send(
        jnp.where(seq_index == 3, kv_far, kv_own), [(0, 1), (2, 3), (3, 2)]
    )
    kv_blocks = (kv_own, kv_near, kv_far)
    before = 2 * local_len
    offset = seq_index * local_len
    padded_seg = jnp.pad(segment_ids, ((0, 0), (before, 0)), constant_values=-1)
    key_seg = lax.dynamic_slice_in_dim(padded_seg, offset, before + local_len, 1)
    query_seg = key_seg[:, before:]
    key_pos = jnp.arange(before + local_len)
    query_pos = before + jnp.arange(local_len)
    allowed = (key_seg[:, :, None] == query_seg[:, None, :]) & (
        key_pos[None, :, None] <= query_pos[None, None, :]
    )
    bias = jnp.where(allowed, 0.0, -1e30).astype(f32)

    attended_rows, outer_chip[0] = attend(query, kv_blocks, bias, outer_own)
    late = together(inner_own[1], outer_own[1], attended_rows)
    inner_chip[1], outer_chip[1] = [swap_chip(part) for part in late[:2]]
    attended = attended_rows.reshape(token_count, model_width)
    hidden = tokens_flat + product(attended, proj_full)
    normed_ffn = layer_norm(hidden, gain_ffn).astype(bf16)
    dense_out, dense_kept = ffn_forward(normed_ffn, up_parts, down_parts, hidden)
    routed = dense_out.astype(bf16)

    received = lax.all_to_all(routed[source_of], "wide", split_axis=0, concat_axis=0, tiled=True)
    received, inner_chip[1] = together(received, inner_chip[1])
    received_f = received.astype(f32)
    inner_both = [swap_core(together(inner_chip[0], attended)[0]), None]
    outer_both = [swap_core(together(outer_chip[0], attended)[0]), None]
    centroid_row = centroids[0]
    centroid_f = centroid_row.astype(f32)
    logit_row = jnp.dot(received, centroid_row, preferred_element_type=f32)
    gate_value = jax.nn.sigmoid(logit_row)
    gains_f = expert_norms[0].astype(f32)
    state_now = received_f
    kept_layers = []
    slices = []
    for sublayer in range(2):
        if sublayer:
            inner_both[1] = swap_core(together(inner_chip[1], state_now)[0])
            outer_both[1] = swap_core(together(outer_chip[1], state_now)[0])
        inner_parts = [part[sublayer] for part in (inner_own, inner_core, inner_chip, inner_both)]
        outer_parts = [part[sublayer] for part in (outer_own, outer_core, outer_chip, outer_both)]
        normed = layer_norm(state_now, gains_f[sublayer]).astype(bf16)
        state_next, kept = ffn_forward(normed, inner_parts, outer_parts, state_now)
        kept_layers.append((state_now, normed, kept))
        slices.append((inner_parts, outer_parts))
        state_now = state_next
    returned = (gate_value[:, None] * state_now).astype(bf16)
    back_rows = lax.all_to_all(returned, "wide", split_axis=0, concat_axis=0, tiled=True)
    output = (
        (dense_out + back_rows[slot_index].astype(f32)).astype(bf16).reshape(block_input.shape)
    )
    gate_sum = jnp.sum(gate_value)
    score_sum = jnp.sum(logit_row * logit_row)
    grad_flat = grad_out.reshape(token_count, model_width)
    grad_back = lax.all_to_all(
        grad_flat[source_of], "wide", split_axis=0, concat_axis=0, tiled=True
    )
    grad_ret = grad_back.astype(f32)
    grad_gate = jnp.sum(grad_ret * state_now, axis=-1)
    grad_state = grad_ret * gate_value[:, None]
    gain_grads = [None, None]
    weight_terms = [None, None]
    sums = [None, None]
    for sublayer in (1, 0):
        state_in, normed_in, kept = kept_layers[sublayer]
        inner_parts, outer_parts = slices[sublayer]
        grad_branch = grad_state.astype(bf16)
        grad_pres, grad_normed = ffn_backward(kept, inner_parts, outer_parts, grad_branch)
        weight_terms[sublayer] = (
            [(act, grad_branch) for act, _ in kept],
            [(normed_in, grad_pre) for grad_pre in grad_pres],
        )
        grad_resid, gain_grad = norm_back(state_in, gains_f[sublayer], grad_normed)
        grad_state = grad_state + grad_resid
        gain_grads[sublayer] = gain_grad
        sums[sublayer] = [SliceSum(operands) for operands in weight_terms[sublayer]]
        if sublayer:
            grad_state, *held = together(grad_state, *[part.term(3) for part in sums[1]])
            for part, values in zip(sums[1], held):
                part.send_both(values)
    grad_logit = grad_gate * gate_value * (1.0 - gate_value)
    grad_routed = (grad_state + grad_logit[:, None] * centroid_f[None, :]).astype(bf16)
    centroid_grad = jnp.dot(grad_logit, received_f, precision=highest)
    grad_routed, *held = together(grad_routed, *[part.chip_sum() for part in sums[1]])
    for part, values in zip(sums[1], held):
        part.send_chip(values)
    returned_grad = lax.all_to_all(grad_routed, "wide", split_axis=0, concat_axis=0, tiled=True)
    returned_grad, *held = together(
        returned_grad,
        *[part.term(3) for part in sums[0]],
        *[part.term(1) for part in sums[1]],
        *[part.term(0) for part in sums[1]],
    )
    for part, values in zip(sums[0], held[:2]):
        part.send_both(values)
    for part, values in zip(sums[1], held[2:4]):
        part.send_core(values)
    for part, values in zip(sums[1], held[4:]):
        part.own = values
    grad_dense = grad_flat.astype(f32) + returned_grad[slot_index].astype(f32)

    grad_down_in = grad_dense.astype(bf16)
    grad_pres, grad_normed_ffn = ffn_backward(dense_kept, up_parts, down_parts, grad_down_in)
    grad_hidden_norm, grad_gain_ffn = norm_back(hidden, gain_ffn, grad_normed_ffn)
    grad_hidden = grad_dense + grad_hidden_norm
    outer1, inner1 = sums[1]
    outer0, inner0 = sums[0]
    grad_hidden, outer1.got_chip = together(grad_hidden, outer1.got_chip)
    grad_proj = grad_hidden.astype(bf16)
    rest_grad = jnp.concatenate(
        [weight_grad(attended, grad_proj)]
        + [weight_grad(normed_ffn, grad_pre) for grad_pre in grad_pres]
        + [weight_grad(act, grad_down_in) for act, _ in dense_kept],
        axis=1,
    )
    rest_grad = row_major(rest_grad)
    grad_attended = product_bt(grad_proj, proj_full).astype(bf16)
    grad_attended, rest_grad = together(grad_attended, rest_grad)
    rest_sum = lax.psum_scatter(rest_grad, every, scatter_dimension=0, tiled=True).astype(f32)
    grad_query, grad_kv0, grad_kv1, grad_kv2 = attend_back(
        query, kv_blocks, bias, grad_attended.reshape(query.shape)
    )
    grad_kv1, inner1.got_chip = together(grad_kv1, inner1.got_chip)
    got_near = seq_send(grad_kv1, [(1, 0), (3, 2), (2, 3)])
    far_sum = jnp.where(
        seq_index == 3, (grad_kv2.astype(f32) + got_near.astype(f32)).astype(bf16), grad_kv2
    )
    got_far = seq_send(far_sum, [(2, 0), (3, 1)])
    got_far, *held = together(
        got_far, *[part.term(1) for part in sums[0]], *[part.term(0) for part in sums[0]]
    )
    for part, values in zip(sums[0], held[:2]):
        part.send_core(values)
    for part, values in zip(sums[0], held[2:]):
        part.own = values
    outer_send, inner_send, got_far = together(outer0.chip_sum(), inner0.chip_sum(), got_far)
    outer0.send_chip(outer_send)
    inner0.send_chip(inner_send)
    kv_sum = grad_kv0.astype(f32) + got_far.astype(f32)
    kv_sum = kv_sum + jnp.where(seq_index % 2 == 0, got_near.astype(f32), 0.0)
    kv_sum = kv_sum.astype(bf16).reshape(2, token_count, model_width)
    grad_qkv = [grad_query.reshape(token_count, model_width), kv_sum[0], kv_sum[1]]
    qkv_grad = row_major(
        jnp.concatenate([weight_grad(normed_attn, part) for part in grad_qkv], axis=1)
    )
    grad_normed_attn = sum(
        product_bt(part, qkv_full[:, index * model_width : (index + 1) * model_width])
        for index, part in enumerate(grad_qkv)
    )
    grad_input_norm, grad_gain_attn = norm_back(tokens_flat, gain_attn, grad_normed_attn)
    grad_input = (grad_hidden + grad_input_norm).reshape(block_input.shape)

    gain_terms = jnp.stack([grad_gain_attn, grad_gain_ffn]).reshape(2, devices, shard)
    gain_terms, qkv_grad = together(gain_terms.transpose(1, 0, 2), qkv_grad)
    gain_terms = lax.all_to_all(gain_terms, every, 0, 0, tiled=True)
    qkv_sum = scatter_rows(qkv_grad)
    gain_sums = jnp.sum(gain_terms, axis=0)
    totals = jnp.concatenate(
        [
            jnp.stack(gain_grads),
            centroid_grad.reshape(1, model_width),
            jnp.pad(jnp.stack([gate_sum, score_sum]), (0, model_width - 2))[None],
        ]
    )
    totals = totals + swap_core(totals)
    totals = totals + swap_chip(totals)
    up_grad = (
        rest_sum[:, model_width : model_width + hidden_width]
        .reshape(shard, BLOCKS, devices, shard)
        .transpose(0, 2, 1, 3)
        .reshape(shard, hidden_width)
    )
    down_grad = (
        rest_sum[:, model_width + hidden_width :]
        .reshape(shard, BLOCKS, model_width)
        .transpose(1, 0, 2)
        .reshape(BLOCKS * shard, model_width)
    )
    token_total = token_count * seq_devices
    return (
        output,
        grad_input,
        gain_sums[0],
        qkv_sum,
        rest_sum[:, :model_width],
        gain_sums[1],
        up_grad,
        down_grad,
        totals[2:3],
        totals[:2][None],
        jnp.stack([inner0.total(), inner1.total()])[None],
        jnp.stack([outer0.total(), outer1.total()])[None],
        totals[3, :1] / token_total,
        totals[3, 1:2] / token_total,
    )


def solution(mesh):
    in_specs = (
        P("wide", "seq", None),
        P("wide", None),
        P("wide", "seq"),
        P(("seq", "wide")),
        P(("seq", "wide"), None),
        P(("seq", "wide"), None),
        P(("seq", "wide")),
        P(("seq", "wide"), None),
        P(("seq", "wide"), None),
        P("wide", None),
        P("wide", None, None),
        P("wide", None, None, "seq"),
        P("wide", None, "seq", None),
        P("wide", "seq", None),
    )
    out_specs = (
        P("wide", "seq", None),
        P("wide", "seq", None),
        P(("seq", "wide")),
        P(("seq", "wide"), None),
        P(("seq", "wide"), None),
        P(("seq", "wide")),
        P(("seq", "wide"), None),
        P(("seq", "wide"), None),
        P("wide", None),
        P("wide", None, None),
        P("wide", None, None, "seq"),
        P("wide", None, "seq", None),
        P("wide"),
        P("wide"),
    )
    return jax.shard_map(
        per_device, mesh=mesh, in_specs=in_specs, out_specs=out_specs, check_vma=False
    )
```

```python
import functools
import math

import jax
import jax.numpy as jnp
from jax import lax
from jax.experimental import pallas as pl
from jax.experimental.layout import Layout, with_layout_constraint
from jax.experimental.pallas import tpu as pltpu
from jax.sharding import PartitionSpec as P

HEADS = 16
HEAD_DIM = 64
BLOCKS = 4
LANES = 128

epsilon = 1e-05
highest = lax.Precision.HIGHEST
bf16 = jnp.bfloat16
f32 = jnp.float32


def layer_norm(values, norm_gain):
    centered = values - jnp.mean(values, axis=-1, keepdims=True)
    variance = jnp.mean(centered * centered, axis=-1, keepdims=True)
    return centered * lax.rsqrt(variance + epsilon) * norm_gain


def norm_back(values, norm_gain, grad_normed):
    _, pull_back = jax.vjp(layer_norm, values, norm_gain)
    return pull_back(grad_normed)


def gelu_pair(values):
    cdf = 0.5 * (1.0 + lax.erf(values * math.sqrt(0.5)))
    density = jnp.exp(values * values * -0.5) * (1.0 / math.sqrt(2.0 * math.pi))
    return values * cdf, cdf + values * density


def product(left_side, right_side):
    return jnp.dot(left_side, right_side, preferred_element_type=f32)


def product_bt(left_side, right_side):
    return lax.dot_general(
        left_side, right_side, (((1,), (1,)), ((), ())), preferred_element_type=f32
    )


def product_at(left_side, right_side):
    return lax.dot_general(
        left_side, right_side, (((0,), (0,)), ((), ())), preferred_element_type=f32
    )


def row_major(values):
    return with_layout_constraint(values, Layout(major_to_minor=(0, 1)))


def weight_grad(left_side, right_side):
    return row_major(product_at(left_side, right_side).astype(bf16))


def seq_send(values, pairs):
    return lax.ppermute(values, "seq", pairs)


def swap_core(values):
    return seq_send(values, [(0, 1), (1, 0), (2, 3), (3, 2)])


def swap_chip(values):
    return seq_send(values, [(0, 2), (2, 0), (1, 3), (3, 1)])


def pair_probs(query, keys, bias, score_scale):
    scores = product_bt(keys, query) * score_scale + bias
    exp_scores = jnp.exp(scores - jnp.max(scores, axis=0, keepdims=True))
    return exp_scores * (1.0 / jnp.sum(exp_scores, axis=0, keepdims=True))


def ride_chip(source, target, send_sem, recv_sem):
    seq = lax.axis_index("seq")
    other = (lax.rem(seq + 2, 4), lax.axis_index("wide"))
    step = pl.program_id(0) * pl.num_programs(1) + pl.program_id(1)
    copy = pltpu.make_async_remote_copy(
        src_ref=source,
        dst_ref=target,
        send_sem=send_sem,
        recv_sem=recv_sem,
        device_id=other,
        device_id_type=pl.DeviceIdType.MESH,
    )

    @pl.when(step == 0)
    def _():
        barrier = pltpu.get_barrier_semaphore()
        pl.semaphore_signal(
            barrier, inc=1, device_id=other, device_id_type=pl.DeviceIdType.MESH
        )
        pl.semaphore_wait(barrier, 1)
        copy.start()

    @pl.when(step == pl.num_programs(0) * pl.num_programs(1) - 1)
    def _():
        copy.wait()


def attend_kernel(
    score_scale,
    q_ref,
    k0,
    v0,
    k1,
    v1,
    k2,
    v2,
    bias_ref,
    ride_ref,
    out_ref,
    rode_ref,
    send_sem,
    recv_sem,
):
    ride_chip(ride_ref.at[0], rode_ref, send_sem, recv_sem)
    bias = bias_ref[0]
    parts = []
    for head in range(2):
        cols = slice(head * HEAD_DIM, (head + 1) * HEAD_DIM)
        keys = jnp.concatenate([k2[0][:, cols], k1[0][:, cols], k0[0][:, cols]], axis=0)
        vals = jnp.concatenate([v2[0][:, cols], v1[0][:, cols], v0[0][:, cols]], axis=0)
        probs_low = pair_probs(q_ref[0][:, cols], keys, bias, score_scale).astype(bf16)
        parts.append(product_at(vals, probs_low))
    out_ref[0] = jnp.concatenate(parts, axis=0).T.astype(bf16)


def attend_back_kernel(
    score_scale,
    q_ref,
    k0,
    v0,
    k1,
    v1,
    k2,
    v2,
    bias_ref,
    grad_ref,
    dq_ref,
    d0,
    d1,
    d2,
):
    bias = bias_ref[0]
    dq_parts, dk_parts, dv_parts = [], [], []
    for head in range(2):
        cols = slice(head * HEAD_DIM, (head + 1) * HEAD_DIM)
        query = q_ref[0][:, cols]
        grad_att = grad_ref[0][:, cols]
        keys = jnp.concatenate([k2[0][:, cols], k1[0][:, cols], k0[0][:, cols]], axis=0)
        vals = jnp.concatenate([v2[0][:, cols], v1[0][:, cols], v0[0][:, cols]], axis=0)
        probs = pair_probs(query, keys, bias, score_scale)
        grad_probs = product_bt(vals, grad_att)
        dv_parts.append(product(probs.astype(bf16), grad_att))
        inner_sum = jnp.sum(probs * grad_probs, axis=0, keepdims=True)
        grad_scores = (probs * (grad_probs - inner_sum)).astype(bf16)
        dk_parts.append(product(grad_scores, query) * score_scale)
        dq_parts.append(product_at(keys, grad_scores) * score_scale)
    dq_ref[0] = jnp.concatenate(dq_parts, axis=0).T.astype(bf16)
    d_keys = jnp.concatenate(dk_parts, axis=1).astype(bf16)
    d_vals = jnp.concatenate(dv_parts, axis=1).astype(bf16)
    size = d_keys.shape[0] // 3
    for place, ref in enumerate((d2, d1, d0)):
        ref[0, 0] = d_keys[place * size : (place + 1) * size]
        ref[1, 0] = d_vals[place * size : (place + 1) * size]


def attention_specs(local_len, model_width, key_len):
    width = 2 * HEAD_DIM
    groups = model_width // width
    query = pl.BlockSpec((1, local_len, width), lambda row, head: (row, 0, head))
    values = pl.BlockSpec((1, local_len, width), lambda row, head: (row, 0, head + groups))
    bias = pl.BlockSpec((1, key_len, local_len), lambda row, head: (row, 0, 0))
    return groups, query, [query, query, values, query, values, query, values, bias]


def attend(query, kv_blocks, bias, ride):
    rows, local_len, model_width = query.shape
    groups, spec, in_specs = attention_specs(local_len, model_width, bias.shape[1])
    operands = [block for block in kv_blocks for _ in range(2)]
    flops = 4 * rows * model_width * local_len * bias.shape[1]
    return pl.pallas_call(
        functools.partial(attend_kernel, 1.0 / math.sqrt(HEAD_DIM)),
        grid=(rows, groups),
        in_specs=in_specs + [pl.BlockSpec(memory_space=pl.ANY)],
        out_specs=[spec, pl.BlockSpec(memory_space=pl.ANY)],
        out_shape=[
            jax.ShapeDtypeStruct(query.shape, bf16),
            jax.ShapeDtypeStruct(ride.shape[1:], ride.dtype),
        ],
        scratch_shapes=[pltpu.SemaphoreType.DMA, pltpu.SemaphoreType.DMA],
        compiler_params=pltpu.CompilerParams(collective_id=2, has_side_effects=True),
        cost_estimate=pl.CostEstimate(
            flops=flops * 6, bytes_accessed=8 * query.size * 2, transcendentals=0
        ),
        name="attend",
    )(query, *operands, bias, ride)


def attend_back(query, kv_blocks, bias, grad_attended, row):
    _, local_len, model_width = query.shape
    key_len = bias.shape[1]
    width = 2 * HEAD_DIM
    groups = model_width // width
    spec = pl.BlockSpec((1, local_len, width), lambda head: (row, 0, head))
    value_spec = pl.BlockSpec((1, local_len, width), lambda head: (row, 0, head + groups))
    bias_spec = pl.BlockSpec((1, key_len, local_len), lambda head: (row, 0, 0))
    operands = [block for block in kv_blocks for _ in range(2)]
    pair_spec = pl.BlockSpec((2, 1, local_len, width), lambda head: (0, 0, 0, head))
    pair_shape = jax.ShapeDtypeStruct((2, 1, local_len, model_width), bf16)
    flops = 10 * model_width * local_len * key_len
    return pl.pallas_call(
        functools.partial(attend_back_kernel, 1.0 / math.sqrt(HEAD_DIM)),
        grid=(groups,),
        in_specs=[spec] + [spec, value_spec] * 3 + [bias_spec, spec],
        out_specs=[
            pl.BlockSpec((1, local_len, width), lambda head: (0, 0, head)),
            pair_spec,
            pair_spec,
            pair_spec,
        ],
        out_shape=[jax.ShapeDtypeStruct((1, local_len, model_width), bf16)] + [pair_shape] * 3,
        cost_estimate=pl.CostEstimate(
            flops=flops * 12, bytes_accessed=8 * query.size * 2, transcendentals=0
        ),
        name="attend_back",
    )(query, *operands, bias, grad_attended)


def ffn_forward(normed, inner_parts, outer_parts, residual):
    kept = []
    total = residual
    for inner, outer in zip(inner_parts, outer_parts):
        act, slope = gelu_pair(product(normed, inner))
        act = act.astype(bf16)
        kept.append((act, slope.astype(bf16)))
        total = total + product(act, outer)
    return total, kept


def ffn_backward(kept, inner_parts, outer_parts, grad_branch):
    grad_pres = []
    grad_normed = None
    for (act, slope), inner, outer in zip(kept, inner_parts, outer_parts):
        grad_pre = (product_bt(grad_branch, outer) * slope.astype(f32)).astype(bf16)
        grad_pres.append(grad_pre)
        piece = product_bt(grad_pre, inner)
        grad_normed = piece if grad_normed is None else grad_normed + piece
    return grad_pres, grad_normed


class SliceSum:
    def __init__(self, operands):
        self.operands = operands

    def term(self, place):
        return weight_grad(*self.operands[place])

    def send_both(self, values):
        self.got_both = swap_core(values)

    def send_core(self, values):
        self.got_core = swap_core(values)

    def chip_sum(self):
        values = product_at(*self.operands[2]) + self.got_both.astype(f32)
        return row_major(values.astype(bf16))

    def send_chip(self, values):
        self.got_chip = swap_chip(values)

    def total(self):
        return self.own.astype(f32) + self.got_core.astype(f32) + self.got_chip.astype(f32)


def cube_bits():
    bits = []
    for axis in ("seq", "wide"):
        count = lax.axis_size(axis).bit_length() - 1
        bits += [(axis, bit) for bit in reversed(range(count))]
    return bits


def cube_orders(bits):
    core = bits.index(("seq", 0))
    chip = bits.index(("seq", 1))
    wide = [place for place, (axis, _) in enumerate(bits) if axis == "wide"]
    if len(wide) == 3:
        far, near, across = wide
        return ((chip, far, near, across, core), (chip, across, far, near, core))
    return ((chip, *wide, core), (chip, *wide[2:], *wide[:2], core))


def cube_place(bits):
    index = {axis: lax.axis_index(axis) for axis in ("seq", "wide")}
    mine = [lax.rem(index[axis] // (1 << bit), 2) for axis, bit in bits]

    def partner(place):
        axis, bit = bits[place]
        other = dict(index)
        other[axis] = index[axis] + (1 - 2 * mine[place]) * (1 << bit)
        return (other["seq"], other["wide"])

    return mine, partner


def cube_barrier(bits, partner):
    barrier = pltpu.get_barrier_semaphore()
    for place in range(len(bits)):
        pl.semaphore_signal(
            barrier, inc=1, device_id=partner(place), device_id_type=pl.DeviceIdType.MESH
        )
    pl.semaphore_wait(barrier, len(bits))


def gather_kernel(
    bits,
    orders,
    own_ref,
    inner_ref,
    outer_ref,
    out_ref,
    inner_core_ref,
    outer_core_ref,
    inner_chip_ref,
    send_sem,
    recv_sem,
    copy_sem,
    ride_send,
    ride_recv,
):
    mine, partner = cube_place(bits)
    own_copy = pltpu.make_async_copy(own_ref, out_ref.at[tuple(mine)], copy_sem)
    own_copy.start()
    cube_barrier(bits, partner)
    own_copy.wait()
    width = own_ref.shape[1] // len(orders)
    core = partner(bits.index(("seq", 0)))
    chip = partner(bits.index(("seq", 1)))
    rides = [
        (inner_ref.at[0, 0], inner_chip_ref, chip),
        (inner_ref.at[0], inner_core_ref, core),
        (outer_ref.at[0], outer_core_ref, core),
    ]
    rides = [
        pltpu.make_async_remote_copy(
            src_ref=source,
            dst_ref=target,
            send_sem=ride_send.at[place],
            recv_sem=ride_recv.at[place],
            device_id=device,
            device_id_type=pl.DeviceIdType.MESH,
        )
        for place, (source, target, device) in enumerate(rides)
    ]
    copies = []
    held = [[False] * len(bits) for _ in orders]
    for stage in range(len(bits)):
        for color, order in enumerate(orders):
            if stage:
                copies[(stage - 1) * len(orders) + color].wait_recv()
                held[color][order[stage - 1]] = True
            place = tuple(
                slice(None) if whole else mine[axis] for axis, whole in enumerate(held[color])
            )
            ref = out_ref.at[place + (slice(None), pl.ds(color * width, width))]
            copy = pltpu.make_async_remote_copy(
                src_ref=ref,
                dst_ref=ref,
                send_sem=send_sem.at[color, stage],
                recv_sem=recv_sem.at[color, stage],
                device_id=partner(order[stage]),
                device_id_type=pl.DeviceIdType.MESH,
            )
            copy.start()
            copies.append(copy)
        if stage == 0:
            for ride in rides:
                ride.start()
    for copy in copies:
        copy.wait_send()
    for copy in copies[-len(orders) :]:
        copy.wait_recv()
    for ride in rides:
        ride.wait()


def gather_rows(own, expert_in, expert_out):
    bits = cube_bits()
    orders = cube_orders(bits)
    rows, width = own.shape
    anywhere = pl.BlockSpec(memory_space=pl.ANY)
    out, inner_core, outer_core, inner_chip = pl.pallas_call(
        functools.partial(gather_kernel, bits, orders),
        in_specs=[pl.BlockSpec(memory_space=pltpu.VMEM), anywhere, anywhere],
        out_specs=[anywhere] * 4,
        out_shape=[
            jax.ShapeDtypeStruct((2,) * len(bits) + (rows, width), own.dtype),
            jax.ShapeDtypeStruct(expert_in.shape[1:], expert_in.dtype),
            jax.ShapeDtypeStruct(expert_out.shape[1:], expert_out.dtype),
            jax.ShapeDtypeStruct(expert_in.shape[2:], expert_in.dtype),
        ],
        scratch_shapes=[
            pltpu.SemaphoreType.DMA((len(orders), len(bits))),
            pltpu.SemaphoreType.DMA((len(orders), len(bits))),
            pltpu.SemaphoreType.DMA,
            pltpu.SemaphoreType.DMA((3,)),
            pltpu.SemaphoreType.DMA((3,)),
        ],
        compiler_params=pltpu.CompilerParams(collective_id=0, has_side_effects=True),
        cost_estimate=pl.CostEstimate(flops=0, bytes_accessed=25 * own.size << 5, transcendentals=0),
        name="gather_rows",
    )(own, expert_in, expert_out)
    return out.reshape(rows << len(bits), width), inner_core, outer_core, inner_chip


def scatter_kernel(bits, orders, terms_ref, out_ref, *scratch):
    stages = len(bits)
    colors = len(orders)
    got = scratch[: colors * stages]
    sums = scratch[colors * stages : colors * (2 * stages - 1)]
    send_sem, recv_sem = scratch[colors * (2 * stages - 1) :]
    mine, partner = cube_place(bits)
    cube_barrier(bits, partner)
    width = terms_ref.shape[-1] // colors
    copies = []

    def half(color, stage, keep):
        done = orders[color][:stage]
        place = []
        for axis in range(stages):
            if axis in done:
                continue
            if axis == orders[color][stage]:
                place.append(mine[axis] if keep else 1 - mine[axis])
            else:
                place.append(slice(None))
        if stage == 0:
            return terms_ref.at[tuple(place) + (slice(None), pl.ds(color * width, width))]
        return sums[color * (stages - 1) + stage - 1].at[tuple(place)]

    for stage in range(stages + 1):
        for color in range(colors):
            if stage:
                copies[(stage - 1) * colors + color].wait_recv()
                kept = half(color, stage - 1, True)[...].astype(f32)
                total = kept + got[color * stages + stage - 1][...].astype(f32)
                if stage == stages:
                    out_ref[:, pl.ds(color * width, width)] = total
                    continue
                sums[color * (stages - 1) + stage - 1][...] = total.astype(bf16)
            copy = pltpu.make_async_remote_copy(
                src_ref=half(color, stage, False),
                dst_ref=got[color * stages + stage],
                send_sem=send_sem.at[color, stage],
                recv_sem=recv_sem.at[color, stage],
                device_id=partner(orders[color][stage]),
                device_id_type=pl.DeviceIdType.MESH,
            )
            copy.start()
            copies.append(copy)
    for copy in copies:
        copy.wait_send()


def scatter_rows(terms):
    bits = cube_bits()
    orders = [order[::-1] for order in cube_orders(bits)]
    colors = len(orders)
    stages = len(bits)
    rows = terms.shape[0] >> stages
    width = terms.shape[1]
    got = [
        pltpu.VMEM((2,) * (stages - 1 - stage) + (rows, width // colors), bf16)
        for _ in range(colors)
        for stage in range(stages)
    ]
    sums = [
        pltpu.VMEM((2,) * (stages - 1 - stage) + (rows, width // colors), bf16)
        for _ in range(colors)
        for stage in range(stages - 1)
    ]
    return pl.pallas_call(
        functools.partial(scatter_kernel, bits, orders),
        in_specs=[pl.BlockSpec(memory_space=pltpu.VMEM)],
        out_specs=pl.BlockSpec(memory_space=pltpu.VMEM),
        out_shape=jax.ShapeDtypeStruct((rows, width), f32),
        scratch_shapes=got
        + sums
        + [
            pltpu.SemaphoreType.DMA((colors, stages)),
            pltpu.SemaphoreType.DMA((colors, stages)),
        ],
        compiler_params=pltpu.CompilerParams(collective_id=1, has_side_effects=True),
        cost_estimate=pl.CostEstimate(flops=0, bytes_accessed=50 * terms.size, transcendentals=0),
        name="scatter_rows",
    )(terms.reshape((2,) * stages + (rows, width)))


def together(*values):
    return lax.optimization_barrier(values)


def per_device(
    block_input,
    segment_ids,
    assignment,
    norm_attn,
    weight_qkv,
    weight_proj,
    norm_ffn,
    weight_up,
    weight_down,
    centroids,
    expert_norms,
    expert_in,
    expert_out,
    grad_out,
):
    row_count, local_len, model_width = block_input.shape
    token_count = row_count * local_len
    seq_devices = lax.axis_size("seq")
    seq_index = lax.axis_index("seq")
    experts = lax.axis_size("wide")
    devices = seq_devices * experts
    every = ("seq", "wide")
    shard = weight_up.shape[0]
    hidden_width = weight_up.shape[1]

    gains_own = jnp.stack([norm_attn, norm_ffn], axis=1)
    first_own = jnp.concatenate(
        [weight_qkv, jnp.pad(gains_own, ((0, 0), (0, 2 * LANES - gains_own.shape[1])))], axis=1
    )
    qkv_full, inner_core, outer_core, inner_first = gather_rows(first_own, expert_in, expert_out)
    gains_all = qkv_full[:, 3 * model_width : 3 * model_width + 2].astype(f32).T
    gain_attn = gains_all[0]
    gain_ffn = gains_all[1]
    up_own = (
        weight_up.reshape(shard, devices, BLOCKS, shard)
        .transpose(0, 2, 1, 3)
        .reshape(shard, hidden_width)
    )
    down_own = weight_down.reshape(BLOCKS, shard, model_width).transpose(1, 0, 2)
    rest_own = jnp.concatenate(
        [weight_proj, up_own, down_own.reshape(shard, BLOCKS * model_width)], axis=1
    )
    rest_own, _ = together(rest_own, qkv_full)
    rest_full = lax.all_gather(rest_own, every, axis=0, tiled=True)

    def rest_block(index):
        return rest_full[:, index * model_width : (index + 1) * model_width]

    proj_full = rest_block(0)
    up_parts = [rest_block(1 + index) for index in range(BLOCKS)]
    down_parts = [rest_block(1 + BLOCKS + index) for index in range(BLOCKS)]

    inner_own = expert_in[0]
    outer_own = expert_out[0]
    inner_chip = [inner_first, None]
    outer_chip = [None, None]

    capacity = token_count // experts
    chosen = assignment.reshape(token_count)
    one_hot = (chosen[:, None] == jnp.arange(experts, dtype=jnp.int32)[None, :]).astype(jnp.int32)
    rank_within = jnp.sum((jnp.cumsum(one_hot, axis=0) - 1) * one_hot, axis=1)
    slot_index = chosen * capacity + rank_within
    source_of = (
        jnp.zeros((token_count,), jnp.int32)
        .at[slot_index]
        .set(jnp.arange(token_count, dtype=jnp.int32))
    )

    tokens_flat = block_input.reshape(token_count, model_width).astype(f32)
    normed_attn = layer_norm(tokens_flat, gain_attn).astype(bf16)
    kv_own = product(normed_attn, qkv_full[:, model_width : 3 * model_width]).astype(bf16)
    kv_own = kv_own.reshape(row_count, local_len, 2 * model_width)
    query = product(normed_attn, qkv_full[:, :model_width]).astype(bf16)
    query = query.reshape(row_count, local_len, model_width)

    kv_far = seq_send(kv_own, [(0, 2), (1, 3)])
    kv_near = seq_send(
        jnp.where(seq_index == 3, kv_far, kv_own), [(0, 1), (2, 3), (3, 2)]
    )
    kv_blocks = (kv_own, kv_near, kv_far)
    before = 2 * local_len
    offset = seq_index * local_len
    padded_seg = jnp.pad(segment_ids, ((0, 0), (before, 0)), constant_values=-1)
    key_seg = lax.dynamic_slice_in_dim(padded_seg, offset, before + local_len, 1)
    query_seg = key_seg[:, before:]
    key_pos = jnp.arange(before + local_len)
    query_pos = before + jnp.arange(local_len)
    allowed = (key_seg[:, :, None] == query_seg[:, None, :]) & (
        key_pos[None, :, None] <= query_pos[None, None, :]
    )
    bias = jnp.where(allowed, 0.0, -1e30).astype(f32)

    attended_rows, outer_chip[0] = attend(query, kv_blocks, bias, outer_own)
    late = together(inner_own[1], outer_own[1], attended_rows)
    inner_chip[1], outer_chip[1] = [swap_chip(part) for part in late[:2]]
    attended = attended_rows.reshape(token_count, model_width)
    hidden = tokens_flat + product(attended, proj_full)
    normed_ffn = layer_norm(hidden, gain_ffn).astype(bf16)
    dense_out, dense_kept = ffn_forward(normed_ffn, up_parts, down_parts, hidden)
    routed = dense_out.astype(bf16)

    received = lax.all_to_all(routed[source_of], "wide", split_axis=0, concat_axis=0, tiled=True)
    received, inner_chip[1] = together(received, inner_chip[1])
    received_f = received.astype(f32)
    inner_both = [swap_core(together(inner_chip[0], attended)[0]), None]
    outer_both = [swap_core(together(outer_chip[0], attended)[0]), None]
    centroid_row = centroids[0]
    centroid_f = centroid_row.astype(f32)
    logit_row = jnp.dot(received, centroid_row, preferred_element_type=f32)
    gate_value = jax.nn.sigmoid(logit_row)
    gains_f = expert_norms[0].astype(f32)
    state_now = received_f
    kept_layers = []
    slices = []
    for sublayer in range(2):
        if sublayer:
            inner_both[1] = swap_core(together(inner_chip[1], state_now)[0])
            outer_both[1] = swap_core(together(outer_chip[1], state_now)[0])
        inner_parts = [part[sublayer] for part in (inner_own, inner_core, inner_chip, inner_both)]
        outer_parts = [part[sublayer] for part in (outer_own, outer_core, outer_chip, outer_both)]
        normed = layer_norm(state_now, gains_f[sublayer]).astype(bf16)
        state_next, kept = ffn_forward(normed, inner_parts, outer_parts, state_now)
        kept_layers.append((state_now, normed, kept))
        slices.append((inner_parts, outer_parts))
        state_now = state_next
    returned = (gate_value[:, None] * state_now).astype(bf16)
    back_rows = lax.all_to_all(returned, "wide", split_axis=0, concat_axis=0, tiled=True)
    output = (
        (dense_out + back_rows[slot_index].astype(f32)).astype(bf16).reshape(block_input.shape)
    )
    gate_sum = jnp.sum(gate_value)
    score_sum = jnp.sum(logit_row * logit_row)
    grad_flat = grad_out.reshape(token_count, model_width)
    grad_back = lax.all_to_all(
        grad_flat[source_of], "wide", split_axis=0, concat_axis=0, tiled=True
    )
    grad_ret = grad_back.astype(f32)
    grad_gate = jnp.sum(grad_ret * state_now, axis=-1)
    grad_state = grad_ret * gate_value[:, None]
    gain_grads = [None, None]
    weight_terms = [None, None]
    sums = [None, None]
    for sublayer in (1, 0):
        state_in, normed_in, kept = kept_layers[sublayer]
        inner_parts, outer_parts = slices[sublayer]
        grad_branch = grad_state.astype(bf16)
        grad_pres, grad_normed = ffn_backward(kept, inner_parts, outer_parts, grad_branch)
        weight_terms[sublayer] = (
            [(act, grad_branch) for act, _ in kept],
            [(normed_in, grad_pre) for grad_pre in grad_pres],
        )
        grad_resid, gain_grad = norm_back(state_in, gains_f[sublayer], grad_normed)
        grad_state = grad_state + grad_resid
        gain_grads[sublayer] = gain_grad
        sums[sublayer] = [SliceSum(operands) for operands in weight_terms[sublayer]]
        if sublayer:
            grad_state, *held = together(grad_state, *[part.term(3) for part in sums[1]])
            for part, values in zip(sums[1], held):
                part.send_both(values)
    grad_logit = grad_gate * gate_value * (1.0 - gate_value)
    grad_routed = (grad_state + grad_logit[:, None] * centroid_f[None, :]).astype(bf16)
    centroid_grad = jnp.dot(grad_logit, received_f, precision=highest)
    grad_routed, *held = together(grad_routed, *[part.chip_sum() for part in sums[1]])
    for part, values in zip(sums[1], held):
        part.send_chip(values)
    returned_grad = lax.all_to_all(grad_routed, "wide", split_axis=0, concat_axis=0, tiled=True)
    returned_grad, *held = together(
        returned_grad,
        *[part.term(3) for part in sums[0]],
        *[part.term(1) for part in sums[1]],
        *[part.term(0) for part in sums[1]],
    )
    for part, values in zip(sums[0], held[:2]):
        part.send_both(values)
    for part, values in zip(sums[1], held[2:4]):
        part.send_core(values)
    for part, values in zip(sums[1], held[4:]):
        part.own = values
    grad_dense = grad_flat.astype(f32) + returned_grad[slot_index].astype(f32)

    grad_down_in = grad_dense.astype(bf16)
    grad_pres, grad_normed_ffn = ffn_backward(dense_kept, up_parts, down_parts, grad_down_in)
    grad_hidden_norm, grad_gain_ffn = norm_back(hidden, gain_ffn, grad_normed_ffn)
    grad_hidden = grad_dense + grad_hidden_norm
    outer1, inner1 = sums[1]
    outer0, inner0 = sums[0]
    grad_hidden, outer1.got_chip = together(grad_hidden, outer1.got_chip)
    grad_proj = grad_hidden.astype(bf16)
    rest_grad = jnp.concatenate(
        [weight_grad(attended, grad_proj)]
        + [weight_grad(normed_ffn, grad_pre) for grad_pre in grad_pres]
        + [weight_grad(act, grad_down_in) for act, _ in dense_kept],
        axis=1,
    )
    rest_grad = row_major(rest_grad)
    grad_attended = product_bt(grad_proj, proj_full).astype(bf16)
    grad_attended, rest_grad = together(grad_attended, rest_grad)
    grad_attended, inner1.got_chip = together(grad_attended, inner1.got_chip)
    rest_sum = lax.psum_scatter(rest_grad, every, scatter_dimension=0, tiled=True).astype(f32)
    grad_rows = grad_attended.reshape(query.shape)
    query_rows, kv_rows, far_rows = [], [], []
    for row in range(row_count):
        if row:
            grad_rows, far_rows[-1] = together(grad_rows, far_rows[-1])
            far_rows[-1] = seq_send(far_rows[-1], [(2, 0), (3, 1)])
        grad_query, grad_kv0, grad_kv1, grad_kv2 = attend_back(
            query, kv_blocks, bias, grad_rows, row
        )
        if row:
            grad_kv1, far_rows[-1] = together(grad_kv1, far_rows[-1])
        got_near = seq_send(grad_kv1, [(1, 0), (3, 2), (2, 3)])
        far_sum = jnp.where(
            seq_index == 3, (grad_kv2.astype(f32) + got_near.astype(f32)).astype(bf16), grad_kv2
        )
        near_sum = grad_kv0.astype(f32) + jnp.where(
            seq_index % 2 == 0, got_near.astype(f32), 0.0
        )
        query_rows.append(grad_query)
        kv_rows.append(near_sum)
        far_rows.append(far_sum)
    got_far = seq_send(far_rows[-1], [(2, 0), (3, 1)])
    got_far, *held = together(
        got_far, *[part.term(1) for part in sums[0]], *[part.term(0) for part in sums[0]]
    )
    for part, values in zip(sums[0], held[:2]):
        part.send_core(values)
    for part, values in zip(sums[0], held[2:]):
        part.own = values
    outer_send, inner_send, got_far = together(outer0.chip_sum(), inner0.chip_sum(), got_far)
    outer0.send_chip(outer_send)
    inner0.send_chip(inner_send)
    far_rows[-1] = got_far
    kv_sum = jnp.concatenate(
        [(near + far.astype(f32)).astype(bf16) for near, far in zip(kv_rows, far_rows)], axis=1
    ).reshape(2, token_count, model_width)
    grad_query = jnp.concatenate(query_rows, axis=0)
    grad_qkv = [grad_query.reshape(token_count, model_width), kv_sum[0], kv_sum[1]]
    qkv_grad = row_major(
        jnp.concatenate([weight_grad(normed_attn, part) for part in grad_qkv], axis=1)
    )
    grad_normed_attn = sum(
        product_bt(part, qkv_full[:, index * model_width : (index + 1) * model_width])
        for index, part in enumerate(grad_qkv)
    )
    grad_input_norm, grad_gain_attn = norm_back(tokens_flat, gain_attn, grad_normed_attn)
    grad_input = (grad_hidden + grad_input_norm).reshape(block_input.shape)

    gain_terms = jnp.stack([grad_gain_attn, grad_gain_ffn]).reshape(2, devices, shard)
    gain_terms, qkv_grad = together(gain_terms.transpose(1, 0, 2), qkv_grad)
    gain_terms = lax.all_to_all(gain_terms, every, 0, 0, tiled=True)
    qkv_sum = scatter_rows(qkv_grad)
    gain_sums = jnp.sum(gain_terms, axis=0)
    totals = jnp.concatenate(
        [
            jnp.stack(gain_grads),
            centroid_grad.reshape(1, model_width),
            jnp.pad(jnp.stack([gate_sum, score_sum]), (0, model_width - 2))[None],
        ]
    )
    totals = totals + swap_core(totals)
    totals = totals + swap_chip(totals)
    up_grad = (
        rest_sum[:, model_width : model_width + hidden_width]
        .reshape(shard, BLOCKS, devices, shard)
        .transpose(0, 2, 1, 3)
        .reshape(shard, hidden_width)
    )
    down_grad = (
        rest_sum[:, model_width + hidden_width :]
        .reshape(shard, BLOCKS, model_width)
        .transpose(1, 0, 2)
        .reshape(BLOCKS * shard, model_width)
    )
    token_total = token_count * seq_devices
    return (
        output,
        grad_input,
        gain_sums[0],
        qkv_sum,
        rest_sum[:, :model_width],
        gain_sums[1],
        up_grad,
        down_grad,
        totals[2:3],
        totals[:2][None],
        jnp.stack([inner0.total(), inner1.total()])[None],
        jnp.stack([outer0.total(), outer1.total()])[None],
        totals[3, :1] / token_total,
        totals[3, 1:2] / token_total,
    )


def solution(mesh):
    in_specs = (
        P("wide", "seq", None),
        P("wide", None),
        P("wide", "seq"),
        P(("seq", "wide")),
        P(("seq", "wide"), None),
        P(("seq", "wide"), None),
        P(("seq", "wide")),
        P(("seq", "wide"), None),
        P(("seq", "wide"), None),
        P("wide", None),
        P("wide", None, None),
        P("wide", None, None, "seq"),
        P("wide", None, "seq", None),
        P("wide", "seq", None),
    )
    out_specs = (
        P("wide", "seq", None),
        P("wide", "seq", None),
        P(("seq", "wide")),
        P(("seq", "wide"), None),
        P(("seq", "wide"), None),
        P(("seq", "wide")),
        P(("seq", "wide"), None),
        P(("seq", "wide"), None),
        P("wide", None),
        P("wide", None, None),
        P("wide", None, None, "seq"),
        P("wide", None, "seq", None),
        P("wide"),
        P("wide"),
    )
    return jax.shard_map(
        per_device, mesh=mesh, in_specs=in_specs, out_specs=out_specs, check_vma=False
    )
```

```python
import functools
import math

import jax
import jax.numpy as jnp
from jax import lax
from jax.experimental import pallas as pl
from jax.experimental.layout import Layout, with_layout_constraint
from jax.experimental.pallas import tpu as pltpu
from jax.sharding import PartitionSpec as P

HEADS = 16
HEAD_DIM = 64
BLOCKS = 4
LANES = 128

epsilon = 1e-05
highest = lax.Precision.HIGHEST
bf16 = jnp.bfloat16
f32 = jnp.float32


def layer_norm(values, norm_gain):
    centered = values - jnp.mean(values, axis=-1, keepdims=True)
    variance = jnp.mean(centered * centered, axis=-1, keepdims=True)
    return centered * lax.rsqrt(variance + epsilon) * norm_gain


def norm_back(values, norm_gain, grad_normed):
    _, pull_back = jax.vjp(layer_norm, values, norm_gain)
    return pull_back(grad_normed)


def gelu_pair(values):
    cdf = 0.5 * (1.0 + lax.erf(values * math.sqrt(0.5)))
    density = jnp.exp(values * values * -0.5) * (1.0 / math.sqrt(2.0 * math.pi))
    return values * cdf, cdf + values * density


def product(left_side, right_side):
    return jnp.dot(left_side, right_side, preferred_element_type=f32)


def product_bt(left_side, right_side):
    return lax.dot_general(
        left_side, right_side, (((1,), (1,)), ((), ())), preferred_element_type=f32
    )


def product_at(left_side, right_side):
    return lax.dot_general(
        left_side, right_side, (((0,), (0,)), ((), ())), preferred_element_type=f32
    )


def row_major(values):
    return with_layout_constraint(values, Layout(major_to_minor=(0, 1)))


def weight_grad(left_side, right_side):
    return row_major(product_at(left_side, right_side).astype(bf16))


def seq_send(values, pairs):
    return lax.ppermute(values, "seq", pairs)


def swap_core(values):
    return seq_send(values, [(0, 1), (1, 0), (2, 3), (3, 2)])


def swap_chip(values):
    return seq_send(values, [(0, 2), (2, 0), (1, 3), (3, 1)])


def pair_probs(query, keys, bias, score_scale):
    scores = product_bt(keys, query) * score_scale + bias
    exp_scores = jnp.exp(scores - jnp.max(scores, axis=0, keepdims=True))
    return exp_scores * (1.0 / jnp.sum(exp_scores, axis=0, keepdims=True))


def ride_chip(source, target, send_sem, recv_sem):
    seq = lax.axis_index("seq")
    other = (lax.rem(seq + 2, 4), lax.axis_index("wide"))
    step = pl.program_id(0) * pl.num_programs(1) + pl.program_id(1)
    copy = pltpu.make_async_remote_copy(
        src_ref=source,
        dst_ref=target,
        send_sem=send_sem,
        recv_sem=recv_sem,
        device_id=other,
        device_id_type=pl.DeviceIdType.MESH,
    )

    @pl.when(step == 0)
    def _():
        barrier = pltpu.get_barrier_semaphore()
        pl.semaphore_signal(
            barrier, inc=1, device_id=other, device_id_type=pl.DeviceIdType.MESH
        )
        pl.semaphore_wait(barrier, 1)
        copy.start()

    @pl.when(step == pl.num_programs(0) * pl.num_programs(1) - 1)
    def _():
        copy.wait()


def attend_kernel(
    score_scale,
    q_ref,
    k0,
    v0,
    k1,
    v1,
    k2,
    v2,
    bias_ref,
    ride_ref,
    out_ref,
    rode_ref,
    send_sem,
    recv_sem,
):
    ride_chip(ride_ref.at[0], rode_ref, send_sem, recv_sem)
    bias = bias_ref[0]
    parts = []
    for head in range(2):
        cols = slice(head * HEAD_DIM, (head + 1) * HEAD_DIM)
        keys = jnp.concatenate([k2[0][:, cols], k1[0][:, cols], k0[0][:, cols]], axis=0)
        vals = jnp.concatenate([v2[0][:, cols], v1[0][:, cols], v0[0][:, cols]], axis=0)
        probs_low = pair_probs(q_ref[0][:, cols], keys, bias, score_scale).astype(bf16)
        parts.append(product_at(vals, probs_low))
    out_ref[0] = jnp.concatenate(parts, axis=0).T.astype(bf16)


def attend_back_kernel(
    score_scale,
    q_ref,
    k0,
    v0,
    k1,
    v1,
    k2,
    v2,
    bias_ref,
    grad_ref,
    dq_ref,
    d0,
    d1,
    d2,
):
    bias = bias_ref[0]
    dq_parts, dk_parts, dv_parts = [], [], []
    for head in range(2):
        cols = slice(head * HEAD_DIM, (head + 1) * HEAD_DIM)
        query = q_ref[0][:, cols]
        grad_att = grad_ref[0][:, cols]
        keys = jnp.concatenate([k2[0][:, cols], k1[0][:, cols], k0[0][:, cols]], axis=0)
        vals = jnp.concatenate([v2[0][:, cols], v1[0][:, cols], v0[0][:, cols]], axis=0)
        probs = pair_probs(query, keys, bias, score_scale)
        grad_probs = product_bt(vals, grad_att)
        dv_parts.append(product(probs.astype(bf16), grad_att))
        inner_sum = jnp.sum(probs * grad_probs, axis=0, keepdims=True)
        grad_scores = (probs * (grad_probs - inner_sum)).astype(bf16)
        dk_parts.append(product(grad_scores, query) * score_scale)
        dq_parts.append(product_at(keys, grad_scores) * score_scale)
    dq_ref[0] = jnp.concatenate(dq_parts, axis=0).T.astype(bf16)
    d_keys = jnp.concatenate(dk_parts, axis=1).astype(bf16)
    d_vals = jnp.concatenate(dv_parts, axis=1).astype(bf16)
    size = d_keys.shape[0] // 3
    for place, ref in enumerate((d2, d1, d0)):
        ref[0, 0] = d_keys[place * size : (place + 1) * size]
        ref[1, 0] = d_vals[place * size : (place + 1) * size]


def attention_specs(local_len, model_width, key_len):
    width = 2 * HEAD_DIM
    groups = model_width // width
    query = pl.BlockSpec((1, local_len, width), lambda row, head: (row, 0, head))
    values = pl.BlockSpec((1, local_len, width), lambda row, head: (row, 0, head + groups))
    bias = pl.BlockSpec((1, key_len, local_len), lambda row, head: (row, 0, 0))
    return groups, query, [query, query, values, query, values, query, values, bias]


def attend(query, kv_blocks, bias, ride):
    rows, local_len, model_width = query.shape
    groups, spec, in_specs = attention_specs(local_len, model_width, bias.shape[1])
    operands = [block for block in kv_blocks for _ in range(2)]
    flops = 4 * rows * model_width * local_len * bias.shape[1]
    return pl.pallas_call(
        functools.partial(attend_kernel, 1.0 / math.sqrt(HEAD_DIM)),
        grid=(rows, groups),
        in_specs=in_specs + [pl.BlockSpec(memory_space=pl.ANY)],
        out_specs=[spec, pl.BlockSpec(memory_space=pl.ANY)],
        out_shape=[
            jax.ShapeDtypeStruct(query.shape, bf16),
            jax.ShapeDtypeStruct(ride.shape[1:], ride.dtype),
        ],
        scratch_shapes=[pltpu.SemaphoreType.DMA, pltpu.SemaphoreType.DMA],
        compiler_params=pltpu.CompilerParams(collective_id=2, has_side_effects=True),
        cost_estimate=pl.CostEstimate(
            flops=flops * 6, bytes_accessed=8 * query.size * 2, transcendentals=0
        ),
        name="attend",
    )(query, *operands, bias, ride)


def attend_back(query, kv_blocks, bias, grad_attended):
    rows, local_len, model_width = query.shape
    groups, spec, in_specs = attention_specs(local_len, model_width, bias.shape[1])
    operands = [block for block in kv_blocks for _ in range(2)]
    pair_spec = pl.BlockSpec((2, 1, local_len, 2 * HEAD_DIM), lambda row, head: (0, row, 0, head))
    pair_shape = jax.ShapeDtypeStruct((2, rows, local_len, model_width), bf16)
    flops = 10 * rows * model_width * local_len * bias.shape[1]
    return pl.pallas_call(
        functools.partial(attend_back_kernel, 1.0 / math.sqrt(HEAD_DIM)),
        grid=(rows, groups),
        in_specs=in_specs + [spec],
        out_specs=[spec, pair_spec, pair_spec, pair_spec],
        out_shape=[jax.ShapeDtypeStruct(query.shape, bf16)] + [pair_shape] * 3,
        cost_estimate=pl.CostEstimate(
            flops=flops * 6, bytes_accessed=16 * query.size * 2, transcendentals=0
        ),
        name="attend_back",
    )(query, *operands, bias, grad_attended)


def ffn_forward(normed, inner_parts, outer_parts, residual):
    kept = []
    total = residual
    for inner, outer in zip(inner_parts, outer_parts):
        act, slope = gelu_pair(product(normed, inner))
        act = act.astype(bf16)
        kept.append((act, slope.astype(bf16)))
        total = total + product(act, outer)
    return total, kept


def ffn_backward(kept, inner_parts, outer_parts, grad_branch):
    grad_pres = []
    grad_normed = None
    for (act, slope), inner, outer in zip(kept, inner_parts, outer_parts):
        grad_pre = (product_bt(grad_branch, outer) * slope.astype(f32)).astype(bf16)
        grad_pres.append(grad_pre)
        piece = product_bt(grad_pre, inner)
        grad_normed = piece if grad_normed is None else grad_normed + piece
    return grad_pres, grad_normed


def slices_in_order(operands):
    seq = lax.axis_index("seq")
    terms = None
    for place, (left, right) in enumerate(operands):
        values = weight_grad(left, right)
        owner = seq + (1 - 2 * (seq % 2)) * (place % 2) + (2 - 4 * (seq // 2)) * (place // 2)
        if terms is None:
            terms = jnp.zeros((len(operands),) + values.shape, values.dtype)
        terms = lax.dynamic_update_index_in_dim(terms, values, owner, 0)
    return terms


class SliceSum:
    def __init__(self, operands):
        self.operands = operands

    def term(self, place):
        return weight_grad(*self.operands[place])

    def take(self, place, values):
        if place == 0:
            self.own = values
        elif place == 1:
            self.got_core = swap_core(values)
        else:
            self.got_both = swap_core(values)

    def chip_sum(self):
        values = product_at(*self.operands[2]) + self.got_both.astype(f32)
        return row_major(values.astype(bf16))

    def send_chip(self, values):
        self.got_chip = swap_chip(values)

    def total(self):
        return self.own.astype(f32) + self.got_core.astype(f32) + self.got_chip.astype(f32)


def cube_bits():
    bits = []
    for axis in ("seq", "wide"):
        count = lax.axis_size(axis).bit_length() - 1
        bits += [(axis, bit) for bit in reversed(range(count))]
    return bits


def cube_orders(bits):
    core = bits.index(("seq", 0))
    chip = bits.index(("seq", 1))
    wide = [place for place, (axis, _) in enumerate(bits) if axis == "wide"]
    if len(wide) == 3:
        far, near, across = wide
        return ((chip, far, near, across, core), (chip, across, far, near, core))
    return ((chip, *wide, core), (chip, *wide[2:], *wide[:2], core))


def cube_place(bits):
    index = {axis: lax.axis_index(axis) for axis in ("seq", "wide")}
    mine = [lax.rem(index[axis] // (1 << bit), 2) for axis, bit in bits]

    def partner(place):
        axis, bit = bits[place]
        other = dict(index)
        other[axis] = index[axis] + (1 - 2 * mine[place]) * (1 << bit)
        return (other["seq"], other["wide"])

    return mine, partner


def cube_barrier(bits, partner):
    barrier = pltpu.get_barrier_semaphore()
    for place in range(len(bits)):
        pl.semaphore_signal(
            barrier, inc=1, device_id=partner(place), device_id_type=pl.DeviceIdType.MESH
        )
    pl.semaphore_wait(barrier, len(bits))


def gather_kernel(
    bits,
    orders,
    own_ref,
    inner_ref,
    outer_ref,
    out_ref,
    inner_core_ref,
    outer_core_ref,
    inner_chip_ref,
    send_sem,
    recv_sem,
    copy_sem,
    ride_send,
    ride_recv,
):
    mine, partner = cube_place(bits)
    own_copy = pltpu.make_async_copy(own_ref, out_ref.at[tuple(mine)], copy_sem)
    own_copy.start()
    cube_barrier(bits, partner)
    own_copy.wait()
    width = own_ref.shape[1] // len(orders)
    core = partner(bits.index(("seq", 0)))
    chip = partner(bits.index(("seq", 1)))
    rides = [
        (inner_ref.at[0, 0], inner_chip_ref, chip),
        (inner_ref.at[0], inner_core_ref, core),
        (outer_ref.at[0], outer_core_ref, core),
    ]
    rides = [
        pltpu.make_async_remote_copy(
            src_ref=source,
            dst_ref=target,
            send_sem=ride_send.at[place],
            recv_sem=ride_recv.at[place],
            device_id=device,
            device_id_type=pl.DeviceIdType.MESH,
        )
        for place, (source, target, device) in enumerate(rides)
    ]
    copies = []
    held = [[False] * len(bits) for _ in orders]
    for stage in range(len(bits)):
        for color, order in enumerate(orders):
            if stage:
                copies[(stage - 1) * len(orders) + color].wait_recv()
                held[color][order[stage - 1]] = True
            place = tuple(
                slice(None) if whole else mine[axis] for axis, whole in enumerate(held[color])
            )
            ref = out_ref.at[place + (slice(None), pl.ds(color * width, width))]
            copy = pltpu.make_async_remote_copy(
                src_ref=ref,
                dst_ref=ref,
                send_sem=send_sem.at[color, stage],
                recv_sem=recv_sem.at[color, stage],
                device_id=partner(order[stage]),
                device_id_type=pl.DeviceIdType.MESH,
            )
            copy.start()
            copies.append(copy)
        if stage == 0:
            for ride in rides:
                ride.start()
    for copy in copies:
        copy.wait_send()
    for copy in copies[-len(orders) :]:
        copy.wait_recv()
    for ride in rides:
        ride.wait()


def gather_rows(own, expert_in, expert_out):
    bits = cube_bits()
    orders = cube_orders(bits)
    rows, width = own.shape
    anywhere = pl.BlockSpec(memory_space=pl.ANY)
    out, inner_core, outer_core, inner_chip = pl.pallas_call(
        functools.partial(gather_kernel, bits, orders),
        in_specs=[pl.BlockSpec(memory_space=pltpu.VMEM), anywhere, anywhere],
        out_specs=[anywhere] * 4,
        out_shape=[
            jax.ShapeDtypeStruct((2,) * len(bits) + (rows, width), own.dtype),
            jax.ShapeDtypeStruct(expert_in.shape[1:], expert_in.dtype),
            jax.ShapeDtypeStruct(expert_out.shape[1:], expert_out.dtype),
            jax.ShapeDtypeStruct(expert_in.shape[2:], expert_in.dtype),
        ],
        scratch_shapes=[
            pltpu.SemaphoreType.DMA((len(orders), len(bits))),
            pltpu.SemaphoreType.DMA((len(orders), len(bits))),
            pltpu.SemaphoreType.DMA,
            pltpu.SemaphoreType.DMA((3,)),
            pltpu.SemaphoreType.DMA((3,)),
        ],
        compiler_params=pltpu.CompilerParams(collective_id=0, has_side_effects=True),
        cost_estimate=pl.CostEstimate(flops=0, bytes_accessed=25 * own.size << 5, transcendentals=0),
        name="gather_rows",
    )(own, expert_in, expert_out)
    return out.reshape(rows << len(bits), width), inner_core, outer_core, inner_chip


def scatter_kernel(bits, orders, terms_ref, out_ref, *scratch):
    stages = len(bits)
    colors = len(orders)
    got = scratch[: colors * stages]
    sums = scratch[colors * stages : colors * (2 * stages - 1)]
    send_sem, recv_sem = scratch[colors * (2 * stages - 1) :]
    mine, partner = cube_place(bits)
    cube_barrier(bits, partner)
    width = terms_ref.shape[-1] // colors
    copies = []

    def half(color, stage, keep):
        done = orders[color][:stage]
        place = []
        for axis in range(stages):
            if axis in done:
                continue
            if axis == orders[color][stage]:
                place.append(mine[axis] if keep else 1 - mine[axis])
            else:
                place.append(slice(None))
        if stage == 0:
            return terms_ref.at[tuple(place) + (slice(None), pl.ds(color * width, width))]
        return sums[color * (stages - 1) + stage - 1].at[tuple(place)]

    for stage in range(stages + 1):
        for color in range(colors):
            if stage:
                copies[(stage - 1) * colors + color].wait_recv()
                kept = half(color, stage - 1, True)[...].astype(f32)
                total = kept + got[color * stages + stage - 1][...].astype(f32)
                if stage == stages:
                    out_ref[:, pl.ds(color * width, width)] = total
                    continue
                sums[color * (stages - 1) + stage - 1][...] = total.astype(bf16)
            copy = pltpu.make_async_remote_copy(
                src_ref=half(color, stage, False),
                dst_ref=got[color * stages + stage],
                send_sem=send_sem.at[color, stage],
                recv_sem=recv_sem.at[color, stage],
                device_id=partner(orders[color][stage]),
                device_id_type=pl.DeviceIdType.MESH,
            )
            copy.start()
            copies.append(copy)
    for copy in copies:
        copy.wait_send()


def scatter_rows(terms):
    bits = cube_bits()
    orders = [order[::-1] for order in cube_orders(bits)]
    colors = len(orders)
    stages = len(bits)
    rows = terms.shape[0] >> stages
    width = terms.shape[1]
    got = [
        pltpu.VMEM((2,) * (stages - 1 - stage) + (rows, width // colors), bf16)
        for _ in range(colors)
        for stage in range(stages)
    ]
    sums = [
        pltpu.VMEM((2,) * (stages - 1 - stage) + (rows, width // colors), bf16)
        for _ in range(colors)
        for stage in range(stages - 1)
    ]
    return pl.pallas_call(
        functools.partial(scatter_kernel, bits, orders),
        in_specs=[pl.BlockSpec(memory_space=pltpu.VMEM)],
        out_specs=pl.BlockSpec(memory_space=pltpu.VMEM),
        out_shape=jax.ShapeDtypeStruct((rows, width), f32),
        scratch_shapes=got
        + sums
        + [
            pltpu.SemaphoreType.DMA((colors, stages)),
            pltpu.SemaphoreType.DMA((colors, stages)),
        ],
        compiler_params=pltpu.CompilerParams(collective_id=1, has_side_effects=True),
        cost_estimate=pl.CostEstimate(flops=0, bytes_accessed=50 * terms.size, transcendentals=0),
        name="scatter_rows",
    )(terms.reshape((2,) * stages + (rows, width)))


def together(*values):
    return lax.optimization_barrier(values)


def per_device(
    block_input,
    segment_ids,
    assignment,
    norm_attn,
    weight_qkv,
    weight_proj,
    norm_ffn,
    weight_up,
    weight_down,
    centroids,
    expert_norms,
    expert_in,
    expert_out,
    grad_out,
):
    row_count, local_len, model_width = block_input.shape
    token_count = row_count * local_len
    seq_devices = lax.axis_size("seq")
    seq_index = lax.axis_index("seq")
    experts = lax.axis_size("wide")
    devices = seq_devices * experts
    every = ("seq", "wide")
    shard = weight_up.shape[0]
    hidden_width = weight_up.shape[1]

    gains_own = jnp.stack([norm_attn, norm_ffn], axis=1)
    first_own = jnp.concatenate(
        [weight_qkv, jnp.pad(gains_own, ((0, 0), (0, 2 * LANES - gains_own.shape[1])))], axis=1
    )
    qkv_full, inner_core, outer_core, inner_first = gather_rows(first_own, expert_in, expert_out)
    gains_all = qkv_full[:, 3 * model_width : 3 * model_width + 2].astype(f32).T
    gain_attn = gains_all[0]
    gain_ffn = gains_all[1]
    up_own = (
        weight_up.reshape(shard, devices, BLOCKS, shard)
        .transpose(0, 2, 1, 3)
        .reshape(shard, hidden_width)
    )
    down_own = weight_down.reshape(BLOCKS, shard, model_width).transpose(1, 0, 2)
    rest_own = jnp.concatenate(
        [weight_proj, up_own, down_own.reshape(shard, BLOCKS * model_width)], axis=1
    )
    rest_own, _ = together(rest_own, qkv_full)
    rest_full = lax.all_gather(rest_own, every, axis=0, tiled=True)

    def rest_block(index):
        return rest_full[:, index * model_width : (index + 1) * model_width]

    proj_full = rest_block(0)
    up_parts = [rest_block(1 + index) for index in range(BLOCKS)]
    down_parts = [rest_block(1 + BLOCKS + index) for index in range(BLOCKS)]

    inner_own = expert_in[0]
    outer_own = expert_out[0]
    inner_chip = [inner_first, None]
    outer_chip = [None, None]

    capacity = token_count // experts
    chosen = assignment.reshape(token_count)
    one_hot = (chosen[:, None] == jnp.arange(experts, dtype=jnp.int32)[None, :]).astype(jnp.int32)
    rank_within = jnp.sum((jnp.cumsum(one_hot, axis=0) - 1) * one_hot, axis=1)
    slot_index = chosen * capacity + rank_within
    source_of = (
        jnp.zeros((token_count,), jnp.int32)
        .at[slot_index]
        .set(jnp.arange(token_count, dtype=jnp.int32))
    )

    tokens_flat = block_input.reshape(token_count, model_width).astype(f32)
    normed_attn = layer_norm(tokens_flat, gain_attn).astype(bf16)
    kv_own = product(normed_attn, qkv_full[:, model_width : 3 * model_width]).astype(bf16)
    kv_own = kv_own.reshape(row_count, local_len, 2 * model_width)
    query = product(normed_attn, qkv_full[:, :model_width]).astype(bf16)
    query = query.reshape(row_count, local_len, model_width)

    kv_far = seq_send(kv_own, [(0, 2), (1, 3)])
    kv_near = seq_send(
        jnp.where(seq_index == 3, kv_far, kv_own), [(0, 1), (2, 3), (3, 2)]
    )
    kv_blocks = (kv_own, kv_near, kv_far)
    before = 2 * local_len
    offset = seq_index * local_len
    padded_seg = jnp.pad(segment_ids, ((0, 0), (before, 0)), constant_values=-1)
    key_seg = lax.dynamic_slice_in_dim(padded_seg, offset, before + local_len, 1)
    query_seg = key_seg[:, before:]
    key_pos = jnp.arange(before + local_len)
    query_pos = before + jnp.arange(local_len)
    allowed = (key_seg[:, :, None] == query_seg[:, None, :]) & (
        key_pos[None, :, None] <= query_pos[None, None, :]
    )
    bias = jnp.where(allowed, 0.0, -1e30).astype(f32)

    attended_rows, outer_chip[0] = attend(query, kv_blocks, bias, outer_own)
    late = together(inner_own[1], outer_own[1], attended_rows)
    inner_chip[1], outer_chip[1] = [swap_chip(part) for part in late[:2]]
    attended = attended_rows.reshape(token_count, model_width)
    hidden = tokens_flat + product(attended, proj_full)
    normed_ffn = layer_norm(hidden, gain_ffn).astype(bf16)
    dense_out, dense_kept = ffn_forward(normed_ffn, up_parts, down_parts, hidden)
    routed = dense_out.astype(bf16)

    received = lax.all_to_all(routed[source_of], "wide", split_axis=0, concat_axis=0, tiled=True)
    received, inner_chip[1] = together(received, inner_chip[1])
    received_f = received.astype(f32)
    inner_both = [swap_core(together(inner_chip[0], attended)[0]), None]
    outer_both = [swap_core(together(outer_chip[0], attended)[0]), None]
    centroid_row = centroids[0]
    centroid_f = centroid_row.astype(f32)
    logit_row = jnp.dot(received, centroid_row, preferred_element_type=f32)
    gate_value = jax.nn.sigmoid(logit_row)
    gains_f = expert_norms[0].astype(f32)
    state_now = received_f
    kept_layers = []
    slices = []
    for sublayer in range(2):
        if sublayer:
            inner_both[1] = swap_core(together(inner_chip[1], state_now)[0])
            outer_both[1] = swap_core(together(outer_chip[1], state_now)[0])
        inner_parts = [part[sublayer] for part in (inner_own, inner_core, inner_chip, inner_both)]
        outer_parts = [part[sublayer] for part in (outer_own, outer_core, outer_chip, outer_both)]
        normed = layer_norm(state_now, gains_f[sublayer]).astype(bf16)
        state_next, kept = ffn_forward(normed, inner_parts, outer_parts, state_now)
        kept_layers.append((state_now, normed, kept))
        slices.append((inner_parts, outer_parts))
        state_now = state_next
    returned = (gate_value[:, None] * state_now).astype(bf16)
    back_rows = lax.all_to_all(returned, "wide", split_axis=0, concat_axis=0, tiled=True)
    output = (
        (dense_out + back_rows[slot_index].astype(f32)).astype(bf16).reshape(block_input.shape)
    )
    gate_sum = jnp.sum(gate_value)
    score_sum = jnp.sum(logit_row * logit_row)
    grad_flat = grad_out.reshape(token_count, model_width)
    grad_back = lax.all_to_all(
        grad_flat[source_of], "wide", split_axis=0, concat_axis=0, tiled=True
    )
    grad_ret = grad_back.astype(f32)
    grad_gate = jnp.sum(grad_ret * state_now, axis=-1)
    grad_state = grad_ret * gate_value[:, None]
    gain_grads = [None, None]
    second_sums = []
    for sublayer in (1, 0):
        state_in, normed_in, kept = kept_layers[sublayer]
        inner_parts, outer_parts = slices[sublayer]
        grad_branch = grad_state.astype(bf16)
        outer_terms = [(act, grad_branch) for act, _ in kept]
        if sublayer:
            terms, grad_branch = together(slices_in_order(outer_terms), grad_branch)
            second_sums.append(lax.psum_scatter(terms, "seq", scatter_dimension=0, tiled=True))
        grad_pres, grad_normed = ffn_backward(kept, inner_parts, outer_parts, grad_branch)
        inner_terms = [(normed_in, grad_pre) for grad_pre in grad_pres]
        grad_resid, gain_grad = norm_back(state_in, gains_f[sublayer], grad_normed)
        grad_state = grad_state + grad_resid
        gain_grads[sublayer] = gain_grad
        if sublayer:
            terms, grad_state = together(slices_in_order(inner_terms), grad_state)
            second_sums.append(lax.psum_scatter(terms, "seq", scatter_dimension=0, tiled=True))
    outer0 = SliceSum(outer_terms)
    inner0 = SliceSum(inner_terms)
    grad_logit = grad_gate * gate_value * (1.0 - gate_value)
    grad_routed = (grad_state + grad_logit[:, None] * centroid_f[None, :]).astype(bf16)
    centroid_grad = jnp.dot(grad_logit, received_f, precision=highest)
    returned_grad = lax.all_to_all(grad_routed, "wide", split_axis=0, concat_axis=0, tiled=True)
    firsts = (outer0, inner0)
    for part in firsts:
        part.take(3, part.term(3))
    returned_grad, *held = together(
        returned_grad,
        *[part.term(place) for place in (1, 0) for part in firsts],
        *[part.chip_sum() for part in firsts],
    )
    for part, core, own, chip in zip(firsts, held[:2], held[2:4], held[4:]):
        part.take(1, core)
        part.take(0, own)
        part.send_chip(chip)
    grad_dense = grad_flat.astype(f32) + returned_grad[slot_index].astype(f32)

    grad_down_in = grad_dense.astype(bf16)
    grad_pres, grad_normed_ffn = ffn_backward(dense_kept, up_parts, down_parts, grad_down_in)
    grad_hidden_norm, grad_gain_ffn = norm_back(hidden, gain_ffn, grad_normed_ffn)
    grad_hidden = grad_dense + grad_hidden_norm
    grad_down_late, outer0.got_chip = together(grad_down_in, outer0.got_chip)
    grad_proj = grad_hidden.astype(bf16)
    rest_grad = jnp.concatenate(
        [weight_grad(attended, grad_proj)]
        + [weight_grad(normed_ffn, grad_pre) for grad_pre in grad_pres]
        + [weight_grad(act, grad_down_late) for act, _ in dense_kept],
        axis=1,
    )
    rest_grad = row_major(rest_grad)
    grad_attended = product_bt(grad_proj, proj_full).astype(bf16)
    grad_attended, rest_grad = together(grad_attended, rest_grad)
    rest_sum = lax.psum_scatter(rest_grad, every, scatter_dimension=0, tiled=True).astype(f32)
    grad_query, grad_kv0, grad_kv1, grad_kv2 = attend_back(
        query, kv_blocks, bias, grad_attended.reshape(query.shape)
    )
    grad_kv1, inner0.got_chip = together(grad_kv1, inner0.got_chip)
    got_near = seq_send(grad_kv1, [(1, 0), (3, 2), (2, 3)])
    far_sum = jnp.where(
        seq_index == 3, (grad_kv2.astype(f32) + got_near.astype(f32)).astype(bf16), grad_kv2
    )
    got_far = seq_send(far_sum, [(2, 0), (3, 1)])
    outer_total = jnp.stack([outer0.total(), second_sums[0][0].astype(f32)])
    inner_total = jnp.stack([inner0.total(), second_sums[1][0].astype(f32)])
    got_far, outer_total, inner_total = together(got_far, outer_total, inner_total)
    kv_sum = grad_kv0.astype(f32) + got_far.astype(f32)
    kv_sum = kv_sum + jnp.where(seq_index % 2 == 0, got_near.astype(f32), 0.0)
    kv_sum = kv_sum.astype(bf16).reshape(2, token_count, model_width)
    grad_qkv = [grad_query.reshape(token_count, model_width), kv_sum[0], kv_sum[1]]
    qkv_grad = row_major(
        jnp.concatenate([weight_grad(normed_attn, part) for part in grad_qkv], axis=1)
    )
    grad_normed_attn = sum(
        product_bt(part, qkv_full[:, index * model_width : (index + 1) * model_width])
        for index, part in enumerate(grad_qkv)
    )
    grad_input_norm, grad_gain_attn = norm_back(tokens_flat, gain_attn, grad_normed_attn)
    grad_input = (grad_hidden + grad_input_norm).reshape(block_input.shape)

    gain_terms = jnp.stack([grad_gain_attn, grad_gain_ffn]).reshape(2, devices, shard)
    gain_terms, qkv_grad = together(gain_terms.transpose(1, 0, 2), qkv_grad)
    gain_terms = lax.all_to_all(gain_terms, every, 0, 0, tiled=True)
    qkv_sum = scatter_rows(qkv_grad)
    gain_sums = jnp.sum(gain_terms, axis=0)
    totals = jnp.concatenate(
        [
            jnp.stack(gain_grads),
            centroid_grad.reshape(1, model_width),
            jnp.pad(jnp.stack([gate_sum, score_sum]), (0, model_width - 2))[None],
        ]
    )
    totals = totals + swap_core(totals)
    totals = totals + swap_chip(totals)
    up_grad = (
        rest_sum[:, model_width : model_width + hidden_width]
        .reshape(shard, BLOCKS, devices, shard)
        .transpose(0, 2, 1, 3)
        .reshape(shard, hidden_width)
    )
    down_grad = (
        rest_sum[:, model_width + hidden_width :]
        .reshape(shard, BLOCKS, model_width)
        .transpose(1, 0, 2)
        .reshape(BLOCKS * shard, model_width)
    )
    token_total = token_count * seq_devices
    return (
        output,
        grad_input,
        gain_sums[0],
        qkv_sum,
        rest_sum[:, :model_width],
        gain_sums[1],
        up_grad,
        down_grad,
        totals[2:3],
        totals[:2][None],
        inner_total[None],
        outer_total[None],
        totals[3, :1] / token_total,
        totals[3, 1:2] / token_total,
    )


def solution(mesh):
    in_specs = (
        P("wide", "seq", None),
        P("wide", None),
        P("wide", "seq"),
        P(("seq", "wide")),
        P(("seq", "wide"), None),
        P(("seq", "wide"), None),
        P(("seq", "wide")),
        P(("seq", "wide"), None),
        P(("seq", "wide"), None),
        P("wide", None),
        P("wide", None, None),
        P("wide", None, None, "seq"),
        P("wide", None, "seq", None),
        P("wide", "seq", None),
    )
    out_specs = (
        P("wide", "seq", None),
        P("wide", "seq", None),
        P(("seq", "wide")),
        P(("seq", "wide"), None),
        P(("seq", "wide"), None),
        P(("seq", "wide")),
        P(("seq", "wide"), None),
        P(("seq", "wide"), None),
        P("wide", None),
        P("wide", None, None),
        P("wide", None, None, "seq"),
        P("wide", None, "seq", None),
        P("wide"),
        P("wide"),
    )
    return jax.shard_map(
        per_device, mesh=mesh, in_specs=in_specs, out_specs=out_specs, check_vma=False
    )
```

```python
import functools
import math

import jax
import jax.numpy as jnp
from jax import lax
from jax.experimental import pallas as pl
from jax.experimental.layout import Layout, with_layout_constraint
from jax.experimental.pallas import tpu as pltpu
from jax.sharding import PartitionSpec as P

HEADS = 16
HEAD_DIM = 64
BLOCKS = 4
LANES = 128

epsilon = 1e-05
highest = lax.Precision.HIGHEST
bf16 = jnp.bfloat16
f32 = jnp.float32


def layer_norm(values, norm_gain):
    centered = values - jnp.mean(values, axis=-1, keepdims=True)
    variance = jnp.mean(centered * centered, axis=-1, keepdims=True)
    return centered * lax.rsqrt(variance + epsilon) * norm_gain


def norm_back(values, norm_gain, grad_normed):
    _, pull_back = jax.vjp(layer_norm, values, norm_gain)
    return pull_back(grad_normed)


def gelu_pair(values):
    cdf = 0.5 * (1.0 + lax.erf(values * math.sqrt(0.5)))
    density = jnp.exp(values * values * -0.5) * (1.0 / math.sqrt(2.0 * math.pi))
    return values * cdf, cdf + values * density


def product(left_side, right_side):
    return jnp.dot(left_side, right_side, preferred_element_type=f32)


def product_bt(left_side, right_side):
    return lax.dot_general(
        left_side, right_side, (((1,), (1,)), ((), ())), preferred_element_type=f32
    )


def product_at(left_side, right_side):
    return lax.dot_general(
        left_side, right_side, (((0,), (0,)), ((), ())), preferred_element_type=f32
    )


def row_major(values):
    return with_layout_constraint(values, Layout(major_to_minor=(0, 1)))


def weight_grad(left_side, right_side):
    return row_major(product_at(left_side, right_side).astype(bf16))


def seq_send(values, pairs):
    return lax.ppermute(values, "seq", pairs)


def swap_core(values):
    return seq_send(values, [(0, 1), (1, 0), (2, 3), (3, 2)])


def swap_chip(values):
    return seq_send(values, [(0, 2), (2, 0), (1, 3), (3, 1)])


def pair_probs(query, keys, bias, score_scale):
    scores = product_bt(keys, query) * score_scale + bias
    exp_scores = jnp.exp(scores - jnp.max(scores, axis=0, keepdims=True))
    return exp_scores * (1.0 / jnp.sum(exp_scores, axis=0, keepdims=True))


def ride_chip(source, target, send_sem, recv_sem):
    seq = lax.axis_index("seq")
    other = (lax.rem(seq + 2, 4), lax.axis_index("wide"))
    step = pl.program_id(0) * pl.num_programs(1) + pl.program_id(1)
    copy = pltpu.make_async_remote_copy(
        src_ref=source,
        dst_ref=target,
        send_sem=send_sem,
        recv_sem=recv_sem,
        device_id=other,
        device_id_type=pl.DeviceIdType.MESH,
    )

    @pl.when(step == 0)
    def _():
        barrier = pltpu.get_barrier_semaphore()
        pl.semaphore_signal(
            barrier, inc=1, device_id=other, device_id_type=pl.DeviceIdType.MESH
        )
        pl.semaphore_wait(barrier, 1)
        copy.start()

    @pl.when(step == pl.num_programs(0) * pl.num_programs(1) - 1)
    def _():
        copy.wait()


def attend_kernel(
    score_scale,
    q_ref,
    k0,
    v0,
    k1,
    v1,
    k2,
    v2,
    bias_ref,
    ride_ref,
    out_ref,
    rode_ref,
    send_sem,
    recv_sem,
):
    ride_chip(ride_ref.at[0], rode_ref, send_sem, recv_sem)
    bias = bias_ref[0]
    parts = []
    for head in range(2):
        cols = slice(head * HEAD_DIM, (head + 1) * HEAD_DIM)
        keys = jnp.concatenate([k2[0][:, cols], k1[0][:, cols], k0[0][:, cols]], axis=0)
        vals = jnp.concatenate([v2[0][:, cols], v1[0][:, cols], v0[0][:, cols]], axis=0)
        probs_low = pair_probs(q_ref[0][:, cols], keys, bias, score_scale).astype(bf16)
        parts.append(product_at(vals, probs_low))
    out_ref[0] = jnp.concatenate(parts, axis=0).T.astype(bf16)


def attend_back_kernel(
    score_scale,
    q_ref,
    k0,
    v0,
    k1,
    v1,
    k2,
    v2,
    bias_ref,
    grad_ref,
    dq_ref,
    d0,
    d1,
    d2,
):
    bias = bias_ref[0]
    dq_parts, dk_parts, dv_parts = [], [], []
    for head in range(2):
        cols = slice(head * HEAD_DIM, (head + 1) * HEAD_DIM)
        query = q_ref[0][:, cols]
        grad_att = grad_ref[0][:, cols]
        keys = jnp.concatenate([k2[0][:, cols], k1[0][:, cols], k0[0][:, cols]], axis=0)
        vals = jnp.concatenate([v2[0][:, cols], v1[0][:, cols], v0[0][:, cols]], axis=0)
        probs = pair_probs(query, keys, bias, score_scale)
        grad_probs = product_bt(vals, grad_att)
        dv_parts.append(product(probs.astype(bf16), grad_att))
        inner_sum = jnp.sum(probs * grad_probs, axis=0, keepdims=True)
        grad_scores = (probs * (grad_probs - inner_sum)).astype(bf16)
        dk_parts.append(product(grad_scores, query) * score_scale)
        dq_parts.append(product_at(keys, grad_scores) * score_scale)
    dq_ref[0] = jnp.concatenate(dq_parts, axis=0).T.astype(bf16)
    d_keys = jnp.concatenate(dk_parts, axis=1).astype(bf16)
    d_vals = jnp.concatenate(dv_parts, axis=1).astype(bf16)
    size = d_keys.shape[0] // 3
    for place, ref in enumerate((d2, d1, d0)):
        ref[0, 0] = d_keys[place * size : (place + 1) * size]
        ref[1, 0] = d_vals[place * size : (place + 1) * size]


def attention_specs(local_len, model_width, key_len):
    width = 2 * HEAD_DIM
    groups = model_width // width
    query = pl.BlockSpec((1, local_len, width), lambda row, head: (row, 0, head))
    values = pl.BlockSpec((1, local_len, width), lambda row, head: (row, 0, head + groups))
    bias = pl.BlockSpec((1, key_len, local_len), lambda row, head: (row, 0, 0))
    return groups, query, [query, query, values, query, values, query, values, bias]


def attend(query, kv_blocks, bias, ride):
    rows, local_len, model_width = query.shape
    groups, spec, in_specs = attention_specs(local_len, model_width, bias.shape[1])
    operands = [block for block in kv_blocks for _ in range(2)]
    flops = 4 * rows * model_width * local_len * bias.shape[1]
    return pl.pallas_call(
        functools.partial(attend_kernel, 1.0 / math.sqrt(HEAD_DIM)),
        grid=(rows, groups),
        in_specs=in_specs + [pl.BlockSpec(memory_space=pl.ANY)],
        out_specs=[spec, pl.BlockSpec(memory_space=pl.ANY)],
        out_shape=[
            jax.ShapeDtypeStruct(query.shape, bf16),
            jax.ShapeDtypeStruct(ride.shape[1:], ride.dtype),
        ],
        scratch_shapes=[pltpu.SemaphoreType.DMA, pltpu.SemaphoreType.DMA],
        compiler_params=pltpu.CompilerParams(collective_id=2, has_side_effects=True),
        cost_estimate=pl.CostEstimate(
            flops=flops * 6, bytes_accessed=8 * query.size * 2, transcendentals=0
        ),
        name="attend",
    )(query, *operands, bias, ride)


def attend_back(query, kv_blocks, bias, grad_attended):
    rows, local_len, model_width = query.shape
    groups, spec, in_specs = attention_specs(local_len, model_width, bias.shape[1])
    operands = [block for block in kv_blocks for _ in range(2)]
    pair_spec = pl.BlockSpec((2, 1, local_len, 2 * HEAD_DIM), lambda row, head: (0, row, 0, head))
    pair_shape = jax.ShapeDtypeStruct((2, rows, local_len, model_width), bf16)
    flops = 10 * rows * model_width * local_len * bias.shape[1]
    return pl.pallas_call(
        functools.partial(attend_back_kernel, 1.0 / math.sqrt(HEAD_DIM)),
        grid=(rows, groups),
        in_specs=in_specs + [spec],
        out_specs=[spec, pair_spec, pair_spec, pair_spec],
        out_shape=[jax.ShapeDtypeStruct(query.shape, bf16)] + [pair_shape] * 3,
        cost_estimate=pl.CostEstimate(
            flops=flops * 6, bytes_accessed=16 * query.size * 2, transcendentals=0
        ),
        name="attend_back",
    )(query, *operands, bias, grad_attended)


def ffn_forward(normed, inner_parts, outer_parts, residual):
    kept = []
    total = residual
    for inner, outer in zip(inner_parts, outer_parts):
        act, slope = gelu_pair(product(normed, inner))
        act = act.astype(bf16)
        kept.append((act, slope.astype(bf16)))
        total = total + product(act, outer)
    return total, kept


def ffn_backward(kept, inner_parts, outer_parts, grad_branch):
    grad_pres = []
    grad_normed = None
    for (act, slope), inner, outer in zip(kept, inner_parts, outer_parts):
        grad_pre = (product_bt(grad_branch, outer) * slope.astype(f32)).astype(bf16)
        grad_pres.append(grad_pre)
        piece = product_bt(grad_pre, inner)
        grad_normed = piece if grad_normed is None else grad_normed + piece
    return grad_pres, grad_normed


def slice_owner(place):
    seq = lax.axis_index("seq")
    return seq + (1 - 2 * (seq % 2)) * (place % 2) + (2 - 4 * (seq // 2)) * (place // 2)


def slices_in_order(terms, operands):
    for place, (left, right) in enumerate(operands):
        values = weight_grad(left, right)
        terms = lax.dynamic_update_index_in_dim(terms, values, slice_owner(place), 0)
    return terms


class SliceSum:
    def __init__(self, operands):
        self.operands = operands

    def term(self, place):
        return weight_grad(*self.operands[place])

    def take(self, place, values):
        if place == 0:
            self.own = values
        elif place == 1:
            self.got_core = swap_core(values)
        else:
            self.got_both = swap_core(values)

    def chip_sum(self):
        values = product_at(*self.operands[2]) + self.got_both.astype(f32)
        return row_major(values.astype(bf16))

    def send_chip(self, values):
        self.got_chip = swap_chip(values)

    def total(self):
        return self.own.astype(f32) + self.got_core.astype(f32) + self.got_chip.astype(f32)


def cube_bits():
    bits = []
    for axis in ("seq", "wide"):
        count = lax.axis_size(axis).bit_length() - 1
        bits += [(axis, bit) for bit in reversed(range(count))]
    return bits


def cube_orders(bits):
    core = bits.index(("seq", 0))
    chip = bits.index(("seq", 1))
    wide = [place for place, (axis, _) in enumerate(bits) if axis == "wide"]
    if len(wide) == 3:
        far, near, across = wide
        return ((chip, far, near, across, core), (chip, across, far, near, core))
    return ((chip, *wide, core), (chip, *wide[2:], *wide[:2], core))


def cube_place(bits):
    index = {axis: lax.axis_index(axis) for axis in ("seq", "wide")}
    mine = [lax.rem(index[axis] // (1 << bit), 2) for axis, bit in bits]

    def partner(place):
        axis, bit = bits[place]
        other = dict(index)
        other[axis] = index[axis] + (1 - 2 * mine[place]) * (1 << bit)
        return (other["seq"], other["wide"])

    return mine, partner


def cube_barrier(bits, partner):
    barrier = pltpu.get_barrier_semaphore()
    for place in range(len(bits)):
        pl.semaphore_signal(
            barrier, inc=1, device_id=partner(place), device_id_type=pl.DeviceIdType.MESH
        )
    pl.semaphore_wait(barrier, len(bits))


def gather_kernel(
    bits,
    orders,
    own_ref,
    inner_ref,
    outer_ref,
    out_ref,
    inner_core_ref,
    outer_core_ref,
    inner_chip_ref,
    send_sem,
    recv_sem,
    copy_sem,
    ride_send,
    ride_recv,
):
    mine, partner = cube_place(bits)
    own_copy = pltpu.make_async_copy(own_ref, out_ref.at[tuple(mine)], copy_sem)
    own_copy.start()
    cube_barrier(bits, partner)
    own_copy.wait()
    width = own_ref.shape[1] // len(orders)
    core = partner(bits.index(("seq", 0)))
    chip = partner(bits.index(("seq", 1)))
    rides = [
        (inner_ref.at[0, 0], inner_chip_ref, chip),
        (inner_ref.at[0], inner_core_ref, core),
        (outer_ref.at[0], outer_core_ref, core),
    ]
    rides = [
        pltpu.make_async_remote_copy(
            src_ref=source,
            dst_ref=target,
            send_sem=ride_send.at[place],
            recv_sem=ride_recv.at[place],
            device_id=device,
            device_id_type=pl.DeviceIdType.MESH,
        )
        for place, (source, target, device) in enumerate(rides)
    ]
    copies = []
    held = [[False] * len(bits) for _ in orders]
    for stage in range(len(bits)):
        for color, order in enumerate(orders):
            if stage:
                copies[(stage - 1) * len(orders) + color].wait_recv()
                held[color][order[stage - 1]] = True
            place = tuple(
                slice(None) if whole else mine[axis] for axis, whole in enumerate(held[color])
            )
            ref = out_ref.at[place + (slice(None), pl.ds(color * width, width))]
            copy = pltpu.make_async_remote_copy(
                src_ref=ref,
                dst_ref=ref,
                send_sem=send_sem.at[color, stage],
                recv_sem=recv_sem.at[color, stage],
                device_id=partner(order[stage]),
                device_id_type=pl.DeviceIdType.MESH,
            )
            copy.start()
            copies.append(copy)
        if stage == 0:
            for ride in rides:
                ride.start()
    for copy in copies:
        copy.wait_send()
    for copy in copies[-len(orders) :]:
        copy.wait_recv()
    for ride in rides:
        ride.wait()


def gather_rows(own, expert_in, expert_out):
    bits = cube_bits()
    orders = cube_orders(bits)
    rows, width = own.shape
    anywhere = pl.BlockSpec(memory_space=pl.ANY)
    out, inner_core, outer_core, inner_chip = pl.pallas_call(
        functools.partial(gather_kernel, bits, orders),
        in_specs=[pl.BlockSpec(memory_space=pltpu.VMEM), anywhere, anywhere],
        out_specs=[anywhere] * 4,
        out_shape=[
            jax.ShapeDtypeStruct((2,) * len(bits) + (rows, width), own.dtype),
            jax.ShapeDtypeStruct(expert_in.shape[1:], expert_in.dtype),
            jax.ShapeDtypeStruct(expert_out.shape[1:], expert_out.dtype),
            jax.ShapeDtypeStruct(expert_in.shape[2:], expert_in.dtype),
        ],
        scratch_shapes=[
            pltpu.SemaphoreType.DMA((len(orders), len(bits))),
            pltpu.SemaphoreType.DMA((len(orders), len(bits))),
            pltpu.SemaphoreType.DMA,
            pltpu.SemaphoreType.DMA((3,)),
            pltpu.SemaphoreType.DMA((3,)),
        ],
        compiler_params=pltpu.CompilerParams(collective_id=0, has_side_effects=True),
        cost_estimate=pl.CostEstimate(flops=0, bytes_accessed=25 * own.size << 5, transcendentals=0),
        name="gather_rows",
    )(own, expert_in, expert_out)
    return out.reshape(rows << len(bits), width), inner_core, outer_core, inner_chip


def scatter_kernel(bits, orders, terms_ref, out_ref, *scratch):
    stages = len(bits)
    colors = len(orders)
    got = scratch[: colors * stages]
    sums = scratch[colors * stages : colors * (2 * stages - 1)]
    send_sem, recv_sem = scratch[colors * (2 * stages - 1) :]
    mine, partner = cube_place(bits)
    cube_barrier(bits, partner)
    width = terms_ref.shape[-1] // colors
    copies = []

    def half(color, stage, keep):
        done = orders[color][:stage]
        place = []
        for axis in range(stages):
            if axis in done:
                continue
            if axis == orders[color][stage]:
                place.append(mine[axis] if keep else 1 - mine[axis])
            else:
                place.append(slice(None))
        if stage == 0:
            return terms_ref.at[tuple(place) + (slice(None), pl.ds(color * width, width))]
        return sums[color * (stages - 1) + stage - 1].at[tuple(place)]

    for stage in range(stages + 1):
        for color in range(colors):
            if stage:
                copies[(stage - 1) * colors + color].wait_recv()
                kept = half(color, stage - 1, True)[...].astype(f32)
                total = kept + got[color * stages + stage - 1][...].astype(f32)
                if stage == stages:
                    out_ref[:, pl.ds(color * width, width)] = total
                    continue
                sums[color * (stages - 1) + stage - 1][...] = total.astype(bf16)
            copy = pltpu.make_async_remote_copy(
                src_ref=half(color, stage, False),
                dst_ref=got[color * stages + stage],
                send_sem=send_sem.at[color, stage],
                recv_sem=recv_sem.at[color, stage],
                device_id=partner(orders[color][stage]),
                device_id_type=pl.DeviceIdType.MESH,
            )
            copy.start()
            copies.append(copy)
    for copy in copies:
        copy.wait_send()


def scatter_rows(terms):
    bits = cube_bits()
    orders = [order[::-1] for order in cube_orders(bits)]
    colors = len(orders)
    stages = len(bits)
    rows = terms.shape[0] >> stages
    width = terms.shape[1]
    got = [
        pltpu.VMEM((2,) * (stages - 1 - stage) + (rows, width // colors), bf16)
        for _ in range(colors)
        for stage in range(stages)
    ]
    sums = [
        pltpu.VMEM((2,) * (stages - 1 - stage) + (rows, width // colors), bf16)
        for _ in range(colors)
        for stage in range(stages - 1)
    ]
    return pl.pallas_call(
        functools.partial(scatter_kernel, bits, orders),
        in_specs=[pl.BlockSpec(memory_space=pltpu.VMEM)],
        out_specs=pl.BlockSpec(memory_space=pltpu.VMEM),
        out_shape=jax.ShapeDtypeStruct((rows, width), f32),
        scratch_shapes=got
        + sums
        + [
            pltpu.SemaphoreType.DMA((colors, stages)),
            pltpu.SemaphoreType.DMA((colors, stages)),
        ],
        compiler_params=pltpu.CompilerParams(collective_id=1, has_side_effects=True),
        cost_estimate=pl.CostEstimate(flops=0, bytes_accessed=50 * terms.size, transcendentals=0),
        name="scatter_rows",
    )(terms.reshape((2,) * stages + (rows, width)))


def together(*values):
    return lax.optimization_barrier(values)


def per_device(
    block_input,
    segment_ids,
    assignment,
    norm_attn,
    weight_qkv,
    weight_proj,
    norm_ffn,
    weight_up,
    weight_down,
    centroids,
    expert_norms,
    expert_in,
    expert_out,
    grad_out,
):
    row_count, local_len, model_width = block_input.shape
    token_count = row_count * local_len
    seq_devices = lax.axis_size("seq")
    seq_index = lax.axis_index("seq")
    experts = lax.axis_size("wide")
    devices = seq_devices * experts
    every = ("seq", "wide")
    shard = weight_up.shape[0]
    hidden_width = weight_up.shape[1]

    gains_own = jnp.stack([norm_attn, norm_ffn], axis=1)
    first_own = jnp.concatenate(
        [weight_qkv, jnp.pad(gains_own, ((0, 0), (0, 2 * LANES - gains_own.shape[1])))], axis=1
    )
    qkv_full, inner_core, outer_core, inner_first = gather_rows(first_own, expert_in, expert_out)
    gains_all = qkv_full[:, 3 * model_width : 3 * model_width + 2].astype(f32).T
    gain_attn = gains_all[0]
    gain_ffn = gains_all[1]
    up_own = (
        weight_up.reshape(shard, devices, BLOCKS, shard)
        .transpose(0, 2, 1, 3)
        .reshape(shard, hidden_width)
    )
    down_own = weight_down.reshape(BLOCKS, shard, model_width).transpose(1, 0, 2)
    rest_own = jnp.concatenate(
        [weight_proj, up_own, down_own.reshape(shard, BLOCKS * model_width)], axis=1
    )
    rest_own, _ = together(rest_own, qkv_full)
    rest_full = lax.all_gather(rest_own, every, axis=0, tiled=True)

    def rest_block(index):
        return rest_full[:, index * model_width : (index + 1) * model_width]

    proj_full = rest_block(0)
    up_parts = [rest_block(1 + index) for index in range(BLOCKS)]
    down_parts = [rest_block(1 + BLOCKS + index) for index in range(BLOCKS)]

    inner_own = expert_in[0]
    outer_own = expert_out[0]
    inner_chip = [inner_first, None]
    outer_chip = [None, None]

    capacity = token_count // experts
    chosen = assignment.reshape(token_count)
    one_hot = (chosen[:, None] == jnp.arange(experts, dtype=jnp.int32)[None, :]).astype(jnp.int32)
    rank_within = jnp.sum((jnp.cumsum(one_hot, axis=0) - 1) * one_hot, axis=1)
    slot_index = chosen * capacity + rank_within
    source_of = (
        jnp.zeros((token_count,), jnp.int32)
        .at[slot_index]
        .set(jnp.arange(token_count, dtype=jnp.int32))
    )

    tokens_flat = block_input.reshape(token_count, model_width).astype(f32)
    normed_attn = layer_norm(tokens_flat, gain_attn).astype(bf16)
    kv_own = product(normed_attn, qkv_full[:, model_width : 3 * model_width]).astype(bf16)
    kv_own = kv_own.reshape(row_count, local_len, 2 * model_width)
    query = product(normed_attn, qkv_full[:, :model_width]).astype(bf16)
    query = query.reshape(row_count, local_len, model_width)

    kv_far = seq_send(kv_own, [(0, 2), (1, 3)])
    kv_near = seq_send(
        jnp.where(seq_index == 3, kv_far, kv_own), [(0, 1), (2, 3), (3, 2)]
    )
    kv_blocks = (kv_own, kv_near, kv_far)
    before = 2 * local_len
    offset = seq_index * local_len
    padded_seg = jnp.pad(segment_ids, ((0, 0), (before, 0)), constant_values=-1)
    key_seg = lax.dynamic_slice_in_dim(padded_seg, offset, before + local_len, 1)
    query_seg = key_seg[:, before:]
    key_pos = jnp.arange(before + local_len)
    query_pos = before + jnp.arange(local_len)
    allowed = (key_seg[:, :, None] == query_seg[:, None, :]) & (
        key_pos[None, :, None] <= query_pos[None, None, :]
    )
    bias = jnp.where(allowed, 0.0, -1e30).astype(f32)

    attended_rows, outer_chip[0] = attend(query, kv_blocks, bias, outer_own)
    inner_chip[1] = swap_chip(together(inner_own[1], attended_rows)[0])
    outer_late, _ = together(outer_own[1], rest_full)
    outer_all = lax.all_gather(outer_late, "seq", axis=0)

    attended = attended_rows.reshape(token_count, model_width)
    hidden = tokens_flat + product(attended, proj_full)
    normed_ffn = layer_norm(hidden, gain_ffn).astype(bf16)
    dense_out, dense_kept = ffn_forward(normed_ffn, up_parts, down_parts, hidden)
    routed = dense_out.astype(bf16)

    received = lax.all_to_all(routed[source_of], "wide", split_axis=0, concat_axis=0, tiled=True)
    fresh = [jnp.zeros((seq_devices,) + part.shape[1:], bf16) for part in (outer_own, inner_own)]
    received, inner_chip[1], *fresh = together(received, inner_chip[1], *fresh)
    received_f = received.astype(f32)
    inner_both = [swap_core(together(inner_chip[0], attended)[0]), None]
    outer_both = [swap_core(together(outer_chip[0], attended)[0]), None]
    centroid_row = centroids[0]
    centroid_f = centroid_row.astype(f32)
    logit_row = jnp.dot(received, centroid_row, preferred_element_type=f32)
    gate_value = jax.nn.sigmoid(logit_row)
    gains_f = expert_norms[0].astype(f32)
    state_now = received_f
    kept_layers = []
    slices = []
    for sublayer in range(2):
        if sublayer:
            inner_both[1] = swap_core(together(inner_chip[1], state_now)[0])
        inner_parts = [part[sublayer] for part in (inner_own, inner_core, inner_chip, inner_both)]
        if sublayer:
            outer_parts = [
                lax.dynamic_index_in_dim(outer_all, slice_owner(place), 0, keepdims=False)
                for place in range(len(inner_parts))
            ]
        else:
            outer_parts = [part[0] for part in (outer_own, outer_core, outer_chip, outer_both)]
        normed = layer_norm(state_now, gains_f[sublayer]).astype(bf16)
        state_next, kept = ffn_forward(normed, inner_parts, outer_parts, state_now)
        kept_layers.append((state_now, normed, kept))
        slices.append((inner_parts, outer_parts))
        state_now = state_next
    returned = (gate_value[:, None] * state_now).astype(bf16)
    back_rows = lax.all_to_all(returned, "wide", split_axis=0, concat_axis=0, tiled=True)
    output = (
        (dense_out + back_rows[slot_index].astype(f32)).astype(bf16).reshape(block_input.shape)
    )
    gate_sum = jnp.sum(gate_value)
    score_sum = jnp.sum(logit_row * logit_row)
    grad_flat = grad_out.reshape(token_count, model_width)
    grad_back = lax.all_to_all(
        grad_flat[source_of], "wide", split_axis=0, concat_axis=0, tiled=True
    )
    grad_ret = grad_back.astype(f32)
    grad_gate = jnp.sum(grad_ret * state_now, axis=-1)
    grad_state = grad_ret * gate_value[:, None]
    gain_grads = [None, None]
    second_sums = []
    for sublayer in (1, 0):
        state_in, normed_in, kept = kept_layers[sublayer]
        inner_parts, outer_parts = slices[sublayer]
        grad_branch = grad_state.astype(bf16)
        outer_terms = [(act, grad_branch) for act, _ in kept]
        if sublayer:
            terms, grad_branch = together(slices_in_order(fresh[0], outer_terms), grad_branch)
            second_sums.append(lax.psum_scatter(terms, "seq", scatter_dimension=0, tiled=True))
        grad_pres, grad_normed = ffn_backward(kept, inner_parts, outer_parts, grad_branch)
        inner_terms = [(normed_in, grad_pre) for grad_pre in grad_pres]
        grad_resid, gain_grad = norm_back(state_in, gains_f[sublayer], grad_normed)
        grad_state = grad_state + grad_resid
        gain_grads[sublayer] = gain_grad
        if sublayer:
            terms, grad_state = together(slices_in_order(fresh[1], inner_terms), grad_state)
            second_sums.append(lax.psum_scatter(terms, "seq", scatter_dimension=0, tiled=True))
    outer0 = SliceSum(outer_terms)
    inner0 = SliceSum(inner_terms)
    grad_logit = grad_gate * gate_value * (1.0 - gate_value)
    grad_routed = (grad_state + grad_logit[:, None] * centroid_f[None, :]).astype(bf16)
    centroid_grad = jnp.dot(grad_logit, received_f, precision=highest)
    returned_grad = lax.all_to_all(grad_routed, "wide", split_axis=0, concat_axis=0, tiled=True)
    firsts = (outer0, inner0)
    for part in firsts:
        part.take(3, part.term(3))
    returned_grad, *held = together(
        returned_grad,
        *[part.term(place) for place in (1, 0) for part in firsts],
        *[part.chip_sum() for part in firsts],
    )
    for part, core, own, chip in zip(firsts, held[:2], held[2:4], held[4:]):
        part.take(1, core)
        part.take(0, own)
        part.send_chip(chip)
    grad_dense = grad_flat.astype(f32) + returned_grad[slot_index].astype(f32)

    grad_down_in = grad_dense.astype(bf16)
    grad_pres, grad_normed_ffn = ffn_backward(dense_kept, up_parts, down_parts, grad_down_in)
    grad_hidden_norm, grad_gain_ffn = norm_back(hidden, gain_ffn, grad_normed_ffn)
    grad_hidden = grad_dense + grad_hidden_norm
    grad_down_late, outer0.got_chip = together(grad_down_in, outer0.got_chip)
    grad_proj = grad_hidden.astype(bf16)
    rest_grad = jnp.concatenate(
        [weight_grad(attended, grad_proj)]
        + [weight_grad(normed_ffn, grad_pre) for grad_pre in grad_pres]
        + [weight_grad(act, grad_down_late) for act, _ in dense_kept],
        axis=1,
    )
    rest_grad = row_major(rest_grad)
    grad_attended = product_bt(grad_proj, proj_full).astype(bf16)
    grad_attended, rest_grad = together(grad_attended, rest_grad)
    rest_sum = lax.psum_scatter(rest_grad, every, scatter_dimension=0, tiled=True).astype(f32)
    grad_query, grad_kv0, grad_kv1, grad_kv2 = attend_back(
        query, kv_blocks, bias, grad_attended.reshape(query.shape)
    )
    grad_kv1, inner0.got_chip = together(grad_kv1, inner0.got_chip)
    got_near = seq_send(grad_kv1, [(1, 0), (3, 2), (2, 3)])
    far_sum = jnp.where(
        seq_index == 3, (grad_kv2.astype(f32) + got_near.astype(f32)).astype(bf16), grad_kv2
    )
    got_far = seq_send(far_sum, [(2, 0), (3, 1)])
    outer_total = jnp.stack([outer0.total(), second_sums[0][0].astype(f32)])
    inner_total = jnp.stack([inner0.total(), second_sums[1][0].astype(f32)])
    got_far, outer_total, inner_total = together(got_far, outer_total, inner_total)
    kv_sum = grad_kv0.astype(f32) + got_far.astype(f32)
    kv_sum = kv_sum + jnp.where(seq_index % 2 == 0, got_near.astype(f32), 0.0)
    kv_sum = kv_sum.astype(bf16).reshape(2, token_count, model_width)
    grad_qkv = [grad_query.reshape(token_count, model_width), kv_sum[0], kv_sum[1]]
    qkv_grad = row_major(
        jnp.concatenate([weight_grad(normed_attn, part) for part in grad_qkv], axis=1)
    )
    grad_normed_attn = sum(
        product_bt(part, qkv_full[:, index * model_width : (index + 1) * model_width])
        for index, part in enumerate(grad_qkv)
    )
    grad_input_norm, grad_gain_attn = norm_back(tokens_flat, gain_attn, grad_normed_attn)
    grad_input = (grad_hidden + grad_input_norm).reshape(block_input.shape)

    gain_terms = jnp.stack([grad_gain_attn, grad_gain_ffn]).reshape(2, devices, shard)
    gain_terms, qkv_grad = together(gain_terms.transpose(1, 0, 2), qkv_grad)
    gain_terms = lax.all_to_all(gain_terms, every, 0, 0, tiled=True)
    qkv_sum = scatter_rows(qkv_grad)
    gain_sums = jnp.sum(gain_terms, axis=0)
    totals = jnp.concatenate(
        [
            jnp.stack(gain_grads),
            centroid_grad.reshape(1, model_width),
            jnp.pad(jnp.stack([gate_sum, score_sum]), (0, model_width - 2))[None],
        ]
    )
    totals = totals + swap_core(totals)
    totals = totals + swap_chip(totals)
    up_grad = (
        rest_sum[:, model_width : model_width + hidden_width]
        .reshape(shard, BLOCKS, devices, shard)
        .transpose(0, 2, 1, 3)
        .reshape(shard, hidden_width)
    )
    down_grad = (
        rest_sum[:, model_width + hidden_width :]
        .reshape(shard, BLOCKS, model_width)
        .transpose(1, 0, 2)
        .reshape(BLOCKS * shard, model_width)
    )
    token_total = token_count * seq_devices
    return (
        output,
        grad_input,
        gain_sums[0],
        qkv_sum,
        rest_sum[:, :model_width],
        gain_sums[1],
        up_grad,
        down_grad,
        totals[2:3],
        totals[:2][None],
        inner_total[None],
        outer_total[None],
        totals[3, :1] / token_total,
        totals[3, 1:2] / token_total,
    )


def solution(mesh):
    in_specs = (
        P("wide", "seq", None),
        P("wide", None),
        P("wide", "seq"),
        P(("seq", "wide")),
        P(("seq", "wide"), None),
        P(("seq", "wide"), None),
        P(("seq", "wide")),
        P(("seq", "wide"), None),
        P(("seq", "wide"), None),
        P("wide", None),
        P("wide", None, None),
        P("wide", None, None, "seq"),
        P("wide", None, "seq", None),
        P("wide", "seq", None),
    )
    out_specs = (
        P("wide", "seq", None),
        P("wide", "seq", None),
        P(("seq", "wide")),
        P(("seq", "wide"), None),
        P(("seq", "wide"), None),
        P(("seq", "wide")),
        P(("seq", "wide"), None),
        P(("seq", "wide"), None),
        P("wide", None),
        P("wide", None, None),
        P("wide", None, None, "seq"),
        P("wide", None, "seq", None),
        P("wide"),
        P("wide"),
    )
    return jax.shard_map(
        per_device, mesh=mesh, in_specs=in_specs, out_specs=out_specs, check_vma=False
    )
```

```python
import functools
import math

import jax
import jax.numpy as jnp
from jax import lax
from jax.experimental import pallas as pl
from jax.experimental.layout import Layout, with_layout_constraint
from jax.experimental.pallas import tpu as pltpu
from jax.sharding import PartitionSpec as P

HEADS = 16
HEAD_DIM = 64
BLOCKS = 4
LANES = 128

epsilon = 1e-05
highest = lax.Precision.HIGHEST
bf16 = jnp.bfloat16
f32 = jnp.float32


def layer_norm(values, norm_gain):
    centered = values - jnp.mean(values, axis=-1, keepdims=True)
    variance = jnp.mean(centered * centered, axis=-1, keepdims=True)
    return centered * lax.rsqrt(variance + epsilon) * norm_gain


def norm_back(values, norm_gain, grad_normed):
    _, pull_back = jax.vjp(layer_norm, values, norm_gain)
    return pull_back(grad_normed)


def gelu_pair(values):
    cdf = 0.5 * (1.0 + lax.erf(values * math.sqrt(0.5)))
    density = jnp.exp(values * values * -0.5) * (1.0 / math.sqrt(2.0 * math.pi))
    return values * cdf, cdf + values * density


def product(left_side, right_side):
    return jnp.dot(left_side, right_side, preferred_element_type=f32)


def product_bt(left_side, right_side):
    return lax.dot_general(
        left_side, right_side, (((1,), (1,)), ((), ())), preferred_element_type=f32
    )


def product_at(left_side, right_side):
    return lax.dot_general(
        left_side, right_side, (((0,), (0,)), ((), ())), preferred_element_type=f32
    )


def row_major(values):
    return with_layout_constraint(values, Layout(major_to_minor=(0, 1)))


def weight_grad(left_side, right_side):
    return row_major(product_at(left_side, right_side).astype(bf16))


def seq_send(values, pairs):
    return lax.ppermute(values, "seq", pairs)


def swap_core(values):
    return seq_send(values, [(0, 1), (1, 0), (2, 3), (3, 2)])


def swap_chip(values):
    return seq_send(values, [(0, 2), (2, 0), (1, 3), (3, 1)])


def pair_probs(query, keys, bias, score_scale):
    scores = product_bt(keys, query) * score_scale + bias
    exp_scores = jnp.exp(scores - jnp.max(scores, axis=0, keepdims=True))
    return exp_scores * (1.0 / jnp.sum(exp_scores, axis=0, keepdims=True))


def ride_chip(source, target, send_sem, recv_sem):
    seq = lax.axis_index("seq")
    other = (lax.rem(seq + 2, 4), lax.axis_index("wide"))
    step = pl.program_id(0) * pl.num_programs(1) + pl.program_id(1)
    copy = pltpu.make_async_remote_copy(
        src_ref=source,
        dst_ref=target,
        send_sem=send_sem,
        recv_sem=recv_sem,
        device_id=other,
        device_id_type=pl.DeviceIdType.MESH,
    )

    @pl.when(step == 0)
    def _():
        barrier = pltpu.get_barrier_semaphore()
        pl.semaphore_signal(
            barrier, inc=1, device_id=other, device_id_type=pl.DeviceIdType.MESH
        )
        pl.semaphore_wait(barrier, 1)
        copy.start()

    @pl.when(step == pl.num_programs(0) * pl.num_programs(1) - 1)
    def _():
        copy.wait()


def attend_kernel(
    score_scale,
    q_ref,
    k0,
    v0,
    k1,
    v1,
    k2,
    v2,
    bias_ref,
    ride_ref,
    out_ref,
    rode_ref,
    send_sem,
    recv_sem,
):
    ride_chip(ride_ref.at[0], rode_ref, send_sem, recv_sem)
    bias = bias_ref[0]
    parts = []
    for head in range(2):
        cols = slice(head * HEAD_DIM, (head + 1) * HEAD_DIM)
        keys = jnp.concatenate([k2[0][:, cols], k1[0][:, cols], k0[0][:, cols]], axis=0)
        vals = jnp.concatenate([v2[0][:, cols], v1[0][:, cols], v0[0][:, cols]], axis=0)
        probs_low = pair_probs(q_ref[0][:, cols], keys, bias, score_scale).astype(bf16)
        parts.append(product_at(vals, probs_low))
    out_ref[0] = jnp.concatenate(parts, axis=0).T.astype(bf16)


def attend_back_kernel(
    score_scale,
    q_ref,
    k0,
    v0,
    k1,
    v1,
    k2,
    v2,
    bias_ref,
    grad_ref,
    dq_ref,
    d0,
    d1,
    d2,
):
    bias = bias_ref[0]
    dq_parts, dk_parts, dv_parts = [], [], []
    for head in range(2):
        cols = slice(head * HEAD_DIM, (head + 1) * HEAD_DIM)
        query = q_ref[0][:, cols]
        grad_att = grad_ref[0][:, cols]
        keys = jnp.concatenate([k2[0][:, cols], k1[0][:, cols], k0[0][:, cols]], axis=0)
        vals = jnp.concatenate([v2[0][:, cols], v1[0][:, cols], v0[0][:, cols]], axis=0)
        probs = pair_probs(query, keys, bias, score_scale)
        grad_probs = product_bt(vals, grad_att)
        dv_parts.append(product(probs.astype(bf16), grad_att))
        inner_sum = jnp.sum(probs * grad_probs, axis=0, keepdims=True)
        grad_scores = (probs * (grad_probs - inner_sum)).astype(bf16)
        dk_parts.append(product(grad_scores, query) * score_scale)
        dq_parts.append(product_at(keys, grad_scores) * score_scale)
    dq_ref[0] = jnp.concatenate(dq_parts, axis=0).T.astype(bf16)
    d_keys = jnp.concatenate(dk_parts, axis=1).astype(bf16)
    d_vals = jnp.concatenate(dv_parts, axis=1).astype(bf16)
    size = d_keys.shape[0] // 3
    for place, ref in enumerate((d2, d1, d0)):
        ref[0, 0] = d_keys[place * size : (place + 1) * size]
        ref[1, 0] = d_vals[place * size : (place + 1) * size]


def attention_specs(local_len, model_width, key_len):
    width = 2 * HEAD_DIM
    groups = model_width // width
    query = pl.BlockSpec((1, local_len, width), lambda row, head: (row, 0, head))
    values = pl.BlockSpec((1, local_len, width), lambda row, head: (row, 0, head + groups))
    bias = pl.BlockSpec((1, key_len, local_len), lambda row, head: (row, 0, 0))
    return groups, query, [query, query, values, query, values, query, values, bias]


def attend(query, kv_blocks, bias, ride):
    rows, local_len, model_width = query.shape
    groups, spec, in_specs = attention_specs(local_len, model_width, bias.shape[1])
    operands = [block for block in kv_blocks for _ in range(2)]
    flops = 4 * rows * model_width * local_len * bias.shape[1]
    return pl.pallas_call(
        functools.partial(attend_kernel, 1.0 / math.sqrt(HEAD_DIM)),
        grid=(rows, groups),
        in_specs=in_specs + [pl.BlockSpec(memory_space=pl.ANY)],
        out_specs=[spec, pl.BlockSpec(memory_space=pl.ANY)],
        out_shape=[
            jax.ShapeDtypeStruct(query.shape, bf16),
            jax.ShapeDtypeStruct(ride.shape[1:], ride.dtype),
        ],
        scratch_shapes=[pltpu.SemaphoreType.DMA, pltpu.SemaphoreType.DMA],
        compiler_params=pltpu.CompilerParams(collective_id=2, has_side_effects=True),
        cost_estimate=pl.CostEstimate(
            flops=flops * 6, bytes_accessed=8 * query.size * 2, transcendentals=0
        ),
        name="attend",
    )(query, *operands, bias, ride)


def attend_back(query, kv_blocks, bias, grad_attended):
    rows, local_len, model_width = query.shape
    groups, spec, in_specs = attention_specs(local_len, model_width, bias.shape[1])
    operands = [block for block in kv_blocks for _ in range(2)]
    pair_spec = pl.BlockSpec((2, 1, local_len, 2 * HEAD_DIM), lambda row, head: (0, row, 0, head))
    pair_shape = jax.ShapeDtypeStruct((2, rows, local_len, model_width), bf16)
    flops = 10 * rows * model_width * local_len * bias.shape[1]
    return pl.pallas_call(
        functools.partial(attend_back_kernel, 1.0 / math.sqrt(HEAD_DIM)),
        grid=(rows, groups),
        in_specs=in_specs + [spec],
        out_specs=[spec, pair_spec, pair_spec, pair_spec],
        out_shape=[jax.ShapeDtypeStruct(query.shape, bf16)] + [pair_shape] * 3,
        cost_estimate=pl.CostEstimate(
            flops=flops * 6, bytes_accessed=16 * query.size * 2, transcendentals=0
        ),
        name="attend_back",
    )(query, *operands, bias, grad_attended)


def ffn_forward(normed, inner_parts, outer_parts, residual):
    kept = []
    total = residual
    for inner, outer in zip(inner_parts, outer_parts):
        act, slope = gelu_pair(product(normed, inner))
        act = act.astype(bf16)
        kept.append((act, slope.astype(bf16)))
        total = total + product(act, outer)
    return total, kept


def ffn_backward(kept, inner_parts, outer_parts, grad_branch):
    grad_pres = []
    grad_normed = None
    for (act, slope), inner, outer in zip(kept, inner_parts, outer_parts):
        grad_pre = (product_bt(grad_branch, outer) * slope.astype(f32)).astype(bf16)
        grad_pres.append(grad_pre)
        piece = product_bt(grad_pre, inner)
        grad_normed = piece if grad_normed is None else grad_normed + piece
    return grad_pres, grad_normed


def slice_owner(place):
    seq = lax.axis_index("seq")
    return seq + (1 - 2 * (seq % 2)) * (place % 2) + (2 - 4 * (seq // 2)) * (place // 2)


def slices_in_order(terms, operands):
    for place, (left, right) in enumerate(operands):
        values = weight_grad(left, right)
        terms = lax.dynamic_update_index_in_dim(terms, values, slice_owner(place), 0)
    return terms


class SliceSum:
    def __init__(self, operands):
        self.operands = operands

    def term(self, place):
        return weight_grad(*self.operands[place])

    def send_both(self, values):
        self.got_both = swap_core(values)

    def send_core(self, values):
        self.got_core = swap_core(values)

    def chip_sum(self):
        values = product_at(*self.operands[2]) + self.got_both.astype(f32)
        return row_major(values.astype(bf16))

    def send_chip(self, values):
        self.got_chip = swap_chip(values)

    def total(self):
        return self.own.astype(f32) + self.got_core.astype(f32) + self.got_chip.astype(f32)


def cube_bits():
    bits = []
    for axis in ("seq", "wide"):
        count = lax.axis_size(axis).bit_length() - 1
        bits += [(axis, bit) for bit in reversed(range(count))]
    return bits


def cube_orders(bits):
    core = bits.index(("seq", 0))
    chip = bits.index(("seq", 1))
    wide = [place for place, (axis, _) in enumerate(bits) if axis == "wide"]
    if len(wide) == 3:
        far, near, across = wide
        return ((chip, far, near, across, core), (chip, across, far, near, core))
    return ((chip, *wide, core), (chip, *wide[2:], *wide[:2], core))


def cube_place(bits):
    index = {axis: lax.axis_index(axis) for axis in ("seq", "wide")}
    mine = [lax.rem(index[axis] // (1 << bit), 2) for axis, bit in bits]

    def partner(place):
        axis, bit = bits[place]
        other = dict(index)
        other[axis] = index[axis] + (1 - 2 * mine[place]) * (1 << bit)
        return (other["seq"], other["wide"])

    return mine, partner


def cube_barrier(bits, partner):
    barrier = pltpu.get_barrier_semaphore()
    for place in range(len(bits)):
        pl.semaphore_signal(
            barrier, inc=1, device_id=partner(place), device_id_type=pl.DeviceIdType.MESH
        )
    pl.semaphore_wait(barrier, len(bits))


def gather_kernel(
    bits,
    orders,
    own_ref,
    inner_ref,
    outer_ref,
    out_ref,
    inner_core_ref,
    outer_core_ref,
    inner_chip_ref,
    send_sem,
    recv_sem,
    copy_sem,
    ride_send,
    ride_recv,
):
    mine, partner = cube_place(bits)
    own_copy = pltpu.make_async_copy(own_ref, out_ref.at[tuple(mine)], copy_sem)
    own_copy.start()
    cube_barrier(bits, partner)
    own_copy.wait()
    width = own_ref.shape[1] // len(orders)
    core = partner(bits.index(("seq", 0)))
    chip = partner(bits.index(("seq", 1)))
    rides = [
        (inner_ref.at[0, 0], inner_chip_ref, chip),
        (inner_ref.at[0], inner_core_ref, core),
        (outer_ref.at[0], outer_core_ref, core),
    ]
    rides = [
        pltpu.make_async_remote_copy(
            src_ref=source,
            dst_ref=target,
            send_sem=ride_send.at[place],
            recv_sem=ride_recv.at[place],
            device_id=device,
            device_id_type=pl.DeviceIdType.MESH,
        )
        for place, (source, target, device) in enumerate(rides)
    ]
    copies = []
    held = [[False] * len(bits) for _ in orders]
    for stage in range(len(bits)):
        for color, order in enumerate(orders):
            if stage:
                copies[(stage - 1) * len(orders) + color].wait_recv()
                held[color][order[stage - 1]] = True
            place = tuple(
                slice(None) if whole else mine[axis] for axis, whole in enumerate(held[color])
            )
            ref = out_ref.at[place + (slice(None), pl.ds(color * width, width))]
            copy = pltpu.make_async_remote_copy(
                src_ref=ref,
                dst_ref=ref,
                send_sem=send_sem.at[color, stage],
                recv_sem=recv_sem.at[color, stage],
                device_id=partner(order[stage]),
                device_id_type=pl.DeviceIdType.MESH,
            )
            copy.start()
            copies.append(copy)
        if stage == 0:
            for ride in rides:
                ride.start()
    for copy in copies:
        copy.wait_send()
    for copy in copies[-len(orders) :]:
        copy.wait_recv()
    for ride in rides:
        ride.wait()


def gather_rows(own, expert_in, expert_out):
    bits = cube_bits()
    orders = cube_orders(bits)
    rows, width = own.shape
    anywhere = pl.BlockSpec(memory_space=pl.ANY)
    out, inner_core, outer_core, inner_chip = pl.pallas_call(
        functools.partial(gather_kernel, bits, orders),
        in_specs=[pl.BlockSpec(memory_space=pltpu.VMEM), anywhere, anywhere],
        out_specs=[anywhere] * 4,
        out_shape=[
            jax.ShapeDtypeStruct((2,) * len(bits) + (rows, width), own.dtype),
            jax.ShapeDtypeStruct(expert_in.shape[1:], expert_in.dtype),
            jax.ShapeDtypeStruct(expert_out.shape[1:], expert_out.dtype),
            jax.ShapeDtypeStruct(expert_in.shape[2:], expert_in.dtype),
        ],
        scratch_shapes=[
            pltpu.SemaphoreType.DMA((len(orders), len(bits))),
            pltpu.SemaphoreType.DMA((len(orders), len(bits))),
            pltpu.SemaphoreType.DMA,
            pltpu.SemaphoreType.DMA((3,)),
            pltpu.SemaphoreType.DMA((3,)),
        ],
        compiler_params=pltpu.CompilerParams(collective_id=0, has_side_effects=True),
        cost_estimate=pl.CostEstimate(flops=0, bytes_accessed=25 * own.size << 5, transcendentals=0),
        name="gather_rows",
    )(own, expert_in, expert_out)
    return out.reshape(rows << len(bits), width), inner_core, outer_core, inner_chip


def scatter_kernel(bits, orders, terms_ref, out_ref, *scratch):
    stages = len(bits)
    colors = len(orders)
    got = scratch[: colors * stages]
    sums = scratch[colors * stages : colors * (2 * stages - 1)]
    send_sem, recv_sem = scratch[colors * (2 * stages - 1) :]
    mine, partner = cube_place(bits)
    cube_barrier(bits, partner)
    width = terms_ref.shape[-1] // colors
    copies = []

    def half(color, stage, keep):
        done = orders[color][:stage]
        place = []
        for axis in range(stages):
            if axis in done:
                continue
            if axis == orders[color][stage]:
                place.append(mine[axis] if keep else 1 - mine[axis])
            else:
                place.append(slice(None))
        if stage == 0:
            return terms_ref.at[tuple(place) + (slice(None), pl.ds(color * width, width))]
        return sums[color * (stages - 1) + stage - 1].at[tuple(place)]

    for stage in range(stages + 1):
        for color in range(colors):
            if stage:
                copies[(stage - 1) * colors + color].wait_recv()
                kept = half(color, stage - 1, True)[...].astype(f32)
                total = kept + got[color * stages + stage - 1][...].astype(f32)
                if stage == stages:
                    out_ref[:, pl.ds(color * width, width)] = total
                    continue
                sums[color * (stages - 1) + stage - 1][...] = total.astype(bf16)
            copy = pltpu.make_async_remote_copy(
                src_ref=half(color, stage, False),
                dst_ref=got[color * stages + stage],
                send_sem=send_sem.at[color, stage],
                recv_sem=recv_sem.at[color, stage],
                device_id=partner(orders[color][stage]),
                device_id_type=pl.DeviceIdType.MESH,
            )
            copy.start()
            copies.append(copy)
    for copy in copies:
        copy.wait_send()


def scatter_rows(terms):
    bits = cube_bits()
    orders = [order[::-1] for order in cube_orders(bits)]
    colors = len(orders)
    stages = len(bits)
    rows = terms.shape[0] >> stages
    width = terms.shape[1]
    got = [
        pltpu.VMEM((2,) * (stages - 1 - stage) + (rows, width // colors), bf16)
        for _ in range(colors)
        for stage in range(stages)
    ]
    sums = [
        pltpu.VMEM((2,) * (stages - 1 - stage) + (rows, width // colors), bf16)
        for _ in range(colors)
        for stage in range(stages - 1)
    ]
    return pl.pallas_call(
        functools.partial(scatter_kernel, bits, orders),
        in_specs=[pl.BlockSpec(memory_space=pltpu.VMEM)],
        out_specs=pl.BlockSpec(memory_space=pltpu.VMEM),
        out_shape=jax.ShapeDtypeStruct((rows, width), f32),
        scratch_shapes=got
        + sums
        + [
            pltpu.SemaphoreType.DMA((colors, stages)),
            pltpu.SemaphoreType.DMA((colors, stages)),
        ],
        compiler_params=pltpu.CompilerParams(collective_id=1, has_side_effects=True),
        cost_estimate=pl.CostEstimate(flops=0, bytes_accessed=50 * terms.size, transcendentals=0),
        name="scatter_rows",
    )(terms.reshape((2,) * stages + (rows, width)))


def together(*values):
    return lax.optimization_barrier(values)


def per_device(
    block_input,
    segment_ids,
    assignment,
    norm_attn,
    weight_qkv,
    weight_proj,
    norm_ffn,
    weight_up,
    weight_down,
    centroids,
    expert_norms,
    expert_in,
    expert_out,
    grad_out,
):
    row_count, local_len, model_width = block_input.shape
    token_count = row_count * local_len
    seq_devices = lax.axis_size("seq")
    seq_index = lax.axis_index("seq")
    experts = lax.axis_size("wide")
    devices = seq_devices * experts
    every = ("seq", "wide")
    shard = weight_up.shape[0]
    hidden_width = weight_up.shape[1]

    gains_own = jnp.stack([norm_attn, norm_ffn], axis=1)
    first_own = jnp.concatenate(
        [weight_qkv, jnp.pad(gains_own, ((0, 0), (0, 2 * LANES - gains_own.shape[1])))], axis=1
    )
    qkv_full, inner_core, outer_core, inner_first = gather_rows(first_own, expert_in, expert_out)
    gains_all = qkv_full[:, 3 * model_width : 3 * model_width + 2].astype(f32).T
    gain_attn = gains_all[0]
    gain_ffn = gains_all[1]
    up_own = (
        weight_up.reshape(shard, devices, BLOCKS, shard)
        .transpose(0, 2, 1, 3)
        .reshape(shard, hidden_width)
    )
    down_own = weight_down.reshape(BLOCKS, shard, model_width).transpose(1, 0, 2)
    rest_own = jnp.concatenate(
        [weight_proj, up_own, down_own.reshape(shard, BLOCKS * model_width)], axis=1
    )
    rest_own, _ = together(rest_own, qkv_full)
    rest_full = lax.all_gather(rest_own, every, axis=0, tiled=True)

    def rest_block(index):
        return rest_full[:, index * model_width : (index + 1) * model_width]

    proj_full = rest_block(0)
    up_parts = [rest_block(1 + index) for index in range(BLOCKS)]
    down_parts = [rest_block(1 + BLOCKS + index) for index in range(BLOCKS)]

    inner_own = expert_in[0]
    outer_own = expert_out[0]
    inner_chip = [inner_first, None]
    outer_chip = [None, None]

    capacity = token_count // experts
    chosen = assignment.reshape(token_count)
    one_hot = (chosen[:, None] == jnp.arange(experts, dtype=jnp.int32)[None, :]).astype(jnp.int32)
    rank_within = jnp.sum((jnp.cumsum(one_hot, axis=0) - 1) * one_hot, axis=1)
    slot_index = chosen * capacity + rank_within
    source_of = (
        jnp.zeros((token_count,), jnp.int32)
        .at[slot_index]
        .set(jnp.arange(token_count, dtype=jnp.int32))
    )

    tokens_flat = block_input.reshape(token_count, model_width).astype(f32)
    normed_attn = layer_norm(tokens_flat, gain_attn).astype(bf16)
    kv_own = product(normed_attn, qkv_full[:, model_width : 3 * model_width]).astype(bf16)
    kv_own = kv_own.reshape(row_count, local_len, 2 * model_width)
    query = product(normed_attn, qkv_full[:, :model_width]).astype(bf16)
    query = query.reshape(row_count, local_len, model_width)

    kv_far = seq_send(kv_own, [(0, 2), (1, 3)])
    kv_near = seq_send(
        jnp.where(seq_index == 3, kv_far, kv_own), [(0, 1), (2, 3), (3, 2)]
    )
    kv_blocks = (kv_own, kv_near, kv_far)
    before = 2 * local_len
    offset = seq_index * local_len
    padded_seg = jnp.pad(segment_ids, ((0, 0), (before, 0)), constant_values=-1)
    key_seg = lax.dynamic_slice_in_dim(padded_seg, offset, before + local_len, 1)
    query_seg = key_seg[:, before:]
    key_pos = jnp.arange(before + local_len)
    query_pos = before + jnp.arange(local_len)
    allowed = (key_seg[:, :, None] == query_seg[:, None, :]) & (
        key_pos[None, :, None] <= query_pos[None, None, :]
    )
    bias = jnp.where(allowed, 0.0, -1e30).astype(f32)

    attended_rows, outer_chip[0] = attend(query, kv_blocks, bias, outer_own)
    late = together(inner_own[1], outer_own[1], attended_rows)
    inner_chip[1], outer_chip[1] = [swap_chip(part) for part in late[:2]]
    attended = attended_rows.reshape(token_count, model_width)
    hidden = tokens_flat + product(attended, proj_full)
    normed_ffn = layer_norm(hidden, gain_ffn).astype(bf16)
    dense_out, dense_kept = ffn_forward(normed_ffn, up_parts, down_parts, hidden)
    routed = dense_out.astype(bf16)

    received = lax.all_to_all(routed[source_of], "wide", split_axis=0, concat_axis=0, tiled=True)
    fresh = jnp.zeros((seq_devices,) + inner_own.shape[1:], bf16)
    received, inner_chip[1], fresh = together(received, inner_chip[1], fresh)
    received_f = received.astype(f32)
    inner_both = [swap_core(together(inner_chip[0], attended)[0]), None]
    outer_both = [swap_core(together(outer_chip[0], attended)[0]), None]
    centroid_row = centroids[0]
    centroid_f = centroid_row.astype(f32)
    logit_row = jnp.dot(received, centroid_row, preferred_element_type=f32)
    gate_value = jax.nn.sigmoid(logit_row)
    gains_f = expert_norms[0].astype(f32)
    state_now = received_f
    kept_layers = []
    slices = []
    for sublayer in range(2):
        if sublayer:
            inner_both[1] = swap_core(together(inner_chip[1], state_now)[0])
            outer_both[1] = swap_core(together(outer_chip[1], state_now)[0])
        inner_parts = [part[sublayer] for part in (inner_own, inner_core, inner_chip, inner_both)]
        outer_parts = [part[sublayer] for part in (outer_own, outer_core, outer_chip, outer_both)]
        normed = layer_norm(state_now, gains_f[sublayer]).astype(bf16)
        state_next, kept = ffn_forward(normed, inner_parts, outer_parts, state_now)
        kept_layers.append((state_now, normed, kept))
        slices.append((inner_parts, outer_parts))
        state_now = state_next
    returned = (gate_value[:, None] * state_now).astype(bf16)
    back_rows = lax.all_to_all(returned, "wide", split_axis=0, concat_axis=0, tiled=True)
    output = (
        (dense_out + back_rows[slot_index].astype(f32)).astype(bf16).reshape(block_input.shape)
    )
    gate_sum = jnp.sum(gate_value)
    score_sum = jnp.sum(logit_row * logit_row)
    grad_flat = grad_out.reshape(token_count, model_width)
    grad_back = lax.all_to_all(
        grad_flat[source_of], "wide", split_axis=0, concat_axis=0, tiled=True
    )
    grad_ret = grad_back.astype(f32)
    grad_gate = jnp.sum(grad_ret * state_now, axis=-1)
    grad_state = grad_ret * gate_value[:, None]
    gain_grads = [None, None]
    weight_terms = [None, None]
    sums = [None, None]
    for sublayer in (1, 0):
        state_in, normed_in, kept = kept_layers[sublayer]
        inner_parts, outer_parts = slices[sublayer]
        grad_branch = grad_state.astype(bf16)
        grad_pres, grad_normed = ffn_backward(kept, inner_parts, outer_parts, grad_branch)
        weight_terms[sublayer] = (
            [(act, grad_branch) for act, _ in kept],
            [(normed_in, grad_pre) for grad_pre in grad_pres],
        )
        grad_resid, gain_grad = norm_back(state_in, gains_f[sublayer], grad_normed)
        grad_state = grad_state + grad_resid
        gain_grads[sublayer] = gain_grad
        sums[sublayer] = [SliceSum(operands) for operands in weight_terms[sublayer]]
        if sublayer:
            outer1 = sums[1][0]
            grad_state, both, fresh = together(
                grad_state, outer1.term(3), slices_in_order(fresh, weight_terms[1][1])
            )
            outer1.send_both(both)
            inner_second = lax.psum_scatter(fresh, "seq", scatter_dimension=0, tiled=True)
    grad_logit = grad_gate * gate_value * (1.0 - gate_value)
    grad_routed = (grad_state + grad_logit[:, None] * centroid_f[None, :]).astype(bf16)
    centroid_grad = jnp.dot(grad_logit, received_f, precision=highest)
    grad_routed, held = together(grad_routed, outer1.chip_sum())
    outer1.send_chip(held)
    returned_grad = lax.all_to_all(grad_routed, "wide", split_axis=0, concat_axis=0, tiled=True)
    outer0, inner0 = sums[0]
    returned_grad, *held = together(
        returned_grad,
        outer0.term(3),
        inner0.term(3),
        outer1.term(1),
        outer0.term(1),
        inner0.term(1),
        outer1.term(0),
    )
    outer0.send_both(held[0])
    inner0.send_both(held[1])
    outer1.send_core(held[2])
    outer0.send_core(held[3])
    inner0.send_core(held[4])
    outer1.own = held[5]
    grad_dense = grad_flat.astype(f32) + returned_grad[slot_index].astype(f32)

    grad_down_in = grad_dense.astype(bf16)
    grad_pres, grad_normed_ffn = ffn_backward(dense_kept, up_parts, down_parts, grad_down_in)
    grad_hidden_norm, grad_gain_ffn = norm_back(hidden, gain_ffn, grad_normed_ffn)
    grad_hidden = grad_dense + grad_hidden_norm
    grad_hidden, outer1.got_chip = together(grad_hidden, outer1.got_chip)
    grad_proj = grad_hidden.astype(bf16)
    rest_grad = jnp.concatenate(
        [weight_grad(attended, grad_proj)]
        + [weight_grad(normed_ffn, grad_pre) for grad_pre in grad_pres]
        + [weight_grad(act, grad_down_in) for act, _ in dense_kept],
        axis=1,
    )
    rest_grad = row_major(rest_grad)
    grad_attended = product_bt(grad_proj, proj_full).astype(bf16)
    grad_attended, rest_grad = together(grad_attended, rest_grad)
    grad_attended, held = together(grad_attended, outer0.chip_sum())
    outer0.send_chip(held)
    rest_sum = lax.psum_scatter(rest_grad, every, scatter_dimension=0, tiled=True).astype(f32)
    grad_query, grad_kv0, grad_kv1, grad_kv2 = attend_back(
        query, kv_blocks, bias, grad_attended.reshape(query.shape)
    )
    grad_kv1, outer0.got_chip = together(grad_kv1, outer0.got_chip)
    got_near = seq_send(grad_kv1, [(1, 0), (3, 2), (2, 3)])
    far_sum = jnp.where(
        seq_index == 3, (grad_kv2.astype(f32) + got_near.astype(f32)).astype(bf16), grad_kv2
    )
    got_far = seq_send(far_sum, [(2, 0), (3, 1)])
    outer0.own = outer0.term(0)
    got_far, inner0.own, inner_send, outer_total = together(
        got_far,
        inner0.term(0),
        inner0.chip_sum(),
        jnp.stack([outer0.total(), outer1.total()]),
    )
    inner0.send_chip(inner_send)
    kv_sum = grad_kv0.astype(f32) + got_far.astype(f32)
    kv_sum = kv_sum + jnp.where(seq_index % 2 == 0, got_near.astype(f32), 0.0)
    kv_sum = kv_sum.astype(bf16).reshape(2, token_count, model_width)
    grad_qkv = [grad_query.reshape(token_count, model_width), kv_sum[0], kv_sum[1]]
    qkv_grad = row_major(
        jnp.concatenate([weight_grad(normed_attn, part) for part in grad_qkv], axis=1)
    )
    grad_normed_attn = sum(
        product_bt(part, qkv_full[:, index * model_width : (index + 1) * model_width])
        for index, part in enumerate(grad_qkv)
    )
    grad_input_norm, grad_gain_attn = norm_back(tokens_flat, gain_attn, grad_normed_attn)
    grad_input = (grad_hidden + grad_input_norm).reshape(block_input.shape)

    gain_terms = jnp.stack([grad_gain_attn, grad_gain_ffn]).reshape(2, devices, shard)
    gain_terms, qkv_grad = together(gain_terms.transpose(1, 0, 2), qkv_grad)
    gain_terms = lax.all_to_all(gain_terms, every, 0, 0, tiled=True)
    qkv_sum = scatter_rows(qkv_grad)
    gain_sums = jnp.sum(gain_terms, axis=0)
    totals = jnp.concatenate(
        [
            jnp.stack(gain_grads),
            centroid_grad.reshape(1, model_width),
            jnp.pad(jnp.stack([gate_sum, score_sum]), (0, model_width - 2))[None],
        ]
    )
    totals = totals + swap_core(totals)
    totals = totals + swap_chip(totals)
    up_grad = (
        rest_sum[:, model_width : model_width + hidden_width]
        .reshape(shard, BLOCKS, devices, shard)
        .transpose(0, 2, 1, 3)
        .reshape(shard, hidden_width)
    )
    down_grad = (
        rest_sum[:, model_width + hidden_width :]
        .reshape(shard, BLOCKS, model_width)
        .transpose(1, 0, 2)
        .reshape(BLOCKS * shard, model_width)
    )
    token_total = token_count * seq_devices
    return (
        output,
        grad_input,
        gain_sums[0],
        qkv_sum,
        rest_sum[:, :model_width],
        gain_sums[1],
        up_grad,
        down_grad,
        totals[2:3],
        totals[:2][None],
        jnp.stack([inner0.total(), inner_second[0].astype(f32)])[None],
        outer_total[None],
        totals[3, :1] / token_total,
        totals[3, 1:2] / token_total,
    )


def solution(mesh):
    in_specs = (
        P("wide", "seq", None),
        P("wide", None),
        P("wide", "seq"),
        P(("seq", "wide")),
        P(("seq", "wide"), None),
        P(("seq", "wide"), None),
        P(("seq", "wide")),
        P(("seq", "wide"), None),
        P(("seq", "wide"), None),
        P("wide", None),
        P("wide", None, None),
        P("wide", None, None, "seq"),
        P("wide", None, "seq", None),
        P("wide", "seq", None),
    )
    out_specs = (
        P("wide", "seq", None),
        P("wide", "seq", None),
        P(("seq", "wide")),
        P(("seq", "wide"), None),
        P(("seq", "wide"), None),
        P(("seq", "wide")),
        P(("seq", "wide"), None),
        P(("seq", "wide"), None),
        P("wide", None),
        P("wide", None, None),
        P("wide", None, None, "seq"),
        P("wide", None, "seq", None),
        P("wide"),
        P("wide"),
    )
    return jax.shard_map(
        per_device, mesh=mesh, in_specs=in_specs, out_specs=out_specs, check_vma=False
    )
```

```python
import functools
import math

import jax
import jax.numpy as jnp
from jax import lax
from jax.experimental import pallas as pl
from jax.experimental.layout import Layout, with_layout_constraint
from jax.experimental.pallas import tpu as pltpu
from jax.sharding import PartitionSpec as P

HEADS = 16
HEAD_DIM = 64
BLOCKS = 4
LANES = 128

epsilon = 1e-05
highest = lax.Precision.HIGHEST
bf16 = jnp.bfloat16
f32 = jnp.float32


def layer_norm(values, norm_gain):
    centered = values - jnp.mean(values, axis=-1, keepdims=True)
    variance = jnp.mean(centered * centered, axis=-1, keepdims=True)
    return centered * lax.rsqrt(variance + epsilon) * norm_gain


def norm_back(values, norm_gain, grad_normed):
    _, pull_back = jax.vjp(layer_norm, values, norm_gain)
    return pull_back(grad_normed)


def gelu_pair(values):
    cdf = 0.5 * (1.0 + lax.erf(values * math.sqrt(0.5)))
    density = jnp.exp(values * values * -0.5) * (1.0 / math.sqrt(2.0 * math.pi))
    return values * cdf, cdf + values * density


def product(left_side, right_side):
    return jnp.dot(left_side, right_side, preferred_element_type=f32)


def product_bt(left_side, right_side):
    return lax.dot_general(
        left_side, right_side, (((1,), (1,)), ((), ())), preferred_element_type=f32
    )


def product_at(left_side, right_side):
    return lax.dot_general(
        left_side, right_side, (((0,), (0,)), ((), ())), preferred_element_type=f32
    )


def row_major(values):
    return with_layout_constraint(values, Layout(major_to_minor=(0, 1)))


def weight_grad(left_side, right_side):
    return row_major(product_at(left_side, right_side).astype(bf16))


def seq_send(values, pairs):
    return lax.ppermute(values, "seq", pairs)


def swap_core(values):
    return seq_send(values, [(0, 1), (1, 0), (2, 3), (3, 2)])


def swap_chip(values):
    return seq_send(values, [(0, 2), (2, 0), (1, 3), (3, 1)])


def pair_probs(query, keys, bias, score_scale):
    scores = product_bt(keys, query) * score_scale + bias
    exp_scores = jnp.exp(scores - jnp.max(scores, axis=0, keepdims=True))
    return exp_scores * (1.0 / jnp.sum(exp_scores, axis=0, keepdims=True))


def ride_chip(source, target, send_sem, recv_sem):
    seq = lax.axis_index("seq")
    other = (lax.rem(seq + 2, 4), lax.axis_index("wide"))
    step = pl.program_id(0) * pl.num_programs(1) + pl.program_id(1)
    copy = pltpu.make_async_remote_copy(
        src_ref=source,
        dst_ref=target,
        send_sem=send_sem,
        recv_sem=recv_sem,
        device_id=other,
        device_id_type=pl.DeviceIdType.MESH,
    )

    @pl.when(step == 0)
    def _():
        barrier = pltpu.get_barrier_semaphore()
        pl.semaphore_signal(
            barrier, inc=1, device_id=other, device_id_type=pl.DeviceIdType.MESH
        )
        pl.semaphore_wait(barrier, 1)
        copy.start()

    @pl.when(step == pl.num_programs(0) * pl.num_programs(1) - 1)
    def _():
        copy.wait()


def attend_kernel(
    score_scale,
    q_ref,
    k0,
    v0,
    k1,
    v1,
    k2,
    v2,
    bias_ref,
    ride_ref,
    out_ref,
    rode_ref,
    send_sem,
    recv_sem,
):
    ride_chip(ride_ref.at[0], rode_ref, send_sem, recv_sem)
    bias = bias_ref[0]
    parts = []
    for head in range(2):
        cols = slice(head * HEAD_DIM, (head + 1) * HEAD_DIM)
        keys = jnp.concatenate([k2[0][:, cols], k1[0][:, cols], k0[0][:, cols]], axis=0)
        vals = jnp.concatenate([v2[0][:, cols], v1[0][:, cols], v0[0][:, cols]], axis=0)
        probs_low = pair_probs(q_ref[0][:, cols], keys, bias, score_scale).astype(bf16)
        parts.append(product_at(vals, probs_low))
    out_ref[0] = jnp.concatenate(parts, axis=0).T.astype(bf16)


def attend_back_kernel(
    score_scale,
    q_ref,
    k0,
    v0,
    k1,
    v1,
    k2,
    v2,
    bias_ref,
    grad_ref,
    dq_ref,
    d0,
    d1,
    d2,
):
    bias = bias_ref[0]
    dq_parts, dk_parts, dv_parts = [], [], []
    for head in range(2):
        cols = slice(head * HEAD_DIM, (head + 1) * HEAD_DIM)
        query = q_ref[0][:, cols]
        grad_att = grad_ref[0][:, cols]
        keys = jnp.concatenate([k2[0][:, cols], k1[0][:, cols], k0[0][:, cols]], axis=0)
        vals = jnp.concatenate([v2[0][:, cols], v1[0][:, cols], v0[0][:, cols]], axis=0)
        probs = pair_probs(query, keys, bias, score_scale)
        grad_probs = product_bt(vals, grad_att)
        dv_parts.append(product(probs.astype(bf16), grad_att))
        inner_sum = jnp.sum(probs * grad_probs, axis=0, keepdims=True)
        grad_scores = (probs * (grad_probs - inner_sum)).astype(bf16)
        dk_parts.append(product(grad_scores, query) * score_scale)
        dq_parts.append(product_at(keys, grad_scores) * score_scale)
    dq_ref[0] = jnp.concatenate(dq_parts, axis=0).T.astype(bf16)
    d_keys = jnp.concatenate(dk_parts, axis=1).astype(bf16)
    d_vals = jnp.concatenate(dv_parts, axis=1).astype(bf16)
    size = d_keys.shape[0] // 3
    for place, ref in enumerate((d2, d1, d0)):
        ref[0, 0] = d_keys[place * size : (place + 1) * size]
        ref[1, 0] = d_vals[place * size : (place + 1) * size]


def attention_specs(local_len, model_width, key_len):
    width = 2 * HEAD_DIM
    groups = model_width // width
    query = pl.BlockSpec((1, local_len, width), lambda row, head: (row, 0, head))
    values = pl.BlockSpec((1, local_len, width), lambda row, head: (row, 0, head + groups))
    bias = pl.BlockSpec((1, key_len, local_len), lambda row, head: (row, 0, 0))
    return groups, query, [query, query, values, query, values, query, values, bias]


def attend(query, kv_blocks, bias, ride):
    rows, local_len, model_width = query.shape
    groups, spec, in_specs = attention_specs(local_len, model_width, bias.shape[1])
    operands = [block for block in kv_blocks for _ in range(2)]
    flops = 4 * rows * model_width * local_len * bias.shape[1]
    return pl.pallas_call(
        functools.partial(attend_kernel, 1.0 / math.sqrt(HEAD_DIM)),
        grid=(rows, groups),
        in_specs=in_specs + [pl.BlockSpec(memory_space=pl.ANY)],
        out_specs=[spec, pl.BlockSpec(memory_space=pl.ANY)],
        out_shape=[
            jax.ShapeDtypeStruct(query.shape, bf16),
            jax.ShapeDtypeStruct(ride.shape[1:], ride.dtype),
        ],
        scratch_shapes=[pltpu.SemaphoreType.DMA, pltpu.SemaphoreType.DMA],
        compiler_params=pltpu.CompilerParams(collective_id=2, has_side_effects=True),
        cost_estimate=pl.CostEstimate(
            flops=flops * 6, bytes_accessed=8 * query.size * 2, transcendentals=0
        ),
        name="attend",
    )(query, *operands, bias, ride)


def attend_back(query, kv_blocks, bias, grad_attended):
    rows, local_len, model_width = query.shape
    groups, spec, in_specs = attention_specs(local_len, model_width, bias.shape[1])
    operands = [block for block in kv_blocks for _ in range(2)]
    pair_spec = pl.BlockSpec((2, 1, local_len, 2 * HEAD_DIM), lambda row, head: (0, row, 0, head))
    pair_shape = jax.ShapeDtypeStruct((2, rows, local_len, model_width), bf16)
    flops = 10 * rows * model_width * local_len * bias.shape[1]
    return pl.pallas_call(
        functools.partial(attend_back_kernel, 1.0 / math.sqrt(HEAD_DIM)),
        grid=(rows, groups),
        in_specs=in_specs + [spec],
        out_specs=[spec, pair_spec, pair_spec, pair_spec],
        out_shape=[jax.ShapeDtypeStruct(query.shape, bf16)] + [pair_shape] * 3,
        cost_estimate=pl.CostEstimate(
            flops=flops * 6, bytes_accessed=16 * query.size * 2, transcendentals=0
        ),
        name="attend_back",
    )(query, *operands, bias, grad_attended)


def ffn_forward(normed, inner_parts, outer_parts, residual):
    kept = []
    total = residual
    for inner, outer in zip(inner_parts, outer_parts):
        act, slope = gelu_pair(product(normed, inner))
        act = act.astype(bf16)
        kept.append((act, slope.astype(bf16)))
        total = total + product(act, outer)
    return total, kept


def ffn_backward(kept, inner_parts, outer_parts, grad_branch):
    grad_pres = []
    grad_normed = None
    for (act, slope), inner, outer in zip(kept, inner_parts, outer_parts):
        grad_pre = (product_bt(grad_branch, outer) * slope.astype(f32)).astype(bf16)
        grad_pres.append(grad_pre)
        piece = product_bt(grad_pre, inner)
        grad_normed = piece if grad_normed is None else grad_normed + piece
    return grad_pres, grad_normed


def slice_owner(place):
    seq = lax.axis_index("seq")
    return seq + (1 - 2 * (seq % 2)) * (place % 2) + (2 - 4 * (seq // 2)) * (place // 2)


def slices_in_order(terms, operands):
    for place, (left, right) in enumerate(operands):
        values = weight_grad(left, right)
        terms = lax.dynamic_update_index_in_dim(terms, values, slice_owner(place), 0)
    return terms


class SliceSum:
    def __init__(self, operands):
        self.operands = operands

    def term(self, place):
        return weight_grad(*self.operands[place])

    def send_both(self, values):
        self.got_both = swap_core(values)

    def send_core(self, values):
        self.got_core = swap_core(values)

    def chip_sum(self):
        values = product_at(*self.operands[2]) + self.got_both.astype(f32)
        return row_major(values.astype(bf16))

    def send_chip(self, values):
        self.got_chip = swap_chip(values)

    def total(self):
        return self.own.astype(f32) + self.got_core.astype(f32) + self.got_chip.astype(f32)


def cube_bits():
    bits = []
    for axis in ("seq", "wide"):
        count = lax.axis_size(axis).bit_length() - 1
        bits += [(axis, bit) for bit in reversed(range(count))]
    return bits


def cube_orders(bits):
    core = bits.index(("seq", 0))
    chip = bits.index(("seq", 1))
    wide = [place for place, (axis, _) in enumerate(bits) if axis == "wide"]
    if len(wide) == 3:
        far, near, across = wide
        return ((chip, far, near, across, core), (chip, across, far, near, core))
    return ((chip, *wide, core), (chip, *wide[2:], *wide[:2], core))


def cube_place(bits):
    index = {axis: lax.axis_index(axis) for axis in ("seq", "wide")}
    mine = [lax.rem(index[axis] // (1 << bit), 2) for axis, bit in bits]

    def partner(place):
        axis, bit = bits[place]
        other = dict(index)
        other[axis] = index[axis] + (1 - 2 * mine[place]) * (1 << bit)
        return (other["seq"], other["wide"])

    return mine, partner


def cube_barrier(bits, partner):
    barrier = pltpu.get_barrier_semaphore()
    for place in range(len(bits)):
        pl.semaphore_signal(
            barrier, inc=1, device_id=partner(place), device_id_type=pl.DeviceIdType.MESH
        )
    pl.semaphore_wait(barrier, len(bits))


def gather_kernel(
    bits,
    orders,
    own_ref,
    inner_ref,
    outer_ref,
    out_ref,
    inner_core_ref,
    outer_core_ref,
    inner_chip_ref,
    send_sem,
    recv_sem,
    copy_sem,
    ride_send,
    ride_recv,
):
    mine, partner = cube_place(bits)
    own_copy = pltpu.make_async_copy(own_ref, out_ref.at[tuple(mine)], copy_sem)
    own_copy.start()
    cube_barrier(bits, partner)
    own_copy.wait()
    width = own_ref.shape[1] // len(orders)
    core = partner(bits.index(("seq", 0)))
    chip = partner(bits.index(("seq", 1)))
    rides = [
        (inner_ref.at[0, 0], inner_chip_ref, chip),
        (inner_ref.at[0], inner_core_ref, core),
        (outer_ref.at[0], outer_core_ref, core),
    ]
    rides = [
        pltpu.make_async_remote_copy(
            src_ref=source,
            dst_ref=target,
            send_sem=ride_send.at[place],
            recv_sem=ride_recv.at[place],
            device_id=device,
            device_id_type=pl.DeviceIdType.MESH,
        )
        for place, (source, target, device) in enumerate(rides)
    ]
    copies = []
    held = [[False] * len(bits) for _ in orders]
    for stage in range(len(bits)):
        for color, order in enumerate(orders):
            if stage:
                copies[(stage - 1) * len(orders) + color].wait_recv()
                held[color][order[stage - 1]] = True
            place = tuple(
                slice(None) if whole else mine[axis] for axis, whole in enumerate(held[color])
            )
            ref = out_ref.at[place + (slice(None), pl.ds(color * width, width))]
            copy = pltpu.make_async_remote_copy(
                src_ref=ref,
                dst_ref=ref,
                send_sem=send_sem.at[color, stage],
                recv_sem=recv_sem.at[color, stage],
                device_id=partner(order[stage]),
                device_id_type=pl.DeviceIdType.MESH,
            )
            copy.start()
            copies.append(copy)
        if stage == 0:
            for ride in rides:
                ride.start()
    for copy in copies:
        copy.wait_send()
    for copy in copies[-len(orders) :]:
        copy.wait_recv()
    for ride in rides:
        ride.wait()


def gather_rows(own, expert_in, expert_out):
    bits = cube_bits()
    orders = cube_orders(bits)
    rows, width = own.shape
    anywhere = pl.BlockSpec(memory_space=pl.ANY)
    out, inner_core, outer_core, inner_chip = pl.pallas_call(
        functools.partial(gather_kernel, bits, orders),
        in_specs=[pl.BlockSpec(memory_space=pltpu.VMEM), anywhere, anywhere],
        out_specs=[anywhere] * 4,
        out_shape=[
            jax.ShapeDtypeStruct((2,) * len(bits) + (rows, width), own.dtype),
            jax.ShapeDtypeStruct(expert_in.shape[1:], expert_in.dtype),
            jax.ShapeDtypeStruct(expert_out.shape[1:], expert_out.dtype),
            jax.ShapeDtypeStruct(expert_in.shape[2:], expert_in.dtype),
        ],
        scratch_shapes=[
            pltpu.SemaphoreType.DMA((len(orders), len(bits))),
            pltpu.SemaphoreType.DMA((len(orders), len(bits))),
            pltpu.SemaphoreType.DMA,
            pltpu.SemaphoreType.DMA((3,)),
            pltpu.SemaphoreType.DMA((3,)),
        ],
        compiler_params=pltpu.CompilerParams(collective_id=0, has_side_effects=True),
        cost_estimate=pl.CostEstimate(flops=0, bytes_accessed=25 * own.size << 5, transcendentals=0),
        name="gather_rows",
    )(own, expert_in, expert_out)
    return out.reshape(rows << len(bits), width), inner_core, outer_core, inner_chip


def scatter_kernel(bits, orders, terms_ref, out_ref, *scratch):
    stages = len(bits)
    colors = len(orders)
    got = scratch[: colors * stages]
    sums = scratch[colors * stages : colors * (2 * stages - 1)]
    send_sem, recv_sem = scratch[colors * (2 * stages - 1) :]
    mine, partner = cube_place(bits)
    cube_barrier(bits, partner)
    width = terms_ref.shape[-1] // colors
    copies = []

    def half(color, stage, keep):
        done = orders[color][:stage]
        place = []
        for axis in range(stages):
            if axis in done:
                continue
            if axis == orders[color][stage]:
                place.append(mine[axis] if keep else 1 - mine[axis])
            else:
                place.append(slice(None))
        if stage == 0:
            return terms_ref.at[tuple(place) + (slice(None), pl.ds(color * width, width))]
        return sums[color * (stages - 1) + stage - 1].at[tuple(place)]

    for stage in range(stages + 1):
        for color in range(colors):
            if stage:
                copies[(stage - 1) * colors + color].wait_recv()
                kept = half(color, stage - 1, True)[...].astype(f32)
                total = kept + got[color * stages + stage - 1][...].astype(f32)
                if stage == stages:
                    out_ref[:, pl.ds(color * width, width)] = total
                    continue
                sums[color * (stages - 1) + stage - 1][...] = total.astype(bf16)
            copy = pltpu.make_async_remote_copy(
                src_ref=half(color, stage, False),
                dst_ref=got[color * stages + stage],
                send_sem=send_sem.at[color, stage],
                recv_sem=recv_sem.at[color, stage],
                device_id=partner(orders[color][stage]),
                device_id_type=pl.DeviceIdType.MESH,
            )
            copy.start()
            copies.append(copy)
    for copy in copies:
        copy.wait_send()


def scatter_rows(terms):
    bits = cube_bits()
    orders = [order[::-1] for order in cube_orders(bits)]
    colors = len(orders)
    stages = len(bits)
    rows = terms.shape[0] >> stages
    width = terms.shape[1]
    got = [
        pltpu.VMEM((2,) * (stages - 1 - stage) + (rows, width // colors), bf16)
        for _ in range(colors)
        for stage in range(stages)
    ]
    sums = [
        pltpu.VMEM((2,) * (stages - 1 - stage) + (rows, width // colors), bf16)
        for _ in range(colors)
        for stage in range(stages - 1)
    ]
    return pl.pallas_call(
        functools.partial(scatter_kernel, bits, orders),
        in_specs=[pl.BlockSpec(memory_space=pltpu.VMEM)],
        out_specs=pl.BlockSpec(memory_space=pltpu.VMEM),
        out_shape=jax.ShapeDtypeStruct((rows, width), f32),
        scratch_shapes=got
        + sums
        + [
            pltpu.SemaphoreType.DMA((colors, stages)),
            pltpu.SemaphoreType.DMA((colors, stages)),
        ],
        compiler_params=pltpu.CompilerParams(collective_id=1, has_side_effects=True),
        cost_estimate=pl.CostEstimate(flops=0, bytes_accessed=50 * terms.size, transcendentals=0),
        name="scatter_rows",
    )(terms.reshape((2,) * stages + (rows, width)))


def together(*values):
    return lax.optimization_barrier(values)


def per_device(
    block_input,
    segment_ids,
    assignment,
    norm_attn,
    weight_qkv,
    weight_proj,
    norm_ffn,
    weight_up,
    weight_down,
    centroids,
    expert_norms,
    expert_in,
    expert_out,
    grad_out,
):
    row_count, local_len, model_width = block_input.shape
    token_count = row_count * local_len
    seq_devices = lax.axis_size("seq")
    seq_index = lax.axis_index("seq")
    experts = lax.axis_size("wide")
    devices = seq_devices * experts
    every = ("seq", "wide")
    shard = weight_up.shape[0]
    hidden_width = weight_up.shape[1]

    gains_own = jnp.stack([norm_attn, norm_ffn], axis=1)
    first_own = jnp.concatenate(
        [weight_qkv, jnp.pad(gains_own, ((0, 0), (0, 2 * LANES - gains_own.shape[1])))], axis=1
    )
    qkv_full, inner_core, outer_core, inner_first = gather_rows(first_own, expert_in, expert_out)
    gains_all = qkv_full[:, 3 * model_width : 3 * model_width + 2].astype(f32).T
    gain_attn = gains_all[0]
    gain_ffn = gains_all[1]
    up_own = (
        weight_up.reshape(shard, devices, BLOCKS, shard)
        .transpose(0, 2, 1, 3)
        .reshape(shard, hidden_width)
    )
    down_own = weight_down.reshape(BLOCKS, shard, model_width).transpose(1, 0, 2)
    rest_own = jnp.concatenate(
        [weight_proj, up_own, down_own.reshape(shard, BLOCKS * model_width)], axis=1
    )
    rest_own, _ = together(rest_own, qkv_full)
    rest_full = lax.all_gather(rest_own, every, axis=0, tiled=True)

    def rest_block(index):
        return rest_full[:, index * model_width : (index + 1) * model_width]

    proj_full = rest_block(0)
    up_parts = [rest_block(1 + index) for index in range(BLOCKS)]
    down_parts = [rest_block(1 + BLOCKS + index) for index in range(BLOCKS)]

    inner_own = expert_in[0]
    outer_own = expert_out[0]
    inner_chip = [inner_first, None]
    outer_chip = [None, None]

    capacity = token_count // experts
    chosen = assignment.reshape(token_count)
    one_hot = (chosen[:, None] == jnp.arange(experts, dtype=jnp.int32)[None, :]).astype(jnp.int32)
    rank_within = jnp.sum((jnp.cumsum(one_hot, axis=0) - 1) * one_hot, axis=1)
    slot_index = chosen * capacity + rank_within
    source_of = (
        jnp.zeros((token_count,), jnp.int32)
        .at[slot_index]
        .set(jnp.arange(token_count, dtype=jnp.int32))
    )

    tokens_flat = block_input.reshape(token_count, model_width).astype(f32)
    normed_attn = layer_norm(tokens_flat, gain_attn).astype(bf16)
    kv_own = product(normed_attn, qkv_full[:, model_width : 3 * model_width]).astype(bf16)
    kv_own = kv_own.reshape(row_count, local_len, 2 * model_width)
    query = product(normed_attn, qkv_full[:, :model_width]).astype(bf16)
    query = query.reshape(row_count, local_len, model_width)

    kv_far = seq_send(kv_own, [(0, 2), (1, 3)])
    kv_near = seq_send(
        jnp.where(seq_index == 3, kv_far, kv_own), [(0, 1), (2, 3), (3, 2)]
    )
    kv_blocks = (kv_own, kv_near, kv_far)
    before = 2 * local_len
    offset = seq_index * local_len
    padded_seg = jnp.pad(segment_ids, ((0, 0), (before, 0)), constant_values=-1)
    key_seg = lax.dynamic_slice_in_dim(padded_seg, offset, before + local_len, 1)
    query_seg = key_seg[:, before:]
    key_pos = jnp.arange(before + local_len)
    query_pos = before + jnp.arange(local_len)
    allowed = (key_seg[:, :, None] == query_seg[:, None, :]) & (
        key_pos[None, :, None] <= query_pos[None, None, :]
    )
    bias = jnp.where(allowed, 0.0, -1e30).astype(f32)

    attended_rows, outer_chip[0] = attend(query, kv_blocks, bias, outer_own)
    late = together(inner_own[1], outer_own[1], attended_rows)
    inner_chip[1], outer_chip[1] = [swap_chip(part) for part in late[:2]]
    attended = attended_rows.reshape(token_count, model_width)
    hidden = tokens_flat + product(attended, proj_full)
    normed_ffn = layer_norm(hidden, gain_ffn).astype(bf16)
    dense_out, dense_kept = ffn_forward(normed_ffn, up_parts, down_parts, hidden)
    routed = dense_out.astype(bf16)

    received = lax.all_to_all(routed[source_of], "wide", split_axis=0, concat_axis=0, tiled=True)
    fresh = jnp.zeros((seq_devices,) + inner_own.shape[1:], bf16)
    received, inner_chip[1], fresh = together(received, inner_chip[1], fresh)
    received_f = received.astype(f32)
    inner_both = [swap_core(together(inner_chip[0], attended)[0]), None]
    outer_both = [swap_core(together(outer_chip[0], attended)[0]), None]
    centroid_row = centroids[0]
    centroid_f = centroid_row.astype(f32)
    logit_row = jnp.dot(received, centroid_row, preferred_element_type=f32)
    gate_value = jax.nn.sigmoid(logit_row)
    gains_f = expert_norms[0].astype(f32)
    state_now = received_f
    kept_layers = []
    slices = []
    for sublayer in range(2):
        if sublayer:
            inner_both[1] = swap_core(together(inner_chip[1], state_now)[0])
            outer_both[1] = swap_core(together(outer_chip[1], state_now)[0])
        inner_parts = [part[sublayer] for part in (inner_own, inner_core, inner_chip, inner_both)]
        outer_parts = [part[sublayer] for part in (outer_own, outer_core, outer_chip, outer_both)]
        normed = layer_norm(state_now, gains_f[sublayer]).astype(bf16)
        state_next, kept = ffn_forward(normed, inner_parts, outer_parts, state_now)
        kept_layers.append((state_now, normed, kept))
        slices.append((inner_parts, outer_parts))
        state_now = state_next
    returned = (gate_value[:, None] * state_now).astype(bf16)
    back_rows = lax.all_to_all(returned, "wide", split_axis=0, concat_axis=0, tiled=True)
    output = (
        (dense_out + back_rows[slot_index].astype(f32)).astype(bf16).reshape(block_input.shape)
    )
    gate_sum = jnp.sum(gate_value)
    score_sum = jnp.sum(logit_row * logit_row)
    grad_flat = grad_out.reshape(token_count, model_width)
    grad_back = lax.all_to_all(
        grad_flat[source_of], "wide", split_axis=0, concat_axis=0, tiled=True
    )
    grad_ret = grad_back.astype(f32)
    grad_gate = jnp.sum(grad_ret * state_now, axis=-1)
    grad_state = grad_ret * gate_value[:, None]
    gain_grads = [None, None]
    weight_terms = [None, None]
    sums = [None, None]
    for sublayer in (1, 0):
        state_in, normed_in, kept = kept_layers[sublayer]
        inner_parts, outer_parts = slices[sublayer]
        grad_branch = grad_state.astype(bf16)
        grad_pres, grad_normed = ffn_backward(kept, inner_parts, outer_parts, grad_branch)
        weight_terms[sublayer] = (
            [(act, grad_branch) for act, _ in kept],
            [(normed_in, grad_pre) for grad_pre in grad_pres],
        )
        grad_resid, gain_grad = norm_back(state_in, gains_f[sublayer], grad_normed)
        grad_state = grad_state + grad_resid
        gain_grads[sublayer] = gain_grad
        sums[sublayer] = [SliceSum(operands) for operands in weight_terms[sublayer]]
        if sublayer:
            outer1 = sums[1][0]
            grad_state, both, fresh = together(
                grad_state, outer1.term(3), slices_in_order(fresh, weight_terms[1][1])
            )
            outer1.send_both(both)
            inner_second = lax.psum_scatter(fresh, "seq", scatter_dimension=0, tiled=True)
    grad_logit = grad_gate * gate_value * (1.0 - gate_value)
    grad_routed = (grad_state + grad_logit[:, None] * centroid_f[None, :]).astype(bf16)
    centroid_grad = jnp.dot(grad_logit, received_f, precision=highest)
    grad_routed, held = together(grad_routed, outer1.chip_sum())
    outer1.send_chip(held)
    returned_grad = lax.all_to_all(grad_routed, "wide", split_axis=0, concat_axis=0, tiled=True)
    outer0, inner0 = sums[0]
    returned_grad, *held = together(
        returned_grad,
        outer0.term(3),
        inner0.term(3),
        outer1.term(1),
        outer0.term(1),
        inner0.term(1),
        outer1.term(0),
    )
    outer0.send_both(held[0])
    inner0.send_both(held[1])
    outer1.send_core(held[2])
    outer0.send_core(held[3])
    inner0.send_core(held[4])
    outer1.own = held[5]
    grad_dense = grad_flat.astype(f32) + returned_grad[slot_index].astype(f32)

    grad_down_in = grad_dense.astype(bf16)
    grad_pres, grad_normed_ffn = ffn_backward(dense_kept, up_parts, down_parts, grad_down_in)
    grad_hidden_norm, grad_gain_ffn = norm_back(hidden, gain_ffn, grad_normed_ffn)
    grad_hidden = grad_dense + grad_hidden_norm
    grad_down_late, outer1.got_chip, held = together(
        grad_down_in, outer1.got_chip, outer0.chip_sum()
    )
    outer0.send_chip(held)
    grad_proj = grad_hidden.astype(bf16)
    rest_grad = jnp.concatenate(
        [weight_grad(attended, grad_proj)]
        + [weight_grad(normed_ffn, grad_pre) for grad_pre in grad_pres]
        + [weight_grad(act, grad_down_late) for act, _ in dense_kept],
        axis=1,
    )
    rest_grad = row_major(rest_grad)
    grad_attended = product_bt(grad_proj, proj_full).astype(bf16)
    grad_attended, rest_grad = together(grad_attended, rest_grad)
    rest_sum = lax.psum_scatter(rest_grad, every, scatter_dimension=0, tiled=True).astype(f32)
    grad_query, grad_kv0, grad_kv1, grad_kv2 = attend_back(
        query, kv_blocks, bias, grad_attended.reshape(query.shape)
    )
    grad_kv1, outer0.got_chip = together(grad_kv1, outer0.got_chip)
    got_near = seq_send(grad_kv1, [(1, 0), (3, 2), (2, 3)])
    far_sum = jnp.where(
        seq_index == 3, (grad_kv2.astype(f32) + got_near.astype(f32)).astype(bf16), grad_kv2
    )
    got_far = seq_send(far_sum, [(2, 0), (3, 1)])
    outer0.own = outer0.term(0)
    got_far, inner0.own, inner_send, outer_total = together(
        got_far,
        inner0.term(0),
        inner0.chip_sum(),
        jnp.stack([outer0.total(), outer1.total()]),
    )
    inner0.send_chip(inner_send)
    kv_sum = grad_kv0.astype(f32) + got_far.astype(f32)
    kv_sum = kv_sum + jnp.where(seq_index % 2 == 0, got_near.astype(f32), 0.0)
    kv_sum = kv_sum.astype(bf16).reshape(2, token_count, model_width)
    grad_qkv = [grad_query.reshape(token_count, model_width), kv_sum[0], kv_sum[1]]
    qkv_grad = row_major(
        jnp.concatenate([weight_grad(normed_attn, part) for part in grad_qkv], axis=1)
    )
    grad_normed_attn = sum(
        product_bt(part, qkv_full[:, index * model_width : (index + 1) * model_width])
        for index, part in enumerate(grad_qkv)
    )
    grad_input_norm, grad_gain_attn = norm_back(tokens_flat, gain_attn, grad_normed_attn)
    grad_input = (grad_hidden + grad_input_norm).reshape(block_input.shape)

    gain_terms = jnp.stack([grad_gain_attn, grad_gain_ffn]).reshape(2, devices, shard)
    gain_terms, qkv_grad = together(gain_terms.transpose(1, 0, 2), qkv_grad)
    gain_terms = lax.all_to_all(gain_terms, every, 0, 0, tiled=True)
    qkv_sum = scatter_rows(qkv_grad)
    gain_sums = jnp.sum(gain_terms, axis=0)
    totals = jnp.concatenate(
        [
            jnp.stack(gain_grads),
            centroid_grad.reshape(1, model_width),
            jnp.pad(jnp.stack([gate_sum, score_sum]), (0, model_width - 2))[None],
        ]
    )
    totals = totals + swap_core(totals)
    totals = totals + swap_chip(totals)
    up_grad = (
        rest_sum[:, model_width : model_width + hidden_width]
        .reshape(shard, BLOCKS, devices, shard)
        .transpose(0, 2, 1, 3)
        .reshape(shard, hidden_width)
    )
    down_grad = (
        rest_sum[:, model_width + hidden_width :]
        .reshape(shard, BLOCKS, model_width)
        .transpose(1, 0, 2)
        .reshape(BLOCKS * shard, model_width)
    )
    token_total = token_count * seq_devices
    return (
        output,
        grad_input,
        gain_sums[0],
        qkv_sum,
        rest_sum[:, :model_width],
        gain_sums[1],
        up_grad,
        down_grad,
        totals[2:3],
        totals[:2][None],
        jnp.stack([inner0.total(), inner_second[0].astype(f32)])[None],
        outer_total[None],
        totals[3, :1] / token_total,
        totals[3, 1:2] / token_total,
    )


def solution(mesh):
    in_specs = (
        P("wide", "seq", None),
        P("wide", None),
        P("wide", "seq"),
        P(("seq", "wide")),
        P(("seq", "wide"), None),
        P(("seq", "wide"), None),
        P(("seq", "wide")),
        P(("seq", "wide"), None),
        P(("seq", "wide"), None),
        P("wide", None),
        P("wide", None, None),
        P("wide", None, None, "seq"),
        P("wide", None, "seq", None),
        P("wide", "seq", None),
    )
    out_specs = (
        P("wide", "seq", None),
        P("wide", "seq", None),
        P(("seq", "wide")),
        P(("seq", "wide"), None),
        P(("seq", "wide"), None),
        P(("seq", "wide")),
        P(("seq", "wide"), None),
        P(("seq", "wide"), None),
        P("wide", None),
        P("wide", None, None),
        P("wide", None, None, "seq"),
        P("wide", None, "seq", None),
        P("wide"),
        P("wide"),
    )
    return jax.shard_map(
        per_device, mesh=mesh, in_specs=in_specs, out_specs=out_specs, check_vma=False
    )
```
